8 devices in a mesh: col: 4 (over z, y, x), row: 2 (over core).
Axes of the slice: x: 2, y: 2, z: 1, core: 2. Of those that a mesh axis runs over, the one named last changes fastest.
Arguments:
- t_amps: float32 [256, 9216], P('row', 'col')
- denoms: float32 [256, 9216], P('row', 'col')
- v_oovv: bfloat16 [256, 9216], P('row', 'col')
- v_vvvv: bfloat16 [9216, 9216], P('row', 'col')
- v_oooo: bfloat16 [256, 256], replicated
- w_direct: bfloat16 [1536, 1536], P(None, 'col')
- w_exch: bfloat16 [1536, 1536], P(None, 'col')
Outputs:
- output: float32 [256, 9216], P('row', 'col')
All inputs are finite; a program needn't handle non-finite values.
Results may differ from the reference program's by a relative error of at most 0.001.
Values are sent between devices in bfloat16 or wider.
A program may use at most 1 GiB of HBM per device.

```python
import jax
import jax.numpy as jnp

OCC = 16
VIRT = 96
PAIRS_OCC = OCC * OCC
PAIRS_VIRT = VIRT * VIRT
PH_DIM = OCC * VIRT


def setup_inputs(seed: int = 0) -> dict:
    keys = jax.random.split(jax.random.key(seed), 7)
    amp_scale = 1.5 * (OCC * VIRT) ** -0.5
    t_amps = amp_scale * jax.random.normal(keys[0], (PAIRS_OCC, PAIRS_VIRT), jnp.float32)
    denoms = -jax.random.uniform(keys[1], (PAIRS_OCC, PAIRS_VIRT), jnp.float32, 1.0, 3.0)
    v_oovv = jax.random.normal(keys[2], (PAIRS_OCC, PAIRS_VIRT), jnp.float32).astype(jnp.bfloat16)
    vvvv_scale = (OCC / VIRT) ** 0.5 / 1.5
    v_vvvv = (vvvv_scale * jax.random.normal(keys[3], (PAIRS_VIRT, PAIRS_VIRT), jnp.float32)).astype(jnp.bfloat16)
    oooo_scale = (VIRT / OCC) ** 0.5 / 1.5
    v_oooo = (oooo_scale * jax.random.normal(keys[4], (PAIRS_OCC, PAIRS_OCC), jnp.float32)).astype(jnp.bfloat16)
    w_direct = (0.6 * jax.random.normal(keys[5], (PH_DIM, PH_DIM), jnp.float32)).astype(jnp.bfloat16)
    w_exch = (0.6 * jax.random.normal(keys[6], (PH_DIM, PH_DIM), jnp.float32)).astype(jnp.bfloat16)
    return {"t_amps": t_amps, "denoms": denoms, "v_oovv": v_oovv, "v_vvvv": v_vvvv, "v_oooo": v_oooo, "w_direct": w_direct, "w_exch": w_exch}


def reference(t_amps, denoms, v_oovv, v_vvvv, v_oooo, w_direct, w_exch):
    t_half = t_amps.astype(jnp.bfloat16)
    ladder = jnp.dot(t_half, v_vvvv, preferred_element_type=jnp.float32)
    inter_x = jnp.dot(v_oovv, t_half.T, preferred_element_type=jnp.float32)
    hole_mat = (v_oooo.astype(jnp.float32) + 0.5 * inter_x).astype(jnp.bfloat16)
    hole_term = jnp.dot(hole_mat.T, t_half, preferred_element_type=jnp.float32)
    t_wide = t_half.astype(jnp.float32).reshape(OCC, OCC, VIRT, VIRT)
    wd_wide = w_direct.astype(jnp.float32).reshape(OCC, VIRT, OCC, VIRT)
    wx_wide = w_exch.astype(jnp.float32).reshape(OCC, VIRT, OCC, VIRT)
    direct_term = jnp.einsum("ikac,kcjb->ijab", t_wide, wd_wide)
    exch_term = jnp.einsum("ikcb,kcja->ijab", t_wide, wx_wide)
    ph_net = direct_term - exch_term
    ph_sym = (ph_net + ph_net.transpose(1, 0, 3, 2)).reshape(PAIRS_OCC, PAIRS_VIRT)
    residual = v_oovv.astype(jnp.float32) + ladder + hole_term + ph_sym
    return residual / denoms
```

```python
import functools

import jax
import jax.numpy as jnp
from jax import lax
from jax.experimental import pallas as pl
from jax.experimental.pallas import tpu as pltpu
from jax.sharding import PartitionSpec as P

MESH = pl.DeviceIdType.MESH
F32 = jnp.float32
BF16 = jnp.bfloat16
NT = (((1,), (1,)), ((), ()))
TN = (((0,), (0,)), ((), ()))


def _place():
    r, c = lax.axis_index("row"), lax.axis_index("col")
    x, y = c % 2, c // 2
    return r, c, y * 2 + (1 - x), (1 - y) * 2 + x, (1 - y) * 2 + (1 - x)


def _dev(c, r):
    return {"col": c, "row": r}


def _barrier(r, c, nx, ny, dg):
    sem = pltpu.get_barrier_semaphore()
    o = 1 - r
    for cc, rr in ((nx, r), (ny, r), (dg, r), (c, o), (nx, o), (ny, o), (dg, o)):
        pl.semaphore_signal(sem, inc=1, device_id=_dev(cc, rr), device_id_type=MESH)
    pl.semaphore_wait(sem, 7)


def _rcopy(src, dst, ssem, rsem, dev):
    return pltpu.make_async_remote_copy(src, dst, ssem, rsem, device_id=dev, device_id_type=MESH)


def gather_kernel(t_ref, oovv_ref, oooo_ref, rows_out, lad_out, hole_out,
                  tg, xp, xr, mfull, hole, ssem, rsem, xs, xrs, ms, mrs, osem):
    r, c, nx, ny, dg = _place()
    o = 1 - r
    n = t_ref.shape[0]
    w = t_ref.shape[1]
    h = w // 2
    rows = pl.ds(pl.multiple_of(r * n, n), n)
    orows = pl.ds(pl.multiple_of(o * n, n), n)
    h0, h1 = pl.ds(0, h), pl.ds(h, h)
    _barrier(r, c, nx, ny, dg)

    d_own = _rcopy(t_ref, tg.at[c, rows], ssem.at[0], rsem.at[0], _dev(c, o))
    x0 = _rcopy(t_ref.at[:, h0], tg.at[c, rows, h0], ssem.at[1], rsem.at[1], _dev(nx, r))
    y1 = _rcopy(t_ref.at[:, h1], tg.at[c, rows, h1], ssem.at[2], rsem.at[2], _dev(ny, r))
    x1 = _rcopy(t_ref.at[:, h1], tg.at[c, rows, h1], ssem.at[3], rsem.at[3], _dev(nx, r))
    y0 = _rcopy(t_ref.at[:, h0], tg.at[c, rows, h0], ssem.at[4], rsem.at[4], _dev(ny, r))
    d_own.start()
    x0.start()
    y1.start()
    tg[c, rows, :] = t_ref[...]

    d_own.wait_recv()
    xp[...] = lax.dot_general(oovv_ref[...], tg[c], NT, preferred_element_type=F32)
    q = n // 4
    xcopies = []
    for s, cc in enumerate((nx, ny, dg)):
        cp = _rcopy(xp.at[pl.ds(pl.multiple_of(cc * q, q), q)], xr.at[c], xs.at[s], xrs.at[s], _dev(cc, r))
        cp.start()
        xcopies.append(cp)
    x1.start()
    y0.start()
    piece = pl.ds(pl.multiple_of(c * q, q), q)
    xr[c, :, :] = xp[piece, :]
    for cp in xcopies:
        cp.wait_recv()
    xsum = (xr[0] + xr[1]) + (xr[2] + xr[3])
    krows = pl.ds(pl.multiple_of(r * n + c * q, q), q)
    mfull[krows, :] = (oooo_ref[krows, :].astype(F32) + 0.5 * xsum).astype(BF16)
    mcopies = []
    for s, (cc, rr) in enumerate(((nx, r), (ny, r), (dg, r), (c, o), (nx, o), (ny, o), (dg, o))):
        cp = _rcopy(mfull.at[krows], mfull.at[krows], ms.at[s], mrs.at[s], _dev(cc, rr))
        cp.start()
        mcopies.append(cp)

    x0.wait_recv()
    f0 = _rcopy(tg.at[nx, rows, h0], tg.at[nx, rows, h0], ssem.at[5], rsem.at[5], _dev(ny, r))
    f0.start()
    y1.wait_recv()
    f1 = _rcopy(tg.at[ny, rows, h1], tg.at[ny, rows, h1], ssem.at[6], rsem.at[6], _dev(nx, r))
    f1.start()
    x1.wait_recv()
    d_x = _rcopy(tg.at[nx, rows], tg.at[nx, rows], ssem.at[7], rsem.at[7], _dev(c, o))
    d_x.start()
    y0.wait_recv()
    d_y = _rcopy(tg.at[ny, rows], tg.at[ny, rows], ssem.at[8], rsem.at[8], _dev(c, o))
    d_y.start()

    for cp in mcopies:
        cp.wait_recv()
    m_mine = mfull[:, rows]
    step = 256

    @pl.loop(0, w // step)
    def _(s):
        lanes = pl.ds(pl.multiple_of(s * step, step), step)
        hole[:, lanes] = lax.dot_general(m_mine, tg[c, :, lanes], TN, preferred_element_type=F32)

    f0.wait_recv()
    f1.wait_recv()
    d_d = _rcopy(tg.at[dg, rows], tg.at[dg, rows], ssem.at[9], rsem.at[9], _dev(c, o))
    d_d.start()
    outs = [pltpu.make_async_copy(hole, hole_out, osem.at[0])]
    for cc in range(4):
        outs.append(pltpu.make_async_copy(tg.at[cc, rows], rows_out.at[:, pl.ds(cc * w, w)], osem.at[1 + cc]))
    for cp in outs:
        cp.start()
    d_x.wait_recv()
    d_y.wait_recv()
    d_d.wait_recv()
    for p in range(2):
        cp = pltpu.make_async_copy(tg.at[2 * r + p], lad_out.at[:, pl.ds(p * w, w)], osem.at[5 + p])
        cp.start()
        outs.append(cp)
    for cp in (d_own, x0, y1, x1, y0, f0, f1, d_x, d_y, d_d, *xcopies, *mcopies):
        cp.wait_send()
    for cp in outs:
        cp.wait()


def exchange_kernel(s_ref, p_ref, t_ref, v_ref, hole_ref, oovv_ref, den_ref, out_ref,
                    srecv, precv, vbuf, tl, mine, theirs, sbuf, ss, srs, ps, prs, vsem, tsem, rs, rrs, lsem):
    r, c, nx, ny, dg = _place()
    o = 1 - r
    w = out_ref.shape[1]
    n = out_ref.shape[0]
    step = vbuf.shape[2]
    steps = w // step
    tload = pltpu.make_async_copy(t_ref, tl, tsem)
    tload.start()

    def vcopy(s, slot):
        lanes = pl.ds(pl.multiple_of(s * step, step), step)
        return pltpu.make_async_copy(v_ref.at[:, lanes], vbuf.at[slot], vsem.at[slot])

    vcopy(0, 0).start()
    vcopy(1, 1).start()
    _barrier(r, c, nx, ny, dg)

    def cols(cc):
        return pl.ds(pl.multiple_of(cc * w, w), w)

    own = c // 2
    half = c % 2
    copies = []
    for s, cc in enumerate((dg, nx, ny)):
        copies.append(_rcopy(s_ref.at[:, :, cols(cc)], srecv.at[c], ss.at[s], srs.at[c], _dev(cc, r)))
        copies.append(_rcopy(p_ref.at[:, :, cols(cc)], precv.at[half, r], ps.at[s], prs.at[half, r], _dev(cc, own)))
    for cp in copies:
        cp.start()
    local = pltpu.make_async_copy(s_ref.at[:, :, cols(c)], srecv.at[c], srs.at[c])
    local.start()
    p_near = pltpu.make_async_copy(p_ref.at[:, :, cols(c)], precv.at[half, r], prs.at[half, r])
    p_far = _rcopy(p_ref.at[:, :, cols(c)], precv.at[half, r], ps.at[3], prs.at[half, r], _dev(c, own))

    @pl.when(own == r)
    def _():
        p_near.start()

    @pl.when(own != r)
    def _():
        p_far.start()

    tload.wait()

    def half_rows(k):
        return pl.ds(pl.multiple_of(k * n, n), n)

    def ladder_copy(s):
        lanes = pl.ds(pl.multiple_of(s * step, step), step)
        return _rcopy(sbuf.at[s], theirs.at[:, lanes], rs.at[s], rrs.at[s], _dev(c, o))

    @pl.loop(0, steps)
    def _(s):
        slot = s % 3

        @pl.when(s + 2 < steps)
        def _():
            vcopy(s + 2, (s + 2) % 3).start()

        vcopy(s, slot).wait()
        lanes = pl.ds(pl.multiple_of(s * step, step), step)
        vb = vbuf.at[slot]
        sbuf[s, :, :] = jnp.dot(tl[half_rows(o), :], vb[...], preferred_element_type=F32)
        ladder_copy(s).start()
        mine[:, lanes] = jnp.dot(tl[half_rows(r), :], vb[...], preferred_element_type=F32)

    @pl.loop(0, steps)
    def _(s):
        ladder_copy(s).wait()

    for cc in range(4):
        pltpu.make_async_copy(s_ref.at[:, :, cols(c)], srecv.at[cc], srs.at[cc]).wait()
    for a in range(2):
        for b in range(2):
            pltpu.make_async_copy(p_ref.at[:, :, cols(c)], precv.at[a, b], prs.at[a, b]).wait()
    for cp in copies:
        cp.wait_send()

    @pl.when(own != r)
    def _():
        p_far.wait_send()

    nb = precv.shape[2]
    for i in range(srecv.shape[1]):
        line = pl.ds(i * 16, 16)
        sv = jnp.concatenate([srecv[cc, i] for cc in range(4)], axis=0)
        pv = jnp.concatenate([precv[i // nb, b, i % nb] for b in range(2)], axis=0)
        total = oovv_ref[line, :].astype(F32) + (mine[line, :] + theirs[line, :] + hole_ref[line, :]) + (sv + pv)
        out_ref[line, :] = total / den_ref[line, :]


VM = pl.BlockSpec(memory_space=pltpu.VMEM)
ANY = pl.BlockSpec(memory_space=pl.ANY)
DMA = pltpu.SemaphoreType.DMA


def gather(t_half, oovv, oooo):
    n, w = t_half.shape
    return pl.pallas_call(
        gather_kernel,
        out_shape=(
            jax.ShapeDtypeStruct((n, 4 * w), BF16),
            jax.ShapeDtypeStruct((2 * n, 2 * w), BF16),
            jax.ShapeDtypeStruct((n, w), F32),
        ),
        in_specs=[VM, VM, VM],
        out_specs=(ANY, ANY, ANY),
        scratch_shapes=[
            pltpu.VMEM((4, 2 * n, w), BF16),
            pltpu.VMEM((n, 2 * n), F32),
            pltpu.VMEM((4, n // 4, 2 * n), F32),
            pltpu.VMEM((2 * n, 2 * n), BF16),
            pltpu.VMEM((n, w), F32),
            DMA((10,)), DMA((10,)), DMA((3,)), DMA((3,)), DMA((7,)), DMA((7,)), DMA((7,)),
        ],
        compiler_params=pltpu.CompilerParams(collective_id=0, has_side_effects=True, vmem_limit_bytes=40 << 20),
        name="gather",
    )(t_half, oovv, oooo)


def exchange(s_parts, p_parts, t_lad, vvvv, hole, oovv, den):
    n, w = den.shape
    step = 256
    steps = w // step
    depth = vvvv.shape[0]
    return pl.pallas_call(
        exchange_kernel,
        out_shape=jax.ShapeDtypeStruct((n, w), F32),
        in_specs=[ANY, ANY, ANY, ANY, VM, VM, VM],
        out_specs=VM,
        scratch_shapes=[
            pltpu.VMEM((4, 8, 4, w), F32),
            pltpu.VMEM((2, 2, 4, 8, w), F32),
            pltpu.VMEM((3, depth, step), BF16),
            pltpu.VMEM((2 * n, depth), BF16),
            pltpu.VMEM((n, w), F32),
            pltpu.VMEM((n, w), F32),
            pltpu.VMEM((steps, n, step), F32),
            DMA((3,)), DMA((4,)), DMA((4,)), DMA((2, 2)), DMA((3,)), DMA, DMA((steps,)), DMA((steps,)), DMA,
        ],
        compiler_params=pltpu.CompilerParams(collective_id=1, has_side_effects=True, vmem_limit_bytes=60 << 20),
        name="exchange",
    )(s_parts, p_parts, t_lad, vvvv, hole, oovv, den)


def solution(mesh):
    def local_sweep(t_blk, d_blk, oovv_blk, vvvv_blk, oooo_full, wd_blk, wx_blk):
        t_half = t_blk.astype(BF16)
        t_rows, t_lad, hole = gather(t_half, oovv_blk, oooo_full)
        t_four = t_rows.reshape(8, 16, 96, 96)
        direct = jnp.einsum("ikac,kcjb->ijab", t_four, wd_blk.reshape(16, 96, 4, 96), preferred_element_type=F32)
        exch = jnp.einsum("ikcb,kcja->ijab", t_four, wx_blk.reshape(16, 96, 4, 96), preferred_element_type=F32)
        s = direct - exch
        s_parts = s.reshape(8, 4, 9216)
        p_parts = s.transpose(1, 0, 3, 2).reshape(4, 8, 9216)
        return exchange(s_parts, p_parts, t_lad, vvvv_blk, hole, oovv_blk, d_blk)

    amp = P("row", "col")
    wide = P(None, "col")
    return jax.shard_map(local_sweep, mesh=mesh, in_specs=(amp, amp, amp, amp, P(), wide, wide), out_specs=amp, check_vma=False)
```

```python
import jax
import jax.numpy as jnp
from jax import lax
from jax.experimental import pallas as pl
from jax.experimental.pallas import tpu as pltpu
from jax.sharding import PartitionSpec as P

MESH = pl.DeviceIdType.MESH
F32 = jnp.float32
BF16 = jnp.bfloat16
NT = (((1,), (1,)), ((), ()))
TN = (((0,), (0,)), ((), ()))

OCC = 16
VIRT = 96
LANE = 128
PITCH = 104
STEP = 256


def _dev(c, r):
    return {"col": c, "row": r}


def _rcopy(src, dst, ssem, rsem, dev):
    return pltpu.make_async_remote_copy(src, dst, ssem, rsem, device_id=dev, device_id_type=MESH)


def sweep_kernel(t_hbm, oovv_hbm, v_hbm, oooo_hbm, wd_hbm, wx_hbm, out_ref,
                 t32, oovv, oooo, wd, wx, tg, xp, xr, mfull, hole, t4, wd4, wxt, ubuf, vbuf_s, s4, st4,
                 smsg, pmsg, srecv, precv, vv, tl, mine, theirs, part,
                 lsem, gs, gr, xs, xrs, ms, mrs, ss, srs, ps, prs, vsem, rs, rrs):
    r, c = lax.axis_index("row"), lax.axis_index("col")
    x, y = c % 2, c // 2
    o = 1 - r
    nx, ny, dg = y * 2 + (1 - x), (1 - y) * 2 + x, (1 - y) * 2 + (1 - x)
    n, w = t32.shape
    h = w // 2
    h0, h1 = pl.ds(0, h), pl.ds(h, h)
    rows = pl.ds(pl.multiple_of(r * n, n), n)
    orows = pl.ds(pl.multiple_of(o * n, n), n)

    loads = [pltpu.make_async_copy(a, b, lsem.at[k]) for k, (a, b) in enumerate(
        ((t_hbm, t32), (oovv_hbm, oovv), (oooo_hbm, oooo), (wd_hbm, wd), (wx_hbm, wx)))]
    for cp in loads:
        cp.start()

    def vcopy(s, slot):
        lanes = pl.ds(pl.multiple_of(s * STEP, STEP), STEP)
        return pltpu.make_async_copy(v_hbm.at[:, lanes], vv.at[slot], vsem.at[slot])

    loads[0].wait()
    tg[c, rows, :] = t32[...].astype(BF16)

    sem = pltpu.get_barrier_semaphore()
    for cc, rr in ((nx, r), (ny, r), (dg, r), (c, o), (nx, o), (ny, o), (dg, o)):
        pl.semaphore_signal(sem, inc=1, device_id=_dev(cc, rr), device_id_type=MESH)
    pl.semaphore_wait(sem, 7)

    def tcopy(chip, lanes, k, dev):
        ref = tg.at[chip, rows, lanes]
        return _rcopy(ref, ref, gs.at[k], gr.at[k], dev)

    whole = pl.ds(0, w)
    x0 = tcopy(c, h0, 1, _dev(nx, r))
    y1 = tcopy(c, h1, 2, _dev(ny, r))
    d_own = tcopy(c, whole, 0, _dev(c, o))
    x1 = tcopy(c, h1, 3, _dev(nx, r))
    y0 = tcopy(c, h0, 4, _dev(ny, r))
    x0.start()
    y1.start()
    d_own.start()
    vcopy(0, 0).start()
    vcopy(1, 1).start()

    loads[1].wait()
    loads[2].wait()
    d_own.wait_recv()
    xp[...] = lax.dot_general(oovv[...], tg[c], NT, preferred_element_type=F32)
    q = n // 4
    xcopies = []
    for s, cc in enumerate((nx, ny, dg)):
        cp = _rcopy(xp.at[pl.ds(pl.multiple_of(cc * q, q), q)], xr.at[c], xs.at[s], xrs.at[s], _dev(cc, r))
        cp.start()
        xcopies.append(cp)
    x1.start()
    y0.start()
    xr[c, :, :] = xp[pl.ds(pl.multiple_of(c * q, q), q), :]

    def spread(chip, first, groups):
        @pl.loop(0, n // 16)
        def _(ib):
            for g in range(first, first + groups):
                tile = tg[chip, pl.ds(pl.multiple_of(r * n + ib * 16, 16), 16), g * 384:(g + 1) * 384].astype(F32)
                for e in range(4):
                    slab = tile[:, e * VIRT:(e + 1) * VIRT]
                    slab = jnp.concatenate([slab, jnp.zeros((16, LANE - VIRT), F32)], axis=1)
                    for half in range(2):
                        start = (ib * 16 + half * 8) * PITCH + chip * 24 + g * 4 + e
                        t4[pl.ds(start, 8, stride=PITCH), :] = slab[half * 8:half * 8 + 8]

    spread(c, 0, 6)

    loads[3].wait()
    loads[4].wait()
    zrow = jnp.zeros((LANE - VIRT, 4 * LANE), BF16)

    @pl.loop(0, OCC)
    def _(k):
        blk = wd[pl.ds(pl.multiple_of(k * VIRT, 16), VIRT), :].astype(F32)
        parts = []
        for j in range(4):
            parts += [blk[:, j * VIRT:(j + 1) * VIRT], jnp.zeros((VIRT, LANE - VIRT), F32)]
        wd4[pl.ds(pl.multiple_of(k * LANE, LANE), VIRT), :] = jnp.concatenate(parts, axis=1).astype(BF16)
        wd4[pl.ds(pl.multiple_of(k * LANE + VIRT, 32), LANE - VIRT), :] = zrow

    for b in range(3):
        wxt[b * LANE:(b + 1) * LANE, :] = wx[:, b * LANE:(b + 1) * LANE].T

    for cp in xcopies:
        cp.wait_recv()
    xsum = (xr[0] + xr[1]) + (xr[2] + xr[3])
    krows = pl.ds(pl.multiple_of(r * n + c * q, q), q)
    mfull[krows, :] = (oooo[krows, :].astype(F32) + 0.5 * xsum).astype(BF16)
    mcopies = []
    for s, (cc, rr) in enumerate(((nx, r), (ny, r), (dg, r), (c, o), (nx, o), (ny, o), (dg, o))):
        cp = _rcopy(mfull.at[krows], mfull.at[krows], ms.at[s], mrs.at[s], _dev(cc, rr))
        cp.start()
        mcopies.append(cp)

    x0.wait_recv()
    f0 = tcopy(nx, h0, 5, _dev(ny, r))
    f0.start()
    y1.wait_recv()
    f1 = tcopy(ny, h1, 6, _dev(nx, r))
    f1.start()
    spread(nx, 0, 3)
    spread(ny, 3, 3)
    x1.wait_recv()
    d_x = tcopy(nx, whole, 7, _dev(c, o))
    d_x.start()
    y0.wait_recv()
    d_y = tcopy(ny, whole, 8, _dev(c, o))
    d_y.start()
    spread(nx, 3, 3)
    spread(ny, 0, 3)

    for cp in mcopies:
        cp.wait_recv()
    m_mine = mfull[:, rows]

    @pl.loop(0, w // STEP)
    def _(s):
        lanes = pl.ds(pl.multiple_of(s * STEP, STEP), STEP)
        hole[:, lanes] = lax.dot_general(m_mine, tg[c, :, lanes], TN, preferred_element_type=F32)

    f0.wait_recv()
    f1.wait_recv()
    d_d = tcopy(dg, whole, 9, _dev(c, o))
    d_d.start()
    spread(dg, 0, 6)

    @pl.loop(0, OCC // 2)
    def _(k2):
        halves = []
        for e in range(2):
            halves.append(jnp.concatenate(
                [t4[pl.ds(pl.multiple_of((i * OCC + 2 * k2 + e) * PITCH, 8), VIRT), :] for i in range(8)], axis=0))
        lhs = jnp.concatenate(halves, axis=1).astype(BF16)
        prod = jnp.dot(lhs, wd4[pl.ds(pl.multiple_of(k2 * 256, 256), 256), :], preferred_element_type=F32)

        @pl.when(k2 == 0)
        def _():
            ubuf[...] = prod

        @pl.when(k2 > 0)
        def _():
            ubuf[...] += prod

    @pl.loop(0, 4)
    def _(i2):
        halves = []
        for e in range(2):
            halves.append(jnp.concatenate(
                [t4[pl.ds(pl.multiple_of(((2 * i2 + e) * OCC + k) * PITCH, 8), VIRT), :] for k in range(OCC)], axis=0))
        rhs = jnp.concatenate(halves, axis=1).astype(BF16)
        vbuf_s[i2, :, :] = jnp.dot(wxt[...], rhs, preferred_element_type=F32)

    own = c // 2
    half = c % 2

    def put(src, chip, dst):
        for g in range(6):
            vals = [src[pl.ds(chip * 24 + g * 4 + e, 8, stride=PITCH), :][:, :VIRT] for e in range(4)]
            dst[:, g * 384:(g + 1) * 384] = jnp.concatenate(vals, axis=1)

    dests = (dg, nx, ny)

    def scopy(j, s):
        return _rcopy(smsg.at[s, j], srecv.at[c, j], ss.at[s, j], srs.at[c, j], _dev(dests[s], r))

    def pcopy(j, s):
        chip = (dg, nx, ny, c)[s]
        return _rcopy(pmsg.at[s, j], precv.at[half, r, j], ps.at[s, j], prs.at[half, r, j], _dev(chip, own))

    @pl.loop(0, 4)
    def _(j):
        for i in range(8):
            blk = (ubuf[i * VIRT:(i + 1) * VIRT, pl.ds(pl.multiple_of(j * LANE, LANE), LANE)]
                   - vbuf_s[i // 2, pl.ds(pl.multiple_of(j * VIRT, 8), VIRT), (i % 2) * LANE:(i % 2 + 1) * LANE])
            s4[i * PITCH:i * PITCH + VIRT, :] = blk
            st4[i * PITCH:i * PITCH + VIRT, :VIRT] = blk.T[:VIRT, :]
        for s in range(3):
            put(s4, dests[s], smsg.at[s, j])
            scopy(j, s).start()
            put(st4, dests[s], pmsg.at[s, j])
            pcopy(j, s).start()
        put(s4, c, srecv.at[c, j])

        @pl.when(own == r)
        def _():
            put(st4, c, precv.at[half, r, j])

        @pl.when(own != r)
        def _():
            put(st4, c, pmsg.at[3, j])
            pcopy(j, 3).start()

    d_x.wait_recv()
    d_y.wait_recv()
    d_d.wait_recv()

    def ladder_copy(s):
        lanes = pl.ds(pl.multiple_of(s * STEP, STEP), STEP)
        return _rcopy(part.at[s], theirs.at[:, lanes], rs.at[s], rrs.at[s], _dev(c, o))

    @pl.loop(0, w // STEP)
    def _(s):
        slot = s % 3

        @pl.when(s + 2 < w // STEP)
        def _():
            vcopy(s + 2, (s + 2) % 3).start()

        vcopy(s, slot).wait()
        lanes = pl.ds(pl.multiple_of(s * STEP, STEP), STEP)
        va, vb = vv.at[slot, pl.ds(0, w)], vv.at[slot, pl.ds(w, w)]
        part[s, :, :] = (jnp.dot(tg[2 * r, orows, :], va[...], preferred_element_type=F32)
                         + jnp.dot(tg[2 * r + 1, orows, :], vb[...], preferred_element_type=F32))
        ladder_copy(s).start()
        mine[:, lanes] = (jnp.dot(tg[2 * r, rows, :], va[...], preferred_element_type=F32)
                          + jnp.dot(tg[2 * r + 1, rows, :], vb[...], preferred_element_type=F32))

    @pl.loop(0, w // STEP)
    def _(s):
        ladder_copy(s).wait()

    for cp in (d_own, x0, y1, x1, y0, f0, f1, d_x, d_y, d_d, *xcopies, *mcopies):
        cp.wait_send()

    @pl.loop(0, 8)
    def _(i):
        line = pl.ds(pl.multiple_of(i * 16, 16), 16)
        out_ref[line, :] = oovv[line, :].astype(F32) + (mine[line, :] + theirs[line, :] + hole[line, :])

    for s in range(3):
        @pl.loop(0, 4)
        def _(j):
            scopy(j, s).wait_send()
            pcopy(j, s).wait_send()

    @pl.when(own != r)
    def _():
        @pl.loop(0, 4)
        def _(j):
            pcopy(j, 3).wait_send()

    def landed(dst, sem):
        return pltpu.make_async_copy(dst, dst, sem)

    for a, chip in enumerate((nx, ny, dg)):
        @pl.loop(0, 4)
        def _(j):
            landed(srecv.at[chip, j], srs.at[chip, j]).wait()

    for a in range(2):
        for b in range(2):
            here = jnp.logical_and(c == 2 * r + a, r == b)

            @pl.when(jnp.logical_not(here))
            def _():
                @pl.loop(0, 4)
                def _(j):
                    landed(precv.at[a, b, j], prs.at[a, b, j]).wait()

    @pl.loop(0, 8)
    def _(i):
        for jh in range(2):
            line = pl.ds(pl.multiple_of(i * 16 + jh * 8, 8), 8)
            sv = jnp.concatenate([srecv.at[2 * jh + e // 4, e % 4][pl.ds(i, 1), :] for e in range(8)], axis=0)
            out_ref[line, :] = out_ref[line, :] + (sv + precv[i // 4, jh, i % 4])


ANY = pl.BlockSpec(memory_space=pl.ANY)
DMA = pltpu.SemaphoreType.DMA


def sweep(t, oovv, vvvv, oooo, wd, wx):
    n, w = t.shape
    depth = vvvv.shape[0]
    V = pltpu.VMEM
    return pl.pallas_call(
        sweep_kernel,
        out_shape=jax.ShapeDtypeStruct((n, w), F32),
        in_specs=[ANY] * 6,
        out_specs=pl.BlockSpec(memory_space=pltpu.VMEM),
        scratch_shapes=[
            V((n, w), F32), V((n, w), BF16), V(oooo.shape, BF16), V(wd.shape, BF16), V(wx.shape, BF16),
            V((4, 2 * n, w), BF16),
            V((n, 2 * n), F32), V((4, n // 4, 2 * n), F32), V((2 * n, 2 * n), BF16), V((n, w), F32),
            V((n * PITCH, LANE), F32), V((OCC * LANE, 4 * LANE), BF16), V((wx.shape[1], wx.shape[0]), BF16),
            V((8 * VIRT, 4 * LANE), F32), V((4, 4 * VIRT, 2 * LANE), F32),
            V((8 * PITCH, LANE), F32), V((8 * PITCH, LANE), F32),
            V((3, 4, 8, w), F32), V((4, 4, 8, w), F32), V((4, 4, 8, w), F32), V((2, 2, 4, 8, w), F32),
            V((3, depth, STEP), BF16), V((8, LANE), BF16), V((n, w), F32), V((n, w), F32), V((w // STEP, n, STEP), F32),
            DMA((5,)), DMA((10,)), DMA((10,)), DMA((3,)), DMA((3,)), DMA((7,)), DMA((7,)),
            DMA((3, 4)), DMA((4, 4)), DMA((4, 4)), DMA((2, 2, 4)), DMA((3,)), DMA((w // STEP,)), DMA((w // STEP,)),
        ],
        compiler_params=pltpu.CompilerParams(collective_id=0, has_side_effects=True, vmem_limit_bytes=60 << 20),
        name="sweep",
    )(t, oovv, vvvv, oooo, wd, wx)


def solution(mesh):
    def local_sweep(t_blk, d_blk, oovv_blk, vvvv_blk, oooo_full, wd_blk, wx_blk):
        return sweep(t_blk, oovv_blk, vvvv_blk, oooo_full, wd_blk, wx_blk) / d_blk

    amp = P("row", "col")
    wide = P(None, "col")
    return jax.shard_map(local_sweep, mesh=mesh, in_specs=(amp, amp, amp, amp, P(), wide, wide), out_specs=amp, check_vma=False)
```

```python
import jax
import jax.numpy as jnp
from jax import lax
from jax.experimental import pallas as pl
from jax.experimental.pallas import tpu as pltpu
from jax.sharding import PartitionSpec as P

MESH = pl.DeviceIdType.MESH
F32 = jnp.float32
BF16 = jnp.bfloat16
NT = (((1,), (1,)), ((), ()))
TN = (((0,), (0,)), ((), ()))

OCC = 16
VIRT = 96
LANE = 128
PITCH = 104
STEP = 256


def _dev(c, r):
    return {"col": c, "row": r}


def _rcopy(src, dst, ssem, rsem, dev):
    return pltpu.make_async_remote_copy(src, dst, ssem, rsem, device_id=dev, device_id_type=MESH)


def sweep_kernel(t_hbm, oovv_hbm, v_hbm, oooo_hbm, wd_hbm, wx_hbm, out_ref,
                 t32, oovv, oooo, wd, wx, tg, xp, xr, mfull, hole, t4, wd4, wxt, ubuf, vbuf_s, s4, st4,
                 smsg, pmsg, srecv, precv, vv, theirs, part, wxf,
                 lsem, gs, gr, xs, xrs, ms, mrs, ss, srs, ps, prs, vsem, rs, rrs):
    r, c = lax.axis_index("row"), lax.axis_index("col")
    x, y = c % 2, c // 2
    o = 1 - r
    nx, ny, dg = y * 2 + (1 - x), (1 - y) * 2 + x, (1 - y) * 2 + (1 - x)
    n, w = t32.shape
    h = w // 2
    h0, h1 = pl.ds(0, h), pl.ds(h, h)
    rows = pl.ds(pl.multiple_of(r * n, n), n)
    orows = pl.ds(pl.multiple_of(o * n, n), n)

    sem = pltpu.get_barrier_semaphore()
    for cc, rr in ((nx, r), (ny, r), (dg, r), (c, o), (nx, o), (ny, o), (dg, o)):
        pl.semaphore_signal(sem, inc=1, device_id=_dev(cc, rr), device_id_type=MESH)
    loads = [pltpu.make_async_copy(a, b, lsem.at[k]) for k, (a, b) in enumerate(
        ((t_hbm, t32), (oovv_hbm, oovv), (oooo_hbm, oooo), (wd_hbm, wd), (wx_hbm, wx)))]
    for cp in loads:
        cp.start()

    def vcopy(s, slot):
        lanes = pl.ds(pl.multiple_of(s * STEP, STEP), STEP)
        return pltpu.make_async_copy(v_hbm.at[:, lanes], vv.at[slot], vsem.at[slot])

    loads[0].wait()
    tg[c, rows, :] = t32[...].astype(BF16)

    pl.semaphore_wait(sem, 7)

    def tcopy(chip, lanes, k, dev):
        ref = tg.at[chip, rows, lanes]
        return _rcopy(ref, ref, gs.at[k], gr.at[k], dev)

    whole = pl.ds(0, w)
    x0 = tcopy(c, h0, 1, _dev(nx, r))
    y1 = tcopy(c, h1, 2, _dev(ny, r))
    d_own = tcopy(c, whole, 0, _dev(c, o))
    x1 = tcopy(c, h1, 3, _dev(nx, r))
    y0 = tcopy(c, h0, 4, _dev(ny, r))
    x0.start()
    y1.start()
    d_own.start()
    x1.start()
    y0.start()
    vcopy(0, 0).start()
    vcopy(1, 1).start()

    def spread(chip, first, groups):
        @pl.loop(0, n // 16)
        def _(ib):
            for g in range(first, first + groups):
                tile = tg[chip, pl.ds(pl.multiple_of(r * n + ib * 16, 16), 16), g * 384:(g + 1) * 384].astype(F32)
                for e in range(4):
                    slab = tile[:, e * VIRT:(e + 1) * VIRT]
                    slab = jnp.concatenate([slab, jnp.zeros((16, LANE - VIRT), F32)], axis=1)
                    for half in range(2):
                        start = (ib * 16 + half * 8) * PITCH + chip * 24 + g * 4 + e
                        t4[pl.ds(start, 8, stride=PITCH), :] = slab[half * 8:half * 8 + 8]

    spread(c, 0, 6)

    loads[3].wait()
    loads[4].wait()
    zrow = jnp.zeros((LANE - VIRT, 4 * LANE), BF16)

    @pl.loop(0, OCC)
    def _(k):
        blk = wd[pl.ds(pl.multiple_of(k * VIRT, 16), VIRT), :].astype(F32)
        parts = []
        for j in range(4):
            parts += [blk[:, j * VIRT:(j + 1) * VIRT], jnp.zeros((VIRT, LANE - VIRT), F32)]
        wd4[pl.ds(pl.multiple_of(k * LANE, LANE), VIRT), :] = jnp.concatenate(parts, axis=1).astype(BF16)
        wd4[pl.ds(pl.multiple_of(k * LANE + VIRT, 32), LANE - VIRT), :] = zrow
        wxf[pl.ds(pl.multiple_of(k * VIRT, 16), VIRT), :] = wx[pl.ds(pl.multiple_of(k * VIRT, 16), VIRT), :].astype(F32)

    for s, chip in enumerate((c, nx, ny, dg)):
        for b in range(3):
            blk = jnp.concatenate(
                [wxf[pl.ds(pl.multiple_of(k * VIRT + chip * 24, 8), 24), b * LANE:(b + 1) * LANE] for k in range(OCC)],
                axis=0)
            wxt[b * LANE:(b + 1) * LANE, s * 384:(s + 1) * 384] = blk.astype(BF16).T

    loads[1].wait()
    loads[2].wait()
    d_own.wait_recv()
    xp[...] = lax.dot_general(oovv[...], tg[c], NT, preferred_element_type=F32)

    def direct(chip):
        lhs = jnp.concatenate(
            [jnp.concatenate(
                [t4[pl.ds(pl.multiple_of((i * OCC + k) * PITCH + chip * 24, 8), 24), :] for i in range(8)], axis=0)
             for k in range(OCC)], axis=1).astype(BF16)
        ubuf[chip, :, :] = jnp.dot(lhs, wd4[...], preferred_element_type=F32)

    def exchange(chips, first):
        @pl.loop(0, 4)
        def _(i2):
            halves = []
            for e in range(2):
                halves.append(jnp.concatenate(
                    [t4[pl.ds(pl.multiple_of(((2 * i2 + e) * OCC + k) * PITCH + chip * 24, 8), 24), :]
                     for chip in chips for k in range(OCC)], axis=0))
            rhs = jnp.concatenate(halves, axis=1).astype(BF16)
            prod = jnp.dot(wxt[:, first * 384:(first + len(chips)) * 384], rhs, preferred_element_type=F32)
            vbuf_s[i2, :, :] = prod if first == 0 else vbuf_s[i2, :, :] + prod

    direct(c)

    x0.wait_recv()
    f0 = tcopy(nx, h0, 5, _dev(ny, r))
    f0.start()
    y1.wait_recv()
    f1 = tcopy(ny, h1, 6, _dev(nx, r))
    f1.start()
    q = n // 4
    xcopies = []
    for s, cc in enumerate((nx, ny, dg)):
        cp = _rcopy(xp.at[pl.ds(pl.multiple_of(cc * q, q), q)], xr.at[c], xs.at[s], xrs.at[s], _dev(cc, r))
        cp.start()
        xcopies.append(cp)
    xr[c, :, :] = xp[pl.ds(pl.multiple_of(c * q, q), q), :]
    spread(nx, 0, 3)
    spread(ny, 3, 3)
    x1.wait_recv()
    d_x = tcopy(nx, whole, 7, _dev(c, o))
    d_x.start()
    y0.wait_recv()
    d_y = tcopy(ny, whole, 8, _dev(c, o))
    d_y.start()
    spread(nx, 3, 3)
    spread(ny, 0, 3)
    direct(nx)
    direct(ny)
    exchange((c, nx, ny), 0)

    f0.wait_recv()
    f1.wait_recv()
    d_d = tcopy(dg, whole, 9, _dev(c, o))
    d_d.start()
    spread(dg, 0, 6)
    direct(dg)
    exchange((dg,), 3)

    own = c // 2
    half = c % 2

    def put(src, chip, dst):
        for g in range(6):
            vals = [src[pl.ds(chip * 24 + g * 4 + e, 8, stride=PITCH), :][:, :VIRT] for e in range(4)]
            dst[:, g * 384:(g + 1) * 384] = jnp.concatenate(vals, axis=1)

    dests = (dg, nx, ny)

    def scopy(j, s):
        return _rcopy(smsg.at[s, j], srecv.at[c, j], ss.at[s, j], srs.at[c, j], _dev(dests[s], r))

    def pcopy(j, s):
        chip = (dg, nx, ny, c)[s]
        return _rcopy(pmsg.at[s, j], precv.at[half, r, j], ps.at[s, j], prs.at[half, r, j], _dev(chip, own))

    @pl.loop(0, 4)
    def _(j):
        for i in range(8):
            blk = jnp.concatenate(
                [ubuf[chip, i * 24:(i + 1) * 24, pl.ds(pl.multiple_of(j * LANE, LANE), LANE)] for chip in range(4)],
                axis=0)
            s4[i * PITCH:i * PITCH + VIRT, :] = blk - vbuf_s[
                i // 2, pl.ds(pl.multiple_of(j * VIRT, 8), VIRT), (i % 2) * LANE:(i % 2 + 1) * LANE]
        for s in range(3):
            put(s4, dests[s], smsg.at[s, j])
            scopy(j, s).start()
        for i in range(8):
            st4[i * PITCH:i * PITCH + VIRT, :VIRT] = s4[i * PITCH:i * PITCH + VIRT, :].T[:VIRT, :]
        for s in range(3):
            put(st4, dests[s], pmsg.at[s, j])
            pcopy(j, s).start()
        put(s4, c, srecv.at[c, j])

        @pl.when(own == r)
        def _():
            put(st4, c, precv.at[half, r, j])

        @pl.when(own != r)
        def _():
            put(st4, c, pmsg.at[3, j])
            pcopy(j, 3).start()

    for cp in xcopies:
        cp.wait_recv()
    xsum = (xr[0] + xr[1]) + (xr[2] + xr[3])
    krows = pl.ds(pl.multiple_of(r * n + c * q, q), q)
    mfull[krows, :] = (oooo[krows, :].astype(F32) + 0.5 * xsum).astype(BF16)
    mcopies = []
    for s, (cc, rr) in enumerate(((nx, r), (ny, r), (dg, r), (c, o), (nx, o), (ny, o), (dg, o))):
        part_m = mfull.at[krows, pl.ds(pl.multiple_of(rr * n, n), n)]
        cp = _rcopy(part_m, part_m, ms.at[s], mrs.at[s], _dev(cc, rr))
        cp.start()
        mcopies.append(cp)

    d_x.wait_recv()
    d_y.wait_recv()
    d_d.wait_recv()

    def ladder_copy(s):
        lanes = pl.ds(pl.multiple_of(s * STEP, STEP), STEP)
        return _rcopy(part.at[s, orows], theirs.at[:, lanes], rs.at[s], rrs.at[s], _dev(c, o))

    @pl.loop(0, w // STEP)
    def _(s):
        slot = s % 3

        @pl.when(s + 2 < w // STEP)
        def _():
            vcopy(s + 2, (s + 2) % 3).start()

        vcopy(s, slot).wait()
        va, vb = vv.at[slot, pl.ds(0, w)], vv.at[slot, pl.ds(w, w)]
        part[s, :, :] = (jnp.dot(tg[2 * r], va[...], preferred_element_type=F32)
                         + jnp.dot(tg[2 * r + 1], vb[...], preferred_element_type=F32))
        ladder_copy(s).start()

    @pl.loop(0, w // STEP)
    def _(s):
        ladder_copy(s).wait()

    for cp in (d_own, x0, y1, x1, y0, f0, f1, d_x, d_y, d_d, *xcopies, *mcopies):
        cp.wait_send()

    for cp in mcopies:
        cp.wait_recv()
    m_mine = mfull[:, rows]

    @pl.loop(0, w // STEP)
    def _(s):
        lanes = pl.ds(pl.multiple_of(s * STEP, STEP), STEP)
        hole[:, lanes] = lax.dot_general(m_mine, tg[c, :, lanes], TN, preferred_element_type=F32)

    @pl.loop(0, 8)
    def _(i):
        line = pl.ds(pl.multiple_of(i * 16, 16), 16)
        line_r = pl.ds(pl.multiple_of(r * n + i * 16, 16), 16)
        mine = jnp.concatenate([part[s, line_r, :] for s in range(w // STEP)], axis=1)
        out_ref[line, :] = oovv[line, :].astype(F32) + (mine + theirs[line, :] + hole[line, :])

    for s in range(3):
        @pl.loop(0, 4)
        def _(j):
            scopy(j, s).wait_send()
            pcopy(j, s).wait_send()

    @pl.when(own != r)
    def _():
        @pl.loop(0, 4)
        def _(j):
            pcopy(j, 3).wait_send()

    def landed(dst, sem):
        return pltpu.make_async_copy(dst, dst, sem)

    for a, chip in enumerate((nx, ny, dg)):
        @pl.loop(0, 4)
        def _(j):
            landed(srecv.at[chip, j], srs.at[chip, j]).wait()

    for a in range(2):
        for b in range(2):
            here = jnp.logical_and(c == 2 * r + a, r == b)

            @pl.when(jnp.logical_not(here))
            def _():
                @pl.loop(0, 4)
                def _(j):
                    landed(precv.at[a, b, j], prs.at[a, b, j]).wait()

    @pl.loop(0, 8)
    def _(i):
        for jh in range(2):
            line = pl.ds(pl.multiple_of(i * 16 + jh * 8, 8), 8)
            sv = jnp.concatenate([srecv.at[2 * jh + e // 4, e % 4][pl.ds(i, 1), :] for e in range(8)], axis=0)
            out_ref[line, :] = out_ref[line, :] + (sv + precv[i // 4, jh, i % 4])


ANY = pl.BlockSpec(memory_space=pl.ANY)
DMA = pltpu.SemaphoreType.DMA


def sweep(t, oovv, vvvv, oooo, wd, wx):
    n, w = t.shape
    depth = vvvv.shape[0]
    V = pltpu.VMEM
    return pl.pallas_call(
        sweep_kernel,
        out_shape=jax.ShapeDtypeStruct((n, w), F32),
        in_specs=[ANY] * 6,
        out_specs=pl.BlockSpec(memory_space=pltpu.VMEM),
        scratch_shapes=[
            V((n, w), F32), V((n, w), BF16), V(oooo.shape, BF16), V(wd.shape, BF16), V(wx.shape, BF16),
            V((4, 2 * n, w), BF16),
            V((n, 2 * n), F32), V((4, n // 4, 2 * n), F32), V((2 * n, 2 * n), BF16), V((n, w), F32),
            V((n * PITCH, LANE), F32), V((OCC * LANE, 4 * LANE), BF16), V((wx.shape[1], wx.shape[0]), BF16),
            V((4, 2 * VIRT, 4 * LANE), F32), V((4, 4 * VIRT, 2 * LANE), F32),
            V((8 * PITCH, LANE), F32), V((8 * PITCH, LANE), F32),
            V((3, 4, 8, w), F32), V((4, 4, 8, w), F32), V((4, 4, 8, w), F32), V((2, 2, 4, 8, w), F32),
            V((3, depth, STEP), BF16), V((n, w), F32), V((w // STEP, 2 * n, STEP), F32), V(wx.shape, F32),
            DMA((5,)), DMA((10,)), DMA((10,)), DMA((3,)), DMA((3,)), DMA((7,)), DMA((7,)),
            DMA((3, 4)), DMA((4, 4)), DMA((4, 4)), DMA((2, 2, 4)), DMA((3,)), DMA((w // STEP,)), DMA((w // STEP,)),
        ],
        compiler_params=pltpu.CompilerParams(collective_id=0, has_side_effects=True, vmem_limit_bytes=60 << 20),
        name="sweep",
    )(t, oovv, vvvv, oooo, wd, wx)


def solution(mesh):
    def local_sweep(t_blk, d_blk, oovv_blk, vvvv_blk, oooo_full, wd_blk, wx_blk):
        return sweep(t_blk, oovv_blk, vvvv_blk, oooo_full, wd_blk, wx_blk) / d_blk

    amp = P("row", "col")
    wide = P(None, "col")
    return jax.shard_map(local_sweep, mesh=mesh, in_specs=(amp, amp, amp, amp, P(), wide, wide), out_specs=amp, check_vma=False)
```

```python
import jax
import jax.numpy as jnp
from jax import lax
from jax.experimental import pallas as pl
from jax.experimental.pallas import tpu as pltpu
from jax.sharding import PartitionSpec as P

MESH = pl.DeviceIdType.MESH
F32 = jnp.float32
BF16 = jnp.bfloat16
NT = (((1,), (1,)), ((), ()))
TN = (((0,), (0,)), ((), ()))

OCC = 16
VIRT = 96
LANE = 128
PITCH = 104
STEP = 256


def _dev(c, r):
    return {"col": c, "row": r}


def _rcopy(src, dst, ssem, rsem, dev):
    return pltpu.make_async_remote_copy(src, dst, ssem, rsem, device_id=dev, device_id_type=MESH)


def sweep_kernel(t_hbm, oovv_hbm, v_hbm, oooo_hbm, wd_hbm, wx_hbm, out_ref,
                 t32, oovv, oooo, wd, wx, tg, xp, xr, mfull, hole, t4, wd4, wxt, ubuf, vbuf_s, s4, st4,
                 smsg, pmsg, srecv, precv, vv, theirs, part, wxf,
                 lsem, gs, gr, fs, fr, xs, xrs, ms, mrs, ss, srs, ps, prs, vsem, rs, rrs):
    r, c = lax.axis_index("row"), lax.axis_index("col")
    x, y = c % 2, c // 2
    o = 1 - r
    nx, ny, dg = y * 2 + (1 - x), (1 - y) * 2 + x, (1 - y) * 2 + (1 - x)
    n, w = t32.shape
    h = w // 2
    h0, h1 = pl.ds(0, h), pl.ds(h, h)
    rows = pl.ds(pl.multiple_of(r * n, n), n)
    orows = pl.ds(pl.multiple_of(o * n, n), n)

    sem = pltpu.get_barrier_semaphore()
    for cc, rr in ((nx, r), (ny, r), (dg, r), (c, o), (nx, o), (ny, o), (dg, o)):
        pl.semaphore_signal(sem, inc=1, device_id=_dev(cc, rr), device_id_type=MESH)
    loads = [pltpu.make_async_copy(a, b, lsem.at[k]) for k, (a, b) in enumerate(
        ((t_hbm, t32), (oovv_hbm, oovv), (oooo_hbm, oooo), (wd_hbm, wd), (wx_hbm, wx)))]
    for cp in loads:
        cp.start()

    def vcopy(s, slot):
        lanes = pl.ds(pl.multiple_of(s * STEP, STEP), STEP)
        return pltpu.make_async_copy(v_hbm.at[:, lanes], vv.at[slot], vsem.at[slot])

    loads[0].wait()
    tg[c, rows, :] = t32[...].astype(BF16)

    pl.semaphore_wait(sem, 7)

    def tcopy(chip, lanes, k, dev):
        ref = tg.at[chip, rows, lanes]
        return _rcopy(ref, ref, gs.at[k], gr.at[k], dev)

    def fcopy(chip, lanes, k, p, dev):
        ref = tg.at[chip, pl.ds(pl.multiple_of(r * n + p * 32, 32), 32), lanes]
        return _rcopy(ref, ref, fs.at[k, p], fr.at[k, p], dev)

    whole = pl.ds(0, w)
    x0 = tcopy(c, h0, 1, _dev(nx, r))
    y1 = tcopy(c, h1, 2, _dev(ny, r))
    d_own = tcopy(c, whole, 0, _dev(c, o))
    x1 = tcopy(c, h1, 3, _dev(nx, r))
    y0 = tcopy(c, h0, 4, _dev(ny, r))
    x0.start()
    y1.start()
    d_own.start()
    x1.start()
    y0.start()
    vcopy(0, 0).start()
    vcopy(1, 1).start()

    def spread_rows(chip, ib, first, groups):
        for g in range(first, first + groups):
            tile = tg[chip, pl.ds(pl.multiple_of(r * n + ib * 16, 16), 16), g * 384:(g + 1) * 384].astype(F32)
            for e in range(4):
                slab = tile[:, e * VIRT:(e + 1) * VIRT]
                slab = jnp.concatenate([slab, jnp.zeros((16, LANE - VIRT), F32)], axis=1)
                for half in range(2):
                    start = (ib * 16 + half * 8) * PITCH + chip * 24 + g * 4 + e
                    t4[pl.ds(start, 8, stride=PITCH), :] = slab[half * 8:half * 8 + 8]

    def spread(chip, first, groups):
        @pl.loop(0, n // 16)
        def _(ib):
            spread_rows(chip, ib, first, groups)

    spread(c, 0, 6)

    loads[3].wait()
    loads[4].wait()
    zrow = jnp.zeros((LANE - VIRT, 4 * LANE), BF16)

    @pl.loop(0, OCC)
    def _(k):
        blk = wd[pl.ds(pl.multiple_of(k * VIRT, 16), VIRT), :].astype(F32)
        parts = []
        for j in range(4):
            parts += [blk[:, j * VIRT:(j + 1) * VIRT], jnp.zeros((VIRT, LANE - VIRT), F32)]
        wd4[pl.ds(pl.multiple_of(k * LANE, LANE), VIRT), :] = jnp.concatenate(parts, axis=1).astype(BF16)
        wd4[pl.ds(pl.multiple_of(k * LANE + VIRT, 32), LANE - VIRT), :] = zrow
        wxf[pl.ds(pl.multiple_of(k * VIRT, 16), VIRT), :] = wx[pl.ds(pl.multiple_of(k * VIRT, 16), VIRT), :].astype(F32)

    for s, chip in enumerate((c, nx, ny, dg)):
        for b in range(3):
            blk = jnp.concatenate(
                [wxf[pl.ds(pl.multiple_of(k * VIRT + chip * 24, 8), 24), b * LANE:(b + 1) * LANE] for k in range(OCC)],
                axis=0)
            wxt[b * LANE:(b + 1) * LANE, s * 384:(s + 1) * 384] = blk.astype(BF16).T

    loads[1].wait()
    loads[2].wait()
    d_own.wait_recv()
    xp[...] = lax.dot_general(oovv[...], tg[c], NT, preferred_element_type=F32)

    def direct_rows(chip, i0, count):
        lhs = jnp.concatenate(
            [jnp.concatenate(
                [t4[pl.ds(pl.multiple_of(((i0 + i) * OCC + k) * PITCH + chip * 24, 8), 24), :] for i in range(count)],
                axis=0)
             for k in range(OCC)], axis=1).astype(BF16)
        return jnp.dot(lhs, wd4[...], preferred_element_type=F32)

    def direct(chip):
        ubuf[chip, :, :] = direct_rows(chip, 0, 8)

    def exchange_pair(chips, first, i2):
        halves = []
        for e in range(2):
            halves.append(jnp.concatenate(
                [t4[pl.ds(pl.multiple_of(((2 * i2 + e) * OCC + k) * PITCH + chip * 24, 8), 24), :]
                 for chip in chips for k in range(OCC)], axis=0))
        rhs = jnp.concatenate(halves, axis=1).astype(BF16)
        prod = jnp.dot(wxt[:, first * 384:(first + len(chips)) * 384], rhs, preferred_element_type=F32)
        vbuf_s[i2, :, :] = prod if first == 0 else vbuf_s[i2, :, :] + prod

    def exchange(chips, first):
        @pl.loop(0, 4)
        def _(i2):
            exchange_pair(chips, first, i2)

    direct(c)

    x0.wait_recv()
    for p in range(4):
        fcopy(nx, h0, 0, p, _dev(ny, r)).start()
    y1.wait_recv()
    for p in range(4):
        fcopy(ny, h1, 1, p, _dev(nx, r)).start()
    q = n // 4
    xcopies = []
    for s, cc in enumerate((nx, ny, dg)):
        cp = _rcopy(xp.at[pl.ds(pl.multiple_of(cc * q, q), q)], xr.at[c], xs.at[s], xrs.at[s], _dev(cc, r))
        cp.start()
        xcopies.append(cp)
    xr[c, :, :] = xp[pl.ds(pl.multiple_of(c * q, q), q), :]
    spread(nx, 0, 3)
    spread(ny, 3, 3)
    x1.wait_recv()
    d_x = tcopy(nx, whole, 7, _dev(c, o))
    d_x.start()
    y0.wait_recv()
    d_y = tcopy(ny, whole, 8, _dev(c, o))
    d_y.start()
    spread(nx, 3, 3)
    spread(ny, 0, 3)
    direct(nx)
    direct(ny)
    exchange((c, nx, ny), 0)

    @pl.loop(0, 4)
    def _(p):
        fcopy(dg, h0, 0, p, _dev(ny, r)).wait_recv()
        fcopy(dg, h1, 1, p, _dev(nx, r)).wait_recv()
        for ib in range(2):
            spread_rows(dg, 2 * p + ib, 0, 6)
        ubuf[dg, pl.ds(pl.multiple_of(p * 48, 16), 48), :] = direct_rows(dg, 2 * p, 2)
        exchange_pair((dg,), 3, p)

    d_d = tcopy(dg, whole, 9, _dev(c, o))
    d_d.start()

    for cp in xcopies:
        cp.wait_recv()
    xsum = (xr[0] + xr[1]) + (xr[2] + xr[3])
    krows = pl.ds(pl.multiple_of(r * n + c * q, q), q)
    mfull[krows, :] = (oooo[krows, :].astype(F32) + 0.5 * xsum).astype(BF16)
    mcopies = []
    for s, (cc, rr) in enumerate(((nx, r), (ny, r), (dg, r), (c, o), (nx, o), (ny, o), (dg, o))):
        part_m = mfull.at[krows, pl.ds(pl.multiple_of(rr * n, n), n)]
        cp = _rcopy(part_m, part_m, ms.at[s], mrs.at[s], _dev(cc, rr))
        cp.start()
        mcopies.append(cp)

    own = c // 2
    half = c % 2

    def put(src, chip, dst):
        for g in range(6):
            vals = [src[pl.ds(chip * 24 + g * 4 + e, 8, stride=PITCH), :][:, :VIRT] for e in range(4)]
            dst[:, g * 384:(g + 1) * 384] = jnp.concatenate(vals, axis=1)

    dests = (dg, nx, ny)

    def scopy(j, s):
        return _rcopy(smsg.at[s, j], srecv.at[c, j], ss.at[s, j], srs.at[c, j], _dev(dests[s], r))

    def pcopy(j, s):
        chip = (dg, nx, ny, c)[s]
        return _rcopy(pmsg.at[s, j], precv.at[half, r, j], ps.at[s, j], prs.at[half, r, j], _dev(chip, own))

    @pl.loop(0, 4)
    def _(j):
        for i in range(8):
            blk = jnp.concatenate(
                [ubuf[chip, i * 24:(i + 1) * 24, pl.ds(pl.multiple_of(j * LANE, LANE), LANE)] for chip in range(4)],
                axis=0)
            s4[i * PITCH:i * PITCH + VIRT, :] = blk - vbuf_s[
                i // 2, pl.ds(pl.multiple_of(j * VIRT, 8), VIRT), (i % 2) * LANE:(i % 2 + 1) * LANE]
        for s in range(3):
            put(s4, dests[s], smsg.at[s, j])
            scopy(j, s).start()
        for i in range(8):
            st4[i * PITCH:i * PITCH + VIRT, :VIRT] = s4[i * PITCH:i * PITCH + VIRT, :].T[:VIRT, :]
        for s in range(3):
            put(st4, dests[s], pmsg.at[s, j])
            pcopy(j, s).start()
        put(s4, c, srecv.at[c, j])

        @pl.when(own == r)
        def _():
            put(st4, c, precv.at[half, r, j])

        @pl.when(own != r)
        def _():
            put(st4, c, pmsg.at[3, j])
            pcopy(j, 3).start()

    d_x.wait_recv()
    d_y.wait_recv()
    d_d.wait_recv()

    def ladder_copy(s):
        lanes = pl.ds(pl.multiple_of(s * STEP, STEP), STEP)
        return _rcopy(part.at[s, orows], theirs.at[:, lanes], rs.at[s], rrs.at[s], _dev(c, o))

    @pl.loop(0, w // STEP)
    def _(s):
        slot = s % 3

        @pl.when(s + 2 < w // STEP)
        def _():
            vcopy(s + 2, (s + 2) % 3).start()

        vcopy(s, slot).wait()
        va, vb = vv.at[slot, pl.ds(0, w)], vv.at[slot, pl.ds(w, w)]
        part[s, :, :] = (jnp.dot(tg[2 * r], va[...], preferred_element_type=F32)
                         + jnp.dot(tg[2 * r + 1], vb[...], preferred_element_type=F32))
        ladder_copy(s).start()

    @pl.loop(0, w // STEP)
    def _(s):
        ladder_copy(s).wait()

    for cp in (d_own, x0, y1, x1, y0, d_x, d_y, d_d, *xcopies, *mcopies):
        cp.wait_send()
    for p in range(4):
        fcopy(nx, h0, 0, p, _dev(ny, r)).wait_send()
        fcopy(ny, h1, 1, p, _dev(nx, r)).wait_send()

    for cp in mcopies:
        cp.wait_recv()
    m_mine = mfull[:, rows]

    @pl.loop(0, w // STEP)
    def _(s):
        lanes = pl.ds(pl.multiple_of(s * STEP, STEP), STEP)
        hole[:, lanes] = lax.dot_general(m_mine, tg[c, :, lanes], TN, preferred_element_type=F32)

    @pl.loop(0, 8)
    def _(i):
        line = pl.ds(pl.multiple_of(i * 16, 16), 16)
        line_r = pl.ds(pl.multiple_of(r * n + i * 16, 16), 16)
        mine = jnp.concatenate([part[s, line_r, :] for s in range(w // STEP)], axis=1)
        out_ref[line, :] = oovv[line, :].astype(F32) + (mine + theirs[line, :] + hole[line, :])

    for s in range(3):
        @pl.loop(0, 4)
        def _(j):
            scopy(j, s).wait_send()
            pcopy(j, s).wait_send()

    @pl.when(own != r)
    def _():
        @pl.loop(0, 4)
        def _(j):
            pcopy(j, 3).wait_send()

    def landed(dst, sem):
        return pltpu.make_async_copy(dst, dst, sem)

    for a, chip in enumerate((nx, ny, dg)):
        @pl.loop(0, 4)
        def _(j):
            landed(srecv.at[chip, j], srs.at[chip, j]).wait()

    for a in range(2):
        for b in range(2):
            here = jnp.logical_and(c == 2 * r + a, r == b)

            @pl.when(jnp.logical_not(here))
            def _():
                @pl.loop(0, 4)
                def _(j):
                    landed(precv.at[a, b, j], prs.at[a, b, j]).wait()

    @pl.loop(0, 8)
    def _(i):
        for jh in range(2):
            line = pl.ds(pl.multiple_of(i * 16 + jh * 8, 8), 8)
            sv = jnp.concatenate([srecv.at[2 * jh + e // 4, e % 4][pl.ds(i, 1), :] for e in range(8)], axis=0)
            out_ref[line, :] = out_ref[line, :] + (sv + precv[i // 4, jh, i % 4])


ANY = pl.BlockSpec(memory_space=pl.ANY)
DMA = pltpu.SemaphoreType.DMA


def sweep(t, oovv, vvvv, oooo, wd, wx):
    n, w = t.shape
    depth = vvvv.shape[0]
    V = pltpu.VMEM
    return pl.pallas_call(
        sweep_kernel,
        out_shape=jax.ShapeDtypeStruct((n, w), F32),
        in_specs=[ANY] * 6,
        out_specs=pl.BlockSpec(memory_space=pltpu.VMEM),
        scratch_shapes=[
            V((n, w), F32), V((n, w), BF16), V(oooo.shape, BF16), V(wd.shape, BF16), V(wx.shape, BF16),
            V((4, 2 * n, w), BF16),
            V((n, 2 * n), F32), V((4, n // 4, 2 * n), F32), V((2 * n, 2 * n), BF16), V((n, w), F32),
            V((n * PITCH, LANE), F32), V((OCC * LANE, 4 * LANE), BF16), V((wx.shape[1], wx.shape[0]), BF16),
            V((4, 2 * VIRT, 4 * LANE), F32), V((4, 4 * VIRT, 2 * LANE), F32),
            V((8 * PITCH, LANE), F32), V((8 * PITCH, LANE), F32),
            V((3, 4, 8, w), F32), V((4, 4, 8, w), F32), V((4, 4, 8, w), F32), V((2, 2, 4, 8, w), F32),
            V((3, depth, STEP), BF16), V((n, w), F32), V((w // STEP, 2 * n, STEP), F32), V(wx.shape, F32),
            DMA((5,)), DMA((10,)), DMA((10,)), DMA((2, 4)), DMA((2, 4)), DMA((3,)), DMA((3,)), DMA((7,)), DMA((7,)),
            DMA((3, 4)), DMA((4, 4)), DMA((4, 4)), DMA((2, 2, 4)), DMA((3,)), DMA((w // STEP,)), DMA((w // STEP,)),
        ],
        compiler_params=pltpu.CompilerParams(collective_id=0, has_side_effects=True, vmem_limit_bytes=46 << 20),
        name="sweep",
    )(*(pltpu.with_memory_space_constraint(a, pltpu.HBM) for a in (t, oovv, vvvv, oooo, wd, wx)))


def solution(mesh):
    def local_sweep(t_blk, d_blk, oovv_blk, vvvv_blk, oooo_full, wd_blk, wx_blk):
        return sweep(t_blk, oovv_blk, vvvv_blk, oooo_full, wd_blk, wx_blk) / d_blk

    amp = P("row", "col")
    wide = P(None, "col")
    return jax.shard_map(local_sweep, mesh=mesh, in_specs=(amp, amp, amp, amp, P(), wide, wide), out_specs=amp, check_vma=False)
```

```python
import jax
import jax.numpy as jnp
from jax import lax
from jax.experimental import pallas as pl
from jax.experimental.pallas import tpu as pltpu
from jax.sharding import PartitionSpec as P

MESH = pl.DeviceIdType.MESH
F32 = jnp.float32
BF16 = jnp.bfloat16
NT = (((1,), (1,)), ((), ()))
TN = (((0,), (0,)), ((), ()))

OCC = 16
VIRT = 96
LANE = 128
PITCH = 104
STEP = 256


def _dev(c, r):
    return {"col": c, "row": r}


def _rcopy(src, dst, ssem, rsem, dev):
    return pltpu.make_async_remote_copy(src, dst, ssem, rsem, device_id=dev, device_id_type=MESH)


def sweep_kernel(t_hbm, oovv_hbm, v_hbm, oooo_hbm, wd_hbm, wx_hbm, out_ref,
                 t32, oovv, oooo, wd, wx, tg, xp, xr, mfull, hole, t4, wd4, wxt, ubuf, vbuf_s, s4, st4,
                 smsg, pmsg, srecv, phome, pfar, vv, theirs, part, wxf,
                 lsem, gs, gr, fs, fr, xs, xrs, ms, mrs, ss, srs, ps, prs, vsem, rs, rrs):
    r, c = lax.axis_index("row"), lax.axis_index("col")
    x, y = c % 2, c // 2
    o = 1 - r
    nx, ny, dg = y * 2 + (1 - x), (1 - y) * 2 + x, (1 - y) * 2 + (1 - x)
    n, w = t32.shape
    h = w // 2
    h0, h1 = pl.ds(0, h), pl.ds(h, h)
    rows = pl.ds(pl.multiple_of(r * n, n), n)
    orows = pl.ds(pl.multiple_of(o * n, n), n)

    sem = pltpu.get_barrier_semaphore()
    for cc, rr in ((nx, r), (ny, r), (dg, r), (c, o), (nx, o), (ny, o), (dg, o)):
        pl.semaphore_signal(sem, inc=1, device_id=_dev(cc, rr), device_id_type=MESH)
    loads = [pltpu.make_async_copy(a, b, lsem.at[k]) for k, (a, b) in enumerate(
        ((t_hbm, t32), (oovv_hbm, oovv), (oooo_hbm, oooo), (wd_hbm, wd), (wx_hbm, wx)))]
    for cp in loads:
        cp.start()

    def vcopy(s, slot):
        lanes = pl.ds(pl.multiple_of(s * STEP, STEP), STEP)
        return pltpu.make_async_copy(v_hbm.at[:, lanes], vv.at[slot], vsem.at[slot])

    loads[0].wait()
    tg[c, rows, :] = t32[...].astype(BF16)

    pl.semaphore_wait(sem, 7)

    def tcopy(chip, lanes, k, dev):
        ref = tg.at[chip, rows, lanes]
        return _rcopy(ref, ref, gs.at[k], gr.at[k], dev)

    def fcopy(chip, lanes, k, p, dev):
        ref = tg.at[chip, pl.ds(pl.multiple_of(r * n + p * 32, 32), 32), lanes]
        return _rcopy(ref, ref, fs.at[k, p], fr.at[k, p], dev)

    whole = pl.ds(0, w)
    x0 = tcopy(c, h0, 1, _dev(nx, r))
    y1 = tcopy(c, h1, 2, _dev(ny, r))
    d_own = tcopy(c, whole, 0, _dev(c, o))
    x1 = tcopy(c, h1, 3, _dev(nx, r))
    y0 = tcopy(c, h0, 4, _dev(ny, r))
    x0.start()
    y1.start()
    d_own.start()
    x1.start()
    y0.start()
    vcopy(0, 0).start()
    vcopy(1, 1).start()

    def spread_rows(chip, ib, first, groups):
        for g in range(first, first + groups):
            tile = tg[chip, pl.ds(pl.multiple_of(r * n + ib * 16, 16), 16), g * 384:(g + 1) * 384].astype(F32)
            for e in range(4):
                slab = tile[:, e * VIRT:(e + 1) * VIRT]
                slab = jnp.concatenate([slab, jnp.zeros((16, LANE - VIRT), F32)], axis=1)
                for half in range(2):
                    start = (ib * 16 + half * 8) * PITCH + chip * 24 + g * 4 + e
                    t4[pl.ds(start, 8, stride=PITCH), :] = slab[half * 8:half * 8 + 8]

    def spread(chip, first, groups):
        @pl.loop(0, n // 16)
        def _(ib):
            spread_rows(chip, ib, first, groups)

    spread(c, 0, 6)

    loads[3].wait()
    loads[4].wait()
    zrow = jnp.zeros((LANE - VIRT, 4 * LANE), BF16)

    @pl.loop(0, OCC)
    def _(k):
        blk = wd[pl.ds(pl.multiple_of(k * VIRT, 16), VIRT), :].astype(F32)
        parts = []
        for j in range(4):
            parts += [blk[:, j * VIRT:(j + 1) * VIRT], jnp.zeros((VIRT, LANE - VIRT), F32)]
        wd4[pl.ds(pl.multiple_of(k * LANE, LANE), VIRT), :] = jnp.concatenate(parts, axis=1).astype(BF16)
        wd4[pl.ds(pl.multiple_of(k * LANE + VIRT, 32), LANE - VIRT), :] = zrow
        wxf[pl.ds(pl.multiple_of(k * VIRT, 16), VIRT), :] = wx[pl.ds(pl.multiple_of(k * VIRT, 16), VIRT), :].astype(F32)

    for s, chip in enumerate((c, nx, ny, dg)):
        for b in range(3):
            blk = jnp.concatenate(
                [wxf[pl.ds(pl.multiple_of(k * VIRT + chip * 24, 8), 24), b * LANE:(b + 1) * LANE] for k in range(OCC)],
                axis=0)
            wxt[b * LANE:(b + 1) * LANE, s * 384:(s + 1) * 384] = blk.astype(BF16).T

    loads[1].wait()
    loads[2].wait()
    d_own.wait_recv()
    xp[...] = lax.dot_general(oovv[...], tg[c], NT, preferred_element_type=F32)

    def direct_rows(chip, i0, count):
        lhs = jnp.concatenate(
            [jnp.concatenate(
                [t4[pl.ds(pl.multiple_of(((i0 + i) * OCC + k) * PITCH + chip * 24, 8), 24), :] for i in range(count)],
                axis=0)
             for k in range(OCC)], axis=1).astype(BF16)
        return jnp.dot(lhs, wd4[...], preferred_element_type=F32)

    def direct(chip):
        ubuf[chip, :, :] = direct_rows(chip, 0, 8)

    def exchange_pair(chips, first, i2):
        halves = []
        for e in range(2):
            halves.append(jnp.concatenate(
                [t4[pl.ds(pl.multiple_of(((2 * i2 + e) * OCC + k) * PITCH + chip * 24, 8), 24), :]
                 for chip in chips for k in range(OCC)], axis=0))
        rhs = jnp.concatenate(halves, axis=1).astype(BF16)
        prod = jnp.dot(wxt[:, first * 384:(first + len(chips)) * 384], rhs, preferred_element_type=F32)
        vbuf_s[i2, :, :] = prod if first == 0 else vbuf_s[i2, :, :] + prod

    def exchange(chips, first):
        @pl.loop(0, 4)
        def _(i2):
            exchange_pair(chips, first, i2)

    direct(c)

    x0.wait_recv()
    for p in range(4):
        fcopy(nx, h0, 0, p, _dev(ny, r)).start()
    y1.wait_recv()
    for p in range(4):
        fcopy(ny, h1, 1, p, _dev(nx, r)).start()
    q = n // 4
    xcopies = []
    for s, cc in enumerate((nx, ny, dg)):
        cp = _rcopy(xp.at[pl.ds(pl.multiple_of(cc * q, q), q)], xr.at[c], xs.at[s], xrs.at[s], _dev(cc, r))
        cp.start()
        xcopies.append(cp)
    xr[c, :, :] = xp[pl.ds(pl.multiple_of(c * q, q), q), :]
    spread(nx, 0, 3)
    spread(ny, 3, 3)
    x1.wait_recv()
    d_x = tcopy(nx, whole, 7, _dev(c, o))
    d_x.start()
    y0.wait_recv()
    d_y = tcopy(ny, whole, 8, _dev(c, o))
    d_y.start()
    spread(nx, 3, 3)
    spread(ny, 0, 3)
    direct(nx)
    direct(ny)
    exchange((c, nx, ny), 0)

    @pl.loop(0, 4)
    def _(p):
        fcopy(dg, h0, 0, p, _dev(ny, r)).wait_recv()
        fcopy(dg, h1, 1, p, _dev(nx, r)).wait_recv()
        for ib in range(2):
            spread_rows(dg, 2 * p + ib, 0, 6)
        ubuf[dg, pl.ds(pl.multiple_of(p * 48, 16), 48), :] = direct_rows(dg, 2 * p, 2)
        exchange_pair((dg,), 3, p)

    d_d = tcopy(dg, whole, 9, _dev(c, o))
    d_d.start()

    own = c // 2
    half = c % 2

    def put(src, chip, dst, first=0, count=8):
        for g in range(6):
            vals = [src[pl.ds(first * PITCH + chip * 24 + g * 4 + e, count, stride=PITCH), :][:, :VIRT]
                    for e in range(4)]
            dst[:, g * 384:(g + 1) * 384] = jnp.concatenate(vals, axis=1)

    dests = (dg, nx, ny)

    def scopy(j, s):
        return _rcopy(smsg.at[s, j], srecv.at[c, j], ss, srs, _dev(dests[s], r))

    def hcopy(m, s):
        return _rcopy(pmsg.at[s, m], phome.at[half, m], ps, prs.at[0, m], _dev(dests[s], r))

    def pcopy(j, s):
        chip = (dg, nx, ny, c)[s]
        return _rcopy(pmsg.at[s, j], pfar.at[half, j], ps, prs.at[1, j], _dev(chip, o))

    def block(i, j):
        direct_part = jnp.concatenate(
            [ubuf[chip, pl.ds(pl.multiple_of(i * 24, 8), 24), pl.ds(pl.multiple_of(j * LANE, LANE), LANE)]
             for chip in range(4)], axis=0)
        return direct_part - vbuf_s[
            i // 2, pl.ds(pl.multiple_of(j * VIRT, 8), VIRT), pl.ds(pl.multiple_of((i % 2) * LANE, LANE), LANE)]

    def send_s(j):
        for i in range(8):
            s4[i * PITCH:i * PITCH + VIRT, :] = block(i, j)

        @pl.when(own == r)
        def _():
            for e in range(4):
                at = pl.ds(pl.multiple_of((half * 4 + e) * PITCH, 8), VIRT)
                s4[at, :VIRT] = s4[at, :VIRT] + block(half * 4 + j, e).T[:VIRT, :]

        for s in range(3):
            put(s4, dests[s], smsg.at[s, j])
            scopy(j, s).start()
        put(s4, c, srecv.at[c, j])

    def send_p(j):
        @pl.when(own != r)
        def _():
            for i in range(8):
                st4[i * PITCH:i * PITCH + VIRT, :VIRT] = s4[i * PITCH:i * PITCH + VIRT, :].T[:VIRT, :]
            for s in range(3):
                put(st4, dests[s], pmsg.at[s, j])
                pcopy(j, s).start()
            put(st4, c, pmsg.at[3, j])
            pcopy(j, 3).start()

        @pl.when(own == r)
        def _():
            for e in range(4):
                at = pl.ds(pl.multiple_of(((1 - half) * 4 + e) * PITCH, 8), VIRT)
                to = pl.ds(pl.multiple_of(((j % 2) * 4 + e) * PITCH, 8), VIRT)
                st4[to, :VIRT] = s4[at, :].T[:VIRT, :]

            @pl.when(j % 2 == 1)
            def _():
                m = j // 2
                for s in range(3):
                    put(st4, dests[s], pmsg.at[s, m])
                    hcopy(m, s).start()
                put(st4, c, phome.at[half, m])

    send_s(0)
    send_p(0)

    for cp in xcopies:
        cp.wait_recv()
    xsum = (xr[0] + xr[1]) + (xr[2] + xr[3])
    krows = pl.ds(pl.multiple_of(r * n + c * q, q), q)
    mfull[krows, :] = (oooo[krows, :].astype(F32) + 0.5 * xsum).astype(BF16)
    mcopies = []
    for s, (cc, rr) in enumerate(((nx, r), (ny, r), (dg, r), (c, o), (nx, o), (ny, o), (dg, o))):
        part_m = mfull.at[krows, pl.ds(pl.multiple_of(rr * n, n), n)]
        cp = _rcopy(part_m, part_m, ms.at[s], mrs.at[s], _dev(cc, rr))
        cp.start()
        mcopies.append(cp)

    @pl.loop(1, 4)
    def _(j):
        send_s(j)
        send_p(j)

    d_x.wait_recv()
    d_y.wait_recv()
    d_d.wait_recv()

    def ladder_copy(s):
        lanes = pl.ds(pl.multiple_of(s * STEP, STEP), STEP)
        return _rcopy(part.at[s, orows], theirs.at[:, lanes], rs, rrs, _dev(c, o))

    @pl.loop(0, w // STEP)
    def _(s):
        slot = s % 3

        @pl.when(s + 2 < w // STEP)
        def _():
            vcopy(s + 2, (s + 2) % 3).start()

        vcopy(s, slot).wait()
        va, vb = vv.at[slot, pl.ds(0, w)], vv.at[slot, pl.ds(w, w)]
        part[s, :, :] = (jnp.dot(tg[2 * r], va[...], preferred_element_type=F32)
                         + jnp.dot(tg[2 * r + 1], vb[...], preferred_element_type=F32))
        ladder_copy(s).start()

    def landed(like, sem):
        return pltpu.make_async_copy(like, like, sem)

    landed(theirs, rrs).wait()
    landed(theirs, rs).wait()

    for cp in (d_own, x0, y1, x1, y0, d_x, d_y, d_d, *xcopies, *mcopies):
        cp.wait_send()
    for p in range(4):
        fcopy(nx, h0, 0, p, _dev(ny, r)).wait_send()
        fcopy(ny, h1, 1, p, _dev(nx, r)).wait_send()

    for cp in mcopies:
        cp.wait_recv()
    m_mine = mfull[:, rows]

    @pl.loop(0, w // STEP)
    def _(s):
        lanes = pl.ds(pl.multiple_of(s * STEP, STEP), STEP)
        hole[:, lanes] = lax.dot_general(m_mine, tg[c, :, lanes], TN, preferred_element_type=F32)

    @pl.loop(0, 8)
    def _(i):
        line = pl.ds(pl.multiple_of(i * 16, 16), 16)
        line_r = pl.ds(pl.multiple_of(r * n + i * 16, 16), 16)
        mine = jnp.concatenate([part[s, line_r, :] for s in range(w // STEP)], axis=1)
        out_ref[line, :] = oovv[line, :].astype(F32) + (mine + theirs[line, :] + hole[line, :])

    landed(srecv.at[pl.ds(0, 3)], srs).wait()
    landed(smsg, ss).wait()
    @pl.loop(0, 8)
    def _(i):
        for jh in range(2):
            line = pl.ds(pl.multiple_of(i * 16 + jh * 8, 8), 8)
            sv = jnp.concatenate([srecv.at[2 * jh + e // 4, e % 4][pl.ds(i, 1), :] for e in range(8)], axis=0)
            out_ref[line, :] = out_ref[line, :] + sv

    mate = own == r
    zero4 = jnp.zeros((4, w), F32)
    for j in range(4):
        landed(pfar.at[:, j], prs.at[1, j]).wait()
        for a in range(2):
            line = pl.ds(pl.multiple_of((a * 4 + j) * 16 + o * 8, 8), 8)
            out_ref[line, :] = out_ref[line, :] + pfar[a, j]
        if j % 2 == 1:
            m = j // 2

            @pl.when(mate)
            def _():
                landed(phome.at[0, m], prs.at[0, m]).wait()

            @pl.when(jnp.logical_not(mate))
            def _():
                landed(phome.at[:, m], prs.at[0, m]).wait()

            for jj in (j - 1, j):
                for a in range(2):
                    line = pl.ds(pl.multiple_of((a * 4 + jj) * 16 + r * 8, 8), 8)
                    rest = phome[a, m, (jj % 2) * 4:(jj % 2) * 4 + 4, :]
                    both = (zero4, rest) if a == 0 else (rest, zero4)
                    out_ref[line, :] = out_ref[line, :] + jnp.concatenate(both, axis=0)

    @pl.when(mate)
    def _():
        landed(pmsg.at[pl.ds(0, 3), pl.ds(0, 2)], ps).wait()

    @pl.when(jnp.logical_not(mate))
    def _():
        landed(pmsg, ps).wait()


ANY = pl.BlockSpec(memory_space=pl.ANY)
DMA = pltpu.SemaphoreType.DMA


def sweep(t, oovv, vvvv, oooo, wd, wx):
    n, w = t.shape
    depth = vvvv.shape[0]
    V = pltpu.VMEM
    return pl.pallas_call(
        sweep_kernel,
        out_shape=jax.ShapeDtypeStruct((n, w), F32),
        in_specs=[ANY] * 6,
        out_specs=pl.BlockSpec(memory_space=pltpu.VMEM),
        scratch_shapes=[
            V((n, w), F32), V((n, w), BF16), V(oooo.shape, BF16), V(wd.shape, BF16), V(wx.shape, BF16),
            V((4, 2 * n, w), BF16),
            V((n, 2 * n), F32), V((4, n // 4, 2 * n), F32), V((2 * n, 2 * n), BF16), V((n, w), F32),
            V((n * PITCH, LANE), F32), V((OCC * LANE, 4 * LANE), BF16), V((wx.shape[1], wx.shape[0]), BF16),
            V((4, 2 * VIRT, 4 * LANE), F32), V((4, 4 * VIRT, 2 * LANE), F32),
            V((8 * PITCH, LANE), F32), V((8 * PITCH, LANE), F32),
            V((3, 4, 8, w), F32), V((4, 4, 8, w), F32), V((4, 4, 8, w), F32), V((2, 2, 8, w), F32), V((2, 4, 8, w), F32),
            V((3, depth, STEP), BF16), V((n, w), F32), V((w // STEP, 2 * n, STEP), F32), V(wx.shape, F32),
            DMA((5,)), DMA((10,)), DMA((10,)), DMA((2, 4)), DMA((2, 4)), DMA((3,)), DMA((3,)), DMA((7,)), DMA((7,)),
            DMA, DMA, DMA, DMA((2, 4)), DMA((3,)), DMA, DMA,
        ],
        compiler_params=pltpu.CompilerParams(collective_id=0, has_side_effects=True, vmem_limit_bytes=46 << 20),
        name="sweep",
    )(*(pltpu.with_memory_space_constraint(a, pltpu.HBM) for a in (t, oovv, vvvv, oooo, wd, wx)))


def solution(mesh):
    def local_sweep(t_blk, d_blk, oovv_blk, vvvv_blk, oooo_full, wd_blk, wx_blk):
        return sweep(t_blk, oovv_blk, vvvv_blk, oooo_full, wd_blk, wx_blk) / d_blk

    amp = P("row", "col")
    wide = P(None, "col")
    return jax.shard_map(local_sweep, mesh=mesh, in_specs=(amp, amp, amp, amp, P(), wide, wide), out_specs=amp, check_vma=False)
```

```python
import jax
import jax.numpy as jnp
from jax import lax
from jax.experimental import pallas as pl
from jax.experimental.pallas import tpu as pltpu
from jax.sharding import PartitionSpec as P

MESH = pl.DeviceIdType.MESH
F32 = jnp.float32
BF16 = jnp.bfloat16
NT = (((1,), (1,)), ((), ()))
TN = (((0,), (0,)), ((), ()))

OCC = 16
VIRT = 96
LANE = 128
PITCH = 104
STEP = 256


def _dev(c, r):
    return {"col": c, "row": r}


def _rcopy(src, dst, ssem, rsem, dev):
    return pltpu.make_async_remote_copy(src, dst, ssem, rsem, device_id=dev, device_id_type=MESH)


def sweep_kernel(t_hbm, oovv_hbm, v_hbm, oooo_hbm, wd_hbm, wx_hbm, out_ref,
                 t32, oovv, oooo, ww, tg, xp, xr, mfull, hole, t4, wd4, wxt, ubuf, vbuf_s, s4, st4,
                 smsg, pmsg, srecv, precv, rmsg, rrecv, vv, theirs, part, wxf,
                 lsem, gs, gr, fs, fr, xs, xrs, ms, mrs, ss, srs, ps, prs, rls, rlr, vsem, rs, rrs):
    r, c = lax.axis_index("row"), lax.axis_index("col")
    x, y = c % 2, c // 2
    o = 1 - r
    nx, ny, dg = y * 2 + (1 - x), (1 - y) * 2 + x, (1 - y) * 2 + (1 - x)
    n, w = t32.shape
    h = w // 2
    h0, h1 = pl.ds(0, h), pl.ds(h, h)
    rows = pl.ds(pl.multiple_of(r * n, n), n)
    orows = pl.ds(pl.multiple_of(o * n, n), n)

    chunk = n // 4
    tloads = [pltpu.make_async_copy(t_hbm.at[pl.ds(k * chunk, chunk)], t32.at[pl.ds(k * chunk, chunk)], lsem.at[k])
              for k in range(4)]
    for cp in tloads:
        cp.start()
    oload = pltpu.make_async_copy(oovv_hbm, oovv, lsem.at[4])
    hload = pltpu.make_async_copy(oooo_hbm, oooo, lsem.at[5])
    wloads = [pltpu.make_async_copy(a, ww.at[k], lsem.at[6]) for k, a in enumerate((wd_hbm, wx_hbm))]
    for cp in (*wloads, oload, hload):
        cp.start()

    own = c // 2
    half = c % 2
    home = (own + r + 1) % 2
    via = home * nx + (1 - home) * ny
    past = home * ny + (1 - home) * nx
    ro = (home + half) % 2
    di = 1 - ro

    def slot_s(chip, ih, m):
        return pl.ds(pl.multiple_of(((chip * 2 + ih) * 2 + m) * 8, 8), 8)

    def slot_p(kind, a, ih, m):
        return ((kind * 2 + a) * 2 + ih) * 2 + m

    zero8 = jnp.zeros((8, w), F32)
    for m in range(2):
        srecv[slot_s(dg, ro, m), :] = zero8
        precv[slot_p(0, 1 - half, half, m)] = zero8
        precv[slot_p(1, 1 - half, 1 - half, m)] = zero8

    sem = pltpu.get_barrier_semaphore()
    for cc, rr in ((nx, r), (ny, r), (dg, r), (c, o), (nx, o), (ny, o), (dg, o)):
        pl.semaphore_signal(sem, inc=1, device_id=_dev(cc, rr), device_id_type=MESH)

    def vcopy(s, slot):
        lanes = pl.ds(pl.multiple_of(s * STEP, STEP), STEP)
        return pltpu.make_async_copy(v_hbm.at[:, lanes], vv.at[slot], vsem.at[slot])

    def landed(like, sem):
        return pltpu.make_async_copy(like, like, sem)

    for k in range(4):
        tloads[k].wait()
        tg[c, pl.ds(pl.multiple_of(r * n + k * chunk, chunk), chunk), :] = t32[k * chunk:(k + 1) * chunk, :].astype(BF16)

    pl.semaphore_wait(sem, 7)

    def tcopy(chip, lanes, k, dev):
        ref = tg.at[chip, rows, lanes]
        return _rcopy(ref, ref, gs, gr.at[k], dev)

    def fcopy(chip, lanes, p, dev):
        ref = tg.at[chip, pl.ds(pl.multiple_of(r * n + p * 32, 32), 32), lanes]
        return _rcopy(ref, ref, fs, fr.at[p], dev)

    whole = pl.ds(0, w)
    x0 = tcopy(c, h0, 1, _dev(nx, r))
    y1 = tcopy(c, h1, 2, _dev(ny, r))
    d_own = tcopy(c, whole, 0, _dev(c, o))
    x1 = tcopy(c, h1, 3, _dev(nx, r))
    y0 = tcopy(c, h0, 4, _dev(ny, r))
    x0.start()
    y1.start()
    d_own.start()
    x1.start()
    y0.start()
    vcopy(0, 0).start()
    vcopy(1, 1).start()

    def spread_rows(chip, ib, first, groups):
        for g in range(first, first + groups):
            tile = tg[chip, pl.ds(pl.multiple_of(r * n + ib * 16, 16), 16), g * 384:(g + 1) * 384].astype(F32)
            for e in range(4):
                slab = tile[:, e * VIRT:(e + 1) * VIRT]
                slab = jnp.concatenate([slab, jnp.zeros((16, LANE - VIRT), F32)], axis=1)
                for half in range(2):
                    start = (ib * 16 + half * 8) * PITCH + chip * 24 + g * 4 + e
                    t4[pl.ds(start, 8, stride=PITCH), :] = slab[half * 8:half * 8 + 8]

    def spread(chip, first, groups):
        @pl.loop(0, n // 16)
        def _(ib):
            spread_rows(chip, ib, first, groups)

    spread(c, 0, 6)

    landed(ww, lsem.at[6]).wait()
    zrow = jnp.zeros((LANE - VIRT, 4 * LANE), BF16)

    @pl.loop(0, OCC)
    def _(k):
        blk = ww[0, pl.ds(pl.multiple_of(k * VIRT, 16), VIRT), :].astype(F32)
        parts = []
        for j in range(4):
            parts += [blk[:, j * VIRT:(j + 1) * VIRT], jnp.zeros((VIRT, LANE - VIRT), F32)]
        wd4[pl.ds(pl.multiple_of(k * LANE, LANE), VIRT), :] = jnp.concatenate(parts, axis=1).astype(BF16)
        wd4[pl.ds(pl.multiple_of(k * LANE + VIRT, 32), LANE - VIRT), :] = zrow
        wxf[pl.ds(pl.multiple_of(k * VIRT, 16), VIRT), :] = ww[1, pl.ds(pl.multiple_of(k * VIRT, 16), VIRT), :].astype(F32)

    for s, chip in enumerate((c, nx, ny, dg)):
        for b in range(3):
            blk = jnp.concatenate(
                [wxf[pl.ds(pl.multiple_of(k * VIRT + chip * 24, 8), 24), b * LANE:(b + 1) * LANE] for k in range(OCC)],
                axis=0)
            wxt[b * LANE:(b + 1) * LANE, s * 384:(s + 1) * 384] = blk.astype(BF16).T

    oload.wait()
    hload.wait()
    d_own.wait_recv()
    xp[...] = lax.dot_general(oovv[...], tg[c], NT, preferred_element_type=F32)

    def direct_rows(chip, i0, count):
        lhs = jnp.concatenate(
            [jnp.concatenate(
                [t4[pl.ds(pl.multiple_of(((i0 + i) * OCC + k) * PITCH + chip * 24, 8), 24), :] for i in range(count)],
                axis=0)
             for k in range(OCC)], axis=1).astype(BF16)
        return jnp.dot(lhs, wd4[...], preferred_element_type=F32)

    def direct(chip):
        ubuf[chip, :, :] = direct_rows(chip, 0, 8)

    def exchange_pair(chips, first, i2):
        halves = []
        for e in range(2):
            halves.append(jnp.concatenate(
                [t4[pl.ds(pl.multiple_of(((2 * i2 + e) * OCC + k) * PITCH + chip * 24, 8), 24), :]
                 for chip in chips for k in range(OCC)], axis=0))
        rhs = jnp.concatenate(halves, axis=1).astype(BF16)
        prod = jnp.dot(wxt[:, first * 384:(first + len(chips)) * 384], rhs, preferred_element_type=F32)
        vbuf_s[i2, :, :] = prod if first == 0 else vbuf_s[i2, :, :] + prod

    def exchange(chips, first):
        @pl.loop(0, 4)
        def _(i2):
            exchange_pair(chips, first, i2)

    direct(c)

    x0.wait_recv()
    for p in range(4):
        fcopy(nx, h0, p, _dev(ny, r)).start()
    y1.wait_recv()
    for p in range(4):
        fcopy(ny, h1, p, _dev(nx, r)).start()
    q = n // 4
    for cc in (nx, ny, dg):
        cp = _rcopy(xp.at[pl.ds(pl.multiple_of(cc * q, q), q)], xr.at[c], xs, xrs, _dev(cc, r))
        cp.start()
    xr[c, :, :] = xp[pl.ds(pl.multiple_of(c * q, q), q), :]
    spread(nx, 0, 3)
    spread(ny, 3, 3)
    x1.wait_recv()
    d_x = tcopy(nx, whole, 5, _dev(c, o))
    d_x.start()
    y0.wait_recv()
    d_y = tcopy(ny, whole, 5, _dev(c, o))
    d_y.start()
    spread(nx, 3, 3)
    spread(ny, 0, 3)
    direct(nx)
    direct(ny)
    exchange((c, nx, ny), 0)

    @pl.loop(0, 4)
    def _(p):
        landed(tg.at[dg, pl.ds(0, n // 4)], fr.at[p]).wait()
        for ib in range(2):
            spread_rows(dg, 2 * p + ib, 0, 6)
        ubuf[dg, pl.ds(pl.multiple_of(p * 48, 16), 48), :] = direct_rows(dg, 2 * p, 2)
        exchange_pair((dg,), 3, p)

    d_d = tcopy(dg, whole, 5, _dev(c, o))
    d_d.start()

    def row_of(ih, j, e):
        return pl.multiple_of((((j // 2) * 2 + ih) * 8 + (j % 2) * 4 + e) * PITCH, 8)

    def block(i, j):
        direct_part = jnp.concatenate(
            [ubuf[chip, pl.ds(pl.multiple_of(i * 24, 8), 24), pl.ds(pl.multiple_of(j * LANE, LANE), LANE)]
             for chip in range(4)], axis=0)
        return direct_part - vbuf_s[
            i // 2, pl.ds(pl.multiple_of(j * VIRT, 8), VIRT), pl.ds(pl.multiple_of((i % 2) * LANE, LANE), LANE)]

    def fill_s(ih):
        @pl.loop(0, 4)
        def _(j):
            for e in range(4):
                s4[pl.ds(row_of(ih, j, e), VIRT), :] = block(ih * 4 + e, j)

    def fill_t(ih):
        @pl.loop(0, 4)
        def _(j):
            for e in range(4):
                at = pl.ds(row_of(ih, j, e), VIRT)
                st4[at, :VIRT] = s4[at, :].T[:VIRT, :]

    def put(src, ih, m, chip, dst):
        first = ((m * 2 + ih) * 8) * PITCH + chip * 24
        for g in range(6):
            vals = [src[pl.ds(first + g * 4 + e, 8, stride=PITCH), :][:, :VIRT] for e in range(4)]
            dst[:, g * 384:(g + 1) * 384] = jnp.concatenate(vals, axis=1)

    def s_copy(slot, ih, m, chip):
        buf = smsg.at[slot * 4 + ih * 2 + m]
        return _rcopy(buf, srecv.at[slot_s(c, ih, m)], ss, srs, _dev(chip, r))

    def p_copy(slot, ih, m, chip):
        buf = pmsg.at[slot * 4 + ih * 2 + m]
        return _rcopy(buf, precv.at[slot_p(1 - home, half, ih, m)], ps, prs, _dev(chip, own))

    def relay(kind, src):
        @pl.loop(0, 2)
        def _(m):
            put(src, ro, m, dg, rmsg.at[kind * 2 + m])
            to = rrecv.at[pl.ds(pl.multiple_of((kind * 2 + m) * 8, 8), 8)]
            _rcopy(rmsg.at[kind * 2 + m], to, rls, rlr, _dev(via, own)).start()

    def send(src, msg, copy, slot, ih, chip):
        @pl.loop(0, 2)
        def _(m):
            put(src, ih, m, chip, msg.at[slot * 4 + ih * 2 + m])
            copy(slot, ih, m, chip).start()

    fill_s(ro)
    relay(0, s4)
    fill_t(ro)
    relay(1, st4)
    send(s4, smsg, s_copy, 1, ro, via)
    send(st4, pmsg, p_copy, 1, ro, via)

    landed(xr.at[pl.ds(0, 3)], xrs).wait()
    xsum = (xr[0] + xr[1]) + (xr[2] + xr[3])
    krows = pl.ds(pl.multiple_of(r * n + c * q, q), q)
    mfull[krows, :] = (oooo[krows, :].astype(F32) + 0.5 * xsum).astype(BF16)
    for cc, rr in ((nx, r), (ny, r), (dg, r), (c, o), (nx, o), (ny, o), (dg, o)):
        part_m = mfull.at[krows, pl.ds(pl.multiple_of(rr * n, n), n)]
        _rcopy(part_m, part_m, ms, mrs, _dev(cc, rr)).start()

    fill_s(di)

    @pl.when(home == 1)
    def _():
        @pl.loop(0, 4)
        def _(j):
            for e in range(4):
                at = pl.ds(row_of(di, j, e), VIRT)
                s4[at, :VIRT] = s4[at, :VIRT] + block(half * 4 + j, e).T[:VIRT, :]

    send(s4, smsg, s_copy, 0, di, dg)
    send(s4, smsg, s_copy, 1, di, via)
    send(s4, smsg, s_copy, 2, di, past)

    @pl.when(home == 0)
    def _():
        fill_t(di)
        send(st4, pmsg, p_copy, 0, di, dg)
        send(st4, pmsg, p_copy, 1, di, via)
        send(st4, pmsg, p_copy, 2, di, past)
        send(st4, pmsg, p_copy, 3, ro, c)
        send(st4, pmsg, p_copy, 3, di, c)

    @pl.loop(0, 2)
    def _(m):
        for ih in range(2):
            put(s4, ih, m, c, srecv.at[slot_s(c, ih, m)])

    @pl.when(home == 1)
    def _():
        @pl.loop(0, 2)
        def _(m):
            put(st4, ro, m, c, precv.at[slot_p(0, half, ro, m)])

    def every_fourth(ref, first):
        return jnp.concatenate([ref[pl.ds(first + 4 * k, 1), :] for k in range(4)], axis=0)

    def pass_on():
        landed(rrecv, rlr).wait()
        for kind, (src, msg, copy) in ((1, (s4, smsg, s_copy)), (0, (st4, pmsg, p_copy))):
            for m in range(2):
                buf = msg.at[2 * 4 + ro * 2 + m]
                put(src, ro, m, past, buf)
                extra = jnp.concatenate([every_fourth(rrecv, kind * 16 + 2 * m + k) for k in range(2)], axis=0)
                buf[...] = buf[...] + extra
                copy(2, ro, m, past).start()

    landed(tg.at[pl.ds(0, 3), pl.ds(0, n)], gr.at[5]).wait()

    def ladder_copy(s):
        lanes = pl.ds(pl.multiple_of(s * STEP, STEP), STEP)
        return _rcopy(part.at[s, orows], theirs.at[:, lanes], rs, rrs, _dev(c, o))

    @pl.loop(0, w // STEP)
    def _(s):
        slot = s % 3

        @pl.when(s + 2 < w // STEP)
        def _():
            vcopy(s + 2, (s + 2) % 3).start()

        vcopy(s, slot).wait()
        va, vb = vv.at[slot, pl.ds(0, w)], vv.at[slot, pl.ds(w, w)]
        part[s, :, :] = (jnp.dot(tg[2 * r], va[...], preferred_element_type=F32)
                         + jnp.dot(tg[2 * r + 1], vb[...], preferred_element_type=F32))
        ladder_copy(s).start()

        @pl.when(s == 5)
        def _():
            pass_on()

    landed(theirs, rrs).wait()
    landed(theirs, rs).wait()

    landed(tg.at[pl.ds(0, 3)], gs).wait()
    landed(tg.at[0, pl.ds(0, n)], fs).wait()
    landed(xr.at[pl.ds(0, 3)], xs).wait()
    all_m = mfull.at[pl.ds(0, 7 * q), pl.ds(0, n)]
    landed(all_m, mrs).wait()
    landed(all_m, ms).wait()
    m_mine = mfull[:, rows]

    @pl.loop(0, w // STEP)
    def _(s):
        lanes = pl.ds(pl.multiple_of(s * STEP, STEP), STEP)
        hole[:, lanes] = lax.dot_general(m_mine, tg[c, :, lanes], TN, preferred_element_type=F32)

    @pl.loop(0, 8)
    def _(i):
        line = pl.ds(pl.multiple_of(i * 16, 16), 16)
        line_r = pl.ds(pl.multiple_of(r * n + i * 16, 16), 16)
        mine = jnp.concatenate([part[s, line_r, :] for s in range(w // STEP)], axis=1)
        out_ref[line, :] = oovv[line, :].astype(F32) + (mine + theirs[line, :] + hole[line, :])

    landed(rmsg, rls).wait()
    landed(srecv.at[pl.ds(0, 80)], srs).wait()
    @pl.loop(0, 8)
    def _(i):
        for jh in range(2):
            line = pl.ds(pl.multiple_of(i * 16 + jh * 8, 8), 8)
            sv = jnp.concatenate(
                [every_fourth(srecv, ((2 * jh + cc) * 2 + i // 4) * 16 + i % 4) for cc in range(2)], axis=0)
            out_ref[line, :] = out_ref[line, :] + sv

    @pl.when(home == 1)
    def _():
        landed(precv.at[pl.ds(0, 10)], prs).wait()

    @pl.when(home == 0)
    def _():
        landed(precv.at[pl.ds(0, 8)], prs).wait()

    zero4 = jnp.zeros((4, w), F32)
    for a in range(2):
        for j in range(4):
            m, rows4 = j // 2, slice(j % 2 * 4, j % 2 * 4 + 4)
            for kind, row in ((0, r), (1, o)):
                line = pl.ds(pl.multiple_of((a * 4 + j) * 16 + row * 8, 8), 8)
                both = [zero4 if kind == 0 and ih == a else precv[slot_p(kind, a, ih, m), rows4, :] for ih in range(2)]
                out_ref[line, :] = out_ref[line, :] + jnp.concatenate(both, axis=0)

    landed(smsg.at[pl.ds(0, 10)], ss).wait()

    @pl.when(home == 1)
    def _():
        landed(pmsg.at[pl.ds(0, 4)], ps).wait()

    @pl.when(home == 0)
    def _():
        landed(pmsg.at[pl.ds(0, 14)], ps).wait()


ANY = pl.BlockSpec(memory_space=pl.ANY)
DMA = pltpu.SemaphoreType.DMA


def sweep(t, oovv, vvvv, oooo, wd, wx):
    n, w = t.shape
    depth = vvvv.shape[0]
    V = pltpu.VMEM
    return pl.pallas_call(
        sweep_kernel,
        out_shape=jax.ShapeDtypeStruct((n, w), F32),
        in_specs=[ANY] * 6,
        out_specs=pl.BlockSpec(memory_space=pltpu.VMEM),
        scratch_shapes=[
            V((n, w), F32), V((n, w), BF16), V(oooo.shape, BF16), V((2,) + wd.shape, BF16),
            V((4, 2 * n, w), BF16),
            V((n, 2 * n), F32), V((4, n // 4, 2 * n), F32), V((2 * n, 2 * n), BF16), V((n, w), F32),
            V((n * PITCH, LANE), F32), V((OCC * LANE, 4 * LANE), BF16), V((wx.shape[1], wx.shape[0]), BF16),
            V((4, 2 * VIRT, 4 * LANE), F32), V((4, 4 * VIRT, 2 * LANE), F32),
            V((32 * PITCH, LANE), F32), V((32 * PITCH, LANE), F32),
            V((12, 8, w), F32), V((16, 8, w), F32), V((128, w), F32), V((16, 8, w), F32), V((4, 8, w), F32), V((32, w), F32),
            V((3, depth, STEP), BF16), V((n, w), F32), V((w // STEP, 2 * n, STEP), F32), V(wx.shape, F32),
            DMA((7,)), DMA, DMA((6,)), DMA, DMA((4,)), DMA, DMA, DMA, DMA,
            DMA, DMA, DMA, DMA, DMA, DMA, DMA((3,)), DMA, DMA,
        ],
        compiler_params=pltpu.CompilerParams(collective_id=0, has_side_effects=True, vmem_limit_bytes=46 << 20),
        name="sweep",
    )(*(pltpu.with_memory_space_constraint(a, pltpu.HBM) for a in (t, oovv, vvvv, oooo, wd, wx)))


def solution(mesh):
    def local_sweep(t_blk, d_blk, oovv_blk, vvvv_blk, oooo_full, wd_blk, wx_blk):
        return sweep(t_blk, oovv_blk, vvvv_blk, oooo_full, wd_blk, wx_blk) / d_blk

    amp = P("row", "col")
    wide = P(None, "col")
    return jax.shard_map(local_sweep, mesh=mesh, in_specs=(amp, amp, amp, amp, P(), wide, wide), out_specs=amp, check_vma=False)
```

```python
import jax
import jax.numpy as jnp
from jax import lax
from jax.experimental import pallas as pl
from jax.experimental.pallas import tpu as pltpu
from jax.sharding import PartitionSpec as P

MESH = pl.DeviceIdType.MESH
F32 = jnp.float32
BF16 = jnp.bfloat16
NT = (((1,), (1,)), ((), ()))
TN = (((0,), (0,)), ((), ()))

OCC = 16
VIRT = 96
LANE = 128
PITCH = 104
STEP = 256


def _dev(c, r):
    return {"col": c, "row": r}


def _rcopy(src, dst, ssem, rsem, dev):
    return pltpu.make_async_remote_copy(src, dst, ssem, rsem, device_id=dev, device_id_type=MESH)


def sweep_kernel(t_hbm, oovv_hbm, v_hbm, oooo_hbm, wd_hbm, wx_hbm, out_ref,
                 t32, oovv, oooo, ww, tg, xp, xr, mfull, hole, t4, wd4, wxt, ubuf, vbuf_s, s4, st4,
                 smsg, pmsg, srecv, precv, rmsg, rrecv, vv, theirs, part, wxf,
                 lsem, gs, gr, fs, fr, xs, xrs, ms, mrs, ss, srs, ps, prs, rls, rlr, vsem, rs, rrs):
    r, c = lax.axis_index("row"), lax.axis_index("col")
    x, y = c % 2, c // 2
    o = 1 - r
    nx, ny, dg = y * 2 + (1 - x), (1 - y) * 2 + x, (1 - y) * 2 + (1 - x)
    n, w = t32.shape
    h = w // 2
    h0, h1 = pl.ds(0, h), pl.ds(h, h)
    rows = pl.ds(pl.multiple_of(r * n, n), n)
    orows = pl.ds(pl.multiple_of(o * n, n), n)

    chunk = n // 4
    tloads = [pltpu.make_async_copy(t_hbm.at[pl.ds(k * chunk, chunk)], t32.at[pl.ds(k * chunk, chunk)], lsem.at[k])
              for k in range(4)]
    for cp in tloads:
        cp.start()
    oload = pltpu.make_async_copy(oovv_hbm, oovv, lsem.at[4])
    hload = pltpu.make_async_copy(oooo_hbm, oooo, lsem.at[5])
    wloads = [pltpu.make_async_copy(a, ww.at[k], lsem.at[6]) for k, a in enumerate((wd_hbm, wx_hbm))]
    for cp in (*wloads, oload, hload):
        cp.start()

    own = c // 2
    half = c % 2
    home = (own + r + 1) % 2
    via = home * nx + (1 - home) * ny
    past = home * ny + (1 - home) * nx
    ro = (home + half) % 2
    di = 1 - ro

    def slot_s(chip, ih, m):
        return pl.ds(pl.multiple_of(((chip * 2 + ih) * 2 + m) * 8, 8), 8)

    def slot_p(kind, a, ih, m):
        return ((kind * 2 + a) * 2 + ih) * 2 + m

    zero8 = jnp.zeros((8, w), F32)
    for m in range(2):
        srecv[slot_s(dg, ro, m), :] = zero8
        precv[slot_p(0, 1 - half, half, m)] = zero8
        precv[slot_p(1, 1 - half, 1 - half, m)] = zero8

    sem = pltpu.get_barrier_semaphore()
    for cc, rr in ((nx, r), (ny, r), (dg, r), (c, o), (nx, o), (ny, o), (dg, o)):
        pl.semaphore_signal(sem, inc=1, device_id=_dev(cc, rr), device_id_type=MESH)

    def vcopy(s, slot):
        lanes = pl.ds(pl.multiple_of(s * STEP, STEP), STEP)
        return pltpu.make_async_copy(v_hbm.at[:, lanes], vv.at[slot], vsem.at[slot])

    def landed(like, sem):
        return pltpu.make_async_copy(like, like, sem)

    for k in range(4):
        tloads[k].wait()
        tg[c, pl.ds(pl.multiple_of(r * n + k * chunk, chunk), chunk), :] = t32[k * chunk:(k + 1) * chunk, :].astype(BF16)

    pl.semaphore_wait(sem, 7)

    def tcopy(chip, lanes, k, dev):
        ref = tg.at[chip, rows, lanes]
        return _rcopy(ref, ref, gs, gr.at[k], dev)

    def fcopy(chip, lanes, p, dev):
        ref = tg.at[chip, pl.ds(pl.multiple_of(r * n + p * 32, 32), 32), lanes]
        return _rcopy(ref, ref, fs, fr.at[p], dev)

    whole = pl.ds(0, w)
    x0 = tcopy(c, h0, 1, _dev(nx, r))
    y1 = tcopy(c, h1, 2, _dev(ny, r))
    d_own = tcopy(c, whole, 0, _dev(c, o))
    x1 = tcopy(c, h1, 3, _dev(nx, r))
    y0 = tcopy(c, h0, 4, _dev(ny, r))
    x0.start()
    y1.start()
    d_own.start()
    x1.start()
    y0.start()
    vcopy(0, 0).start()
    vcopy(1, 1).start()

    def spread_rows(chip, ib, first, groups):
        for g in range(first, first + groups):
            tile = tg[chip, pl.ds(pl.multiple_of(r * n + ib * 16, 16), 16), g * 384:(g + 1) * 384].astype(F32)
            for e in range(4):
                slab = tile[:, e * VIRT:(e + 1) * VIRT]
                slab = jnp.concatenate([slab, jnp.zeros((16, LANE - VIRT), F32)], axis=1)
                for half in range(2):
                    start = (ib * 16 + half * 8) * PITCH + chip * 24 + g * 4 + e
                    t4[pl.ds(start, 8, stride=PITCH), :] = slab[half * 8:half * 8 + 8]

    def spread(chip, first, groups):
        @pl.loop(0, n // 16)
        def _(ib):
            spread_rows(chip, ib, first, groups)

    spread(c, 0, 6)

    landed(ww, lsem.at[6]).wait()
    zrow = jnp.zeros((LANE - VIRT, 4 * LANE), BF16)

    @pl.loop(0, OCC)
    def _(k):
        blk = ww[0, pl.ds(pl.multiple_of(k * VIRT, 16), VIRT), :].astype(F32)
        parts = []
        for j in range(4):
            parts += [blk[:, j * VIRT:(j + 1) * VIRT], jnp.zeros((VIRT, LANE - VIRT), F32)]
        wd4[pl.ds(pl.multiple_of(k * LANE, LANE), VIRT), :] = jnp.concatenate(parts, axis=1).astype(BF16)
        wd4[pl.ds(pl.multiple_of(k * LANE + VIRT, 32), LANE - VIRT), :] = zrow
        wxf[pl.ds(pl.multiple_of(k * VIRT, 16), VIRT), :] = ww[1, pl.ds(pl.multiple_of(k * VIRT, 16), VIRT), :].astype(F32)

    for s, chip in enumerate((c, nx, ny, dg)):
        for b in range(3):
            blk = jnp.concatenate(
                [wxf[pl.ds(pl.multiple_of(k * VIRT + chip * 24, 8), 24), b * LANE:(b + 1) * LANE] for k in range(OCC)],
                axis=0)
            wxt[b * LANE:(b + 1) * LANE, s * 384:(s + 1) * 384] = blk.astype(BF16).T

    oload.wait()
    hload.wait()
    d_own.wait_recv()
    xp[...] = lax.dot_general(oovv[...], tg[c], NT, preferred_element_type=F32)

    def direct_rows(chip, i0, count):
        lhs = jnp.concatenate(
            [jnp.concatenate(
                [t4[pl.ds(pl.multiple_of(((i0 + i) * OCC + k) * PITCH + chip * 24, 8), 24), :] for i in range(count)],
                axis=0)
             for k in range(OCC)], axis=1).astype(BF16)
        return jnp.dot(lhs, wd4[...], preferred_element_type=F32)

    def direct(chip):
        ubuf[chip, :, :] = direct_rows(chip, 0, 8)

    def exchange_pair(chips, first, i2):
        halves = []
        for e in range(2):
            halves.append(jnp.concatenate(
                [t4[pl.ds(pl.multiple_of(((2 * i2 + e) * OCC + k) * PITCH + chip * 24, 8), 24), :]
                 for chip in chips for k in range(OCC)], axis=0))
        rhs = jnp.concatenate(halves, axis=1).astype(BF16)
        prod = jnp.dot(wxt[:, first * 384:(first + len(chips)) * 384], rhs, preferred_element_type=F32)
        vbuf_s[i2, :, :] = prod if first == 0 else vbuf_s[i2, :, :] + prod

    def exchange(chips, first):
        @pl.loop(0, 4)
        def _(i2):
            exchange_pair(chips, first, i2)

    direct(c)

    x0.wait_recv()
    for p in range(4):
        fcopy(nx, h0, p, _dev(ny, r)).start()
    y1.wait_recv()
    for p in range(4):
        fcopy(ny, h1, p, _dev(nx, r)).start()
    q = n // 4
    for cc in (nx, ny, dg):
        cp = _rcopy(xp.at[pl.ds(pl.multiple_of(cc * q, q), q)], xr.at[c], xs, xrs, _dev(cc, r))
        cp.start()
    xr[c, :, :] = xp[pl.ds(pl.multiple_of(c * q, q), q), :]
    spread(nx, 0, 3)
    spread(ny, 3, 3)
    x1.wait_recv()
    d_x = tcopy(nx, whole, 5, _dev(c, o))
    d_x.start()
    y0.wait_recv()
    d_y = tcopy(ny, whole, 5, _dev(c, o))
    d_y.start()
    spread(nx, 3, 3)
    spread(ny, 0, 3)
    direct(nx)
    direct(ny)
    exchange((c, nx, ny), 0)

    @pl.loop(0, 4)
    def _(p):
        landed(tg.at[dg, pl.ds(0, n // 4)], fr.at[p]).wait()
        for ib in range(2):
            spread_rows(dg, 2 * p + ib, 0, 6)
        ubuf[dg, pl.ds(pl.multiple_of(p * 48, 16), 48), :] = direct_rows(dg, 2 * p, 2)
        exchange_pair((dg,), 3, p)

    d_d = tcopy(dg, whole, 5, _dev(c, o))
    d_d.start()

    def s_rows(i, j):
        return pl.ds(pl.multiple_of((i * 4 + j) * PITCH, 8), VIRT)

    def t_rows(i, j):
        return pl.ds(pl.multiple_of(((i // 4) * 16 + j * 4 + i % 4) * PITCH, 8), VIRT)

    def block(i, j):
        direct_part = jnp.concatenate(
            [ubuf[chip, pl.ds(pl.multiple_of(i * 24, 8), 24), pl.ds(pl.multiple_of(j * LANE, LANE), LANE)]
             for chip in range(4)], axis=0)
        return direct_part - vbuf_s[
            i // 2, pl.ds(pl.multiple_of(j * VIRT, 8), VIRT), pl.ds(pl.multiple_of((i % 2) * LANE, LANE), LANE)]

    def fill_s(ih):
        @pl.loop(0, 4)
        def _(j):
            for e in range(4):
                s4[s_rows(ih * 4 + e, j), :] = block(ih * 4 + e, j)

    def fill_t(ih):
        @pl.loop(0, 4)
        def _(j):
            for e in range(4):
                st4[t_rows(ih * 4 + e, j), :VIRT] = s4[s_rows(ih * 4 + e, j), :].T[:VIRT, :]

    def put(src, ih, m, chip, dst):
        first = (ih * 16 + m * 8) * PITCH + chip * 24
        for g in range(6):
            vals = [src[pl.ds(first + g * 4 + e, 8, stride=PITCH), :][:, :VIRT] for e in range(4)]
            dst[:, g * 384:(g + 1) * 384] = jnp.concatenate(vals, axis=1)

    def s_copy(slot, ih, m, chip):
        buf = smsg.at[slot * 4 + ih * 2 + m]
        return _rcopy(buf, srecv.at[slot_s(c, ih, m)], ss, srs, _dev(chip, r))

    def p_copy(slot, ih, m, chip):
        buf = pmsg.at[slot * 4 + ih * 2 + m]
        return _rcopy(buf, precv.at[slot_p(1 - home, half, ih, m)], ps, prs, _dev(chip, own))

    def relay(kind, src):
        @pl.loop(0, 2)
        def _(m):
            put(src, ro, m, dg, rmsg.at[kind * 2 + m])
            to = rrecv.at[pl.ds(pl.multiple_of((kind * 2 + m) * 8, 8), 8)]
            _rcopy(rmsg.at[kind * 2 + m], to, rls, rlr, _dev(via, own)).start()

    def send(src, msg, copy, slot, ih, chip):
        @pl.loop(0, 2)
        def _(m):
            put(src, ih, m, chip, msg.at[slot * 4 + ih * 2 + m])
            copy(slot, ih, m, chip).start()

    fill_s(ro)
    relay(0, s4)
    fill_t(ro)
    relay(1, st4)

    landed(xr.at[pl.ds(0, 3)], xrs).wait()
    xsum = (xr[0] + xr[1]) + (xr[2] + xr[3])
    krows = pl.ds(pl.multiple_of(r * n + c * q, q), q)
    mfull[krows, :] = (oooo[krows, :].astype(F32) + 0.5 * xsum).astype(BF16)
    for cc, rr in ((nx, r), (ny, r), (dg, r), (c, o), (nx, o), (ny, o), (dg, o)):
        part_m = mfull.at[krows, pl.ds(pl.multiple_of(rr * n, n), n)]
        _rcopy(part_m, part_m, ms, mrs, _dev(cc, rr)).start()

    fill_s(di)

    @pl.when(home == 1)
    def _():
        @pl.loop(0, 4)
        def _(j):
            for e in range(4):
                at = s_rows(half * 4 + e, j)
                s4[at, :VIRT] = s4[at, :VIRT] + block(half * 4 + j, e).T[:VIRT, :]

    send(s4, smsg, s_copy, 2, di, past)
    send(s4, smsg, s_copy, 0, di, dg)

    @pl.when(home == 0)
    def _():
        fill_t(di)
        send(st4, pmsg, p_copy, 2, di, past)
        send(st4, pmsg, p_copy, 0, di, dg)
        send(st4, pmsg, p_copy, 3, ro, c)
        send(st4, pmsg, p_copy, 3, di, c)

    @pl.loop(0, 2)
    def _(m):
        for ih in range(2):
            put(s4, ih, m, c, srecv.at[slot_s(c, ih, m)])

    @pl.when(home == 1)
    def _():
        @pl.loop(0, 2)
        def _(m):
            put(st4, ro, m, c, precv.at[slot_p(0, half, ro, m)])

    def pass_on():
        landed(rrecv, rlr).wait()
        for kind, (src, msg, copy) in ((1, (s4, smsg, s_copy)), (0, (st4, pmsg, p_copy))):
            for m in range(2):
                buf = msg.at[2 * 4 + ro * 2 + m]
                put(src, ro, m, past, buf)
                buf[...] = buf[...] + rrecv[(kind * 2 + m) * 8:(kind * 2 + m + 1) * 8, :]
                copy(2, ro, m, past).start()

    landed(tg.at[pl.ds(0, 3), pl.ds(0, n)], gr.at[5]).wait()

    def ladder_copy(s):
        lanes = pl.ds(pl.multiple_of(s * STEP, STEP), STEP)
        return _rcopy(part.at[s, orows], theirs.at[:, lanes], rs, rrs, _dev(c, o))

    @pl.loop(0, w // STEP)
    def _(s):
        slot = s % 3

        @pl.when(s + 2 < w // STEP)
        def _():
            vcopy(s + 2, (s + 2) % 3).start()

        vcopy(s, slot).wait()
        va, vb = vv.at[slot, pl.ds(0, w)], vv.at[slot, pl.ds(w, w)]
        part[s, :, :] = (jnp.dot(tg[2 * r], va[...], preferred_element_type=F32)
                         + jnp.dot(tg[2 * r + 1], vb[...], preferred_element_type=F32))
        ladder_copy(s).start()

        @pl.when(s == 0)
        def _():
            send(s4, smsg, s_copy, 1, ro, via)

        @pl.when(s == 1)
        def _():
            send(s4, smsg, s_copy, 1, di, via)

        @pl.when(s == 2)
        def _():
            send(st4, pmsg, p_copy, 1, ro, via)

        @pl.when(jnp.logical_and(s == 3, home == 0))
        def _():
            send(st4, pmsg, p_copy, 1, di, via)

        @pl.when(s == 5)
        def _():
            pass_on()

    landed(theirs, rrs).wait()
    landed(theirs, rs).wait()

    landed(tg.at[pl.ds(0, 3)], gs).wait()
    landed(tg.at[0, pl.ds(0, n)], fs).wait()
    landed(xr.at[pl.ds(0, 3)], xs).wait()
    all_m = mfull.at[pl.ds(0, 7 * q), pl.ds(0, n)]
    landed(all_m, mrs).wait()
    landed(all_m, ms).wait()
    m_mine = mfull[:, rows]

    @pl.loop(0, w // STEP)
    def _(s):
        lanes = pl.ds(pl.multiple_of(s * STEP, STEP), STEP)
        hole[:, lanes] = lax.dot_general(m_mine, tg[c, :, lanes], TN, preferred_element_type=F32)

    @pl.loop(0, 8)
    def _(i):
        line = pl.ds(pl.multiple_of(i * 16, 16), 16)
        line_r = pl.ds(pl.multiple_of(r * n + i * 16, 16), 16)
        mine = jnp.concatenate([part[s, line_r, :] for s in range(w // STEP)], axis=1)
        out_ref[line, :] = oovv[line, :].astype(F32) + (mine + theirs[line, :] + hole[line, :])

    landed(rmsg, rls).wait()
    landed(srecv.at[pl.ds(0, 80)], srs).wait()
    for i in range(8):
        for jh in range(2):
            line = slice(i * 16 + jh * 8, i * 16 + jh * 8 + 8)
            rows4 = [((2 * jh + cc) * 4 + i // 2) * 8 + i % 2 * 4 for cc in range(2)]
            out_ref[line, :] = out_ref[line, :] + jnp.concatenate([srecv[k:k + 4, :] for k in rows4], axis=0)

    @pl.when(home == 1)
    def _():
        landed(precv.at[pl.ds(0, 10)], prs).wait()

    @pl.when(home == 0)
    def _():
        landed(precv.at[pl.ds(0, 8)], prs).wait()

    zero4 = jnp.zeros((4, w), F32)
    for a in range(2):
        for j in range(4):
            m, rows4 = j // 2, slice(j % 2 * 4, j % 2 * 4 + 4)
            for kind, row in ((0, r), (1, o)):
                line = pl.ds(pl.multiple_of((a * 4 + j) * 16 + row * 8, 8), 8)
                both = [zero4 if kind == 0 and ih == a else precv[slot_p(kind, a, ih, m), rows4, :] for ih in range(2)]
                out_ref[line, :] = out_ref[line, :] + jnp.concatenate(both, axis=0)

    landed(smsg.at[pl.ds(0, 10)], ss).wait()

    @pl.when(home == 1)
    def _():
        landed(pmsg.at[pl.ds(0, 4)], ps).wait()

    @pl.when(home == 0)
    def _():
        landed(pmsg.at[pl.ds(0, 14)], ps).wait()


ANY = pl.BlockSpec(memory_space=pl.ANY)
DMA = pltpu.SemaphoreType.DMA


def sweep(t, oovv, vvvv, oooo, wd, wx):
    n, w = t.shape
    depth = vvvv.shape[0]
    V = pltpu.VMEM
    return pl.pallas_call(
        sweep_kernel,
        out_shape=jax.ShapeDtypeStruct((n, w), F32),
        in_specs=[ANY] * 6,
        out_specs=pl.BlockSpec(memory_space=pltpu.VMEM),
        scratch_shapes=[
            V((n, w), F32), V((n, w), BF16), V(oooo.shape, BF16), V((2,) + wd.shape, BF16),
            V((4, 2 * n, w), BF16),
            V((n, 2 * n), F32), V((4, n // 4, 2 * n), F32), V((2 * n, 2 * n), BF16), V((n, w), F32),
            V((n * PITCH, LANE), F32), V((OCC * LANE, 4 * LANE), BF16), V((wx.shape[1], wx.shape[0]), BF16),
            V((4, 2 * VIRT, 4 * LANE), F32), V((4, 4 * VIRT, 2 * LANE), F32),
            V((32 * PITCH, LANE), F32), V((32 * PITCH, LANE), F32),
            V((12, 8, w), F32), V((16, 8, w), F32), V((128, w), F32), V((16, 8, w), F32), V((4, 8, w), F32), V((32, w), F32),
            V((3, depth, STEP), BF16), V((n, w), F32), V((w // STEP, 2 * n, STEP), F32), V(wx.shape, F32),
            DMA((7,)), DMA, DMA((6,)), DMA, DMA((4,)), DMA, DMA, DMA, DMA,
            DMA, DMA, DMA, DMA, DMA, DMA, DMA((3,)), DMA, DMA,
        ],
        compiler_params=pltpu.CompilerParams(collective_id=0, has_side_effects=True, vmem_limit_bytes=46 << 20),
        name="sweep",
    )(*(pltpu.with_memory_space_constraint(a, pltpu.HBM) for a in (t, oovv, vvvv, oooo, wd, wx)))


def solution(mesh):
    def local_sweep(t_blk, d_blk, oovv_blk, vvvv_blk, oooo_full, wd_blk, wx_blk):
        return sweep(t_blk, oovv_blk, vvvv_blk, oooo_full, wd_blk, wx_blk) / d_blk

    amp = P("row", "col")
    wide = P(None, "col")
    return jax.shard_map(local_sweep, mesh=mesh, in_specs=(amp, amp, amp, amp, P(), wide, wide), out_specs=amp, check_vma=False)
```

```python
import jax
import jax.numpy as jnp
from jax import lax
from jax.experimental import pallas as pl
from jax.experimental.pallas import tpu as pltpu
from jax.sharding import PartitionSpec as P

MESH = pl.DeviceIdType.MESH
F32 = jnp.float32
BF16 = jnp.bfloat16
NT = (((1,), (1,)), ((), ()))
TN = (((0,), (0,)), ((), ()))

OCC = 16
VIRT = 96
LANE = 128
PITCH = 104
STEP = 256


def _dev(c, r):
    return {"col": c, "row": r}


def _rcopy(src, dst, ssem, rsem, dev):
    return pltpu.make_async_remote_copy(src, dst, ssem, rsem, device_id=dev, device_id_type=MESH)


def sweep_kernel(t_hbm, oovv_hbm, v_hbm, oooo_hbm, wd_hbm, wx_hbm, out_ref,
                 t32, oovv, oooo, ww, tg, xp, xr, mfull, hole, t4, wd4, wxt, ubuf, vbuf_s, s4, st4,
                 smsg, pmsg, srecv, precv, rmsg, rrecv, vv, theirs, part, wxf,
                 lsem, gs, gr, fs, fr, xs, xrs, ms, mrs, ss, srs, ps, prs, rls, rlr, vsem, rs, rrs):
    r, c = lax.axis_index("row"), lax.axis_index("col")
    x, y = c % 2, c // 2
    o = 1 - r
    nx, ny, dg = y * 2 + (1 - x), (1 - y) * 2 + x, (1 - y) * 2 + (1 - x)
    n, w = t32.shape
    h = w // 2
    h0, h1 = pl.ds(0, h), pl.ds(h, h)
    rows = pl.ds(pl.multiple_of(r * n, n), n)
    orows = pl.ds(pl.multiple_of(o * n, n), n)

    chunk = n // 4
    tloads = [pltpu.make_async_copy(t_hbm.at[pl.ds(k * chunk, chunk)], t32.at[pl.ds(k * chunk, chunk)], lsem.at[k])
              for k in range(4)]
    for cp in tloads:
        cp.start()
    oload = pltpu.make_async_copy(oovv_hbm, oovv, lsem.at[4])
    hload = pltpu.make_async_copy(oooo_hbm, oooo, lsem.at[5])
    wloads = [pltpu.make_async_copy(a, ww.at[k], lsem.at[6]) for k, a in enumerate((wd_hbm, wx_hbm))]
    for cp in (*wloads, oload, hload):
        cp.start()

    own = c // 2
    half = c % 2
    home = (own + r + 1) % 2
    via = home * nx + (1 - home) * ny
    past = home * ny + (1 - home) * nx
    ro = (home + half) % 2
    di = 1 - ro

    def slot_s(chip, ih, m):
        return pl.ds(pl.multiple_of(((chip * 2 + ih) * 2 + m) * 8, 8), 8)

    def slot_p(kind, a, ih, m):
        return ((kind * 2 + a) * 2 + ih) * 2 + m

    zero8 = jnp.zeros((8, w), F32)
    for m in range(2):
        srecv[slot_s(dg, ro, m), :] = zero8
        precv[slot_p(0, 1 - half, half, m)] = zero8
        precv[slot_p(1, 1 - half, 1 - half, m)] = zero8

    sem = pltpu.get_barrier_semaphore()
    for cc, rr in ((nx, r), (ny, r), (dg, r), (c, o), (nx, o), (ny, o), (dg, o)):
        pl.semaphore_signal(sem, inc=1, device_id=_dev(cc, rr), device_id_type=MESH)

    def vcopy(s, slot):
        lanes = pl.ds(pl.multiple_of(s * STEP, STEP), STEP)
        return pltpu.make_async_copy(v_hbm.at[:, lanes], vv.at[slot], vsem.at[slot])

    def landed(like, sem):
        return pltpu.make_async_copy(like, like, sem)

    for k in range(4):
        tloads[k].wait()
        tg[c, pl.ds(pl.multiple_of(r * n + k * chunk, chunk), chunk), :] = t32[k * chunk:(k + 1) * chunk, :].astype(BF16)

    pl.semaphore_wait(sem, 7)

    def tcopy(chip, lanes, k, dev):
        ref = tg.at[chip, rows, lanes]
        return _rcopy(ref, ref, gs, gr.at[k], dev)

    def fcopy(chip, lanes, p, dev):
        ref = tg.at[chip, pl.ds(pl.multiple_of(r * n + p * 32, 32), 32), lanes]
        return _rcopy(ref, ref, fs, fr.at[p], dev)

    whole = pl.ds(0, w)
    x0 = tcopy(c, h0, 1, _dev(nx, r))
    y1 = tcopy(c, h1, 2, _dev(ny, r))
    d_own = tcopy(c, whole, 0, _dev(c, o))
    x1 = tcopy(c, h1, 3, _dev(nx, r))
    y0 = tcopy(c, h0, 4, _dev(ny, r))
    x0.start()
    y1.start()
    d_own.start()
    x1.start()
    y0.start()
    vcopy(0, 0).start()
    vcopy(1, 1).start()

    def spread_rows(chip, ib, first, groups):
        for g in range(first, first + groups):
            tile = tg[chip, pl.ds(pl.multiple_of(r * n + ib * 16, 16), 16), g * 384:(g + 1) * 384].astype(F32)
            for e in range(4):
                slab = tile[:, e * VIRT:(e + 1) * VIRT]
                slab = jnp.concatenate([slab, jnp.zeros((16, LANE - VIRT), F32)], axis=1)
                for half in range(2):
                    start = (ib * 16 + half * 8) * PITCH + chip * 24 + g * 4 + e
                    t4[pl.ds(start, 8, stride=PITCH), :] = slab[half * 8:half * 8 + 8]

    def spread(chip, first, groups):
        @pl.loop(0, n // 16)
        def _(ib):
            spread_rows(chip, ib, first, groups)

    spread(c, 0, 6)

    landed(ww, lsem.at[6]).wait()
    zrow = jnp.zeros((LANE - VIRT, 4 * LANE), BF16)

    @pl.loop(0, OCC)
    def _(k):
        blk = ww[0, pl.ds(pl.multiple_of(k * VIRT, 16), VIRT), :].astype(F32)
        parts = []
        for j in range(4):
            parts += [blk[:, j * VIRT:(j + 1) * VIRT], jnp.zeros((VIRT, LANE - VIRT), F32)]
        wd4[pl.ds(pl.multiple_of(k * LANE, LANE), VIRT), :] = jnp.concatenate(parts, axis=1).astype(BF16)
        wd4[pl.ds(pl.multiple_of(k * LANE + VIRT, 32), LANE - VIRT), :] = zrow
        wxf[pl.ds(pl.multiple_of(k * VIRT, 16), VIRT), :] = ww[1, pl.ds(pl.multiple_of(k * VIRT, 16), VIRT), :].astype(F32)

    for s, chip in enumerate((c, nx, ny, dg)):
        for b in range(3):
            blk = jnp.concatenate(
                [wxf[pl.ds(pl.multiple_of(k * VIRT + chip * 24, 8), 24), b * LANE:(b + 1) * LANE] for k in range(OCC)],
                axis=0)
            wxt[b * LANE:(b + 1) * LANE, s * 384:(s + 1) * 384] = blk.astype(BF16).T

    oload.wait()
    hload.wait()
    d_own.wait_recv()
    xp[...] = lax.dot_general(oovv[...], tg[c], NT, preferred_element_type=F32)

    def direct_rows(chip, i0, count):
        lhs = jnp.concatenate(
            [jnp.concatenate(
                [t4[pl.ds(pl.multiple_of(((i0 + i) * OCC + k) * PITCH + chip * 24, 8), 24), :] for i in range(count)],
                axis=0)
             for k in range(OCC)], axis=1).astype(BF16)
        return jnp.dot(lhs, wd4[...], preferred_element_type=F32)

    def direct(chip):
        ubuf[chip, :, :] = direct_rows(chip, 0, 8)

    def exchange_pair(chips, first, i2):
        halves = []
        for e in range(2):
            halves.append(jnp.concatenate(
                [t4[pl.ds(pl.multiple_of(((2 * i2 + e) * OCC + k) * PITCH + chip * 24, 8), 24), :]
                 for chip in chips for k in range(OCC)], axis=0))
        rhs = jnp.concatenate(halves, axis=1).astype(BF16)
        prod = jnp.dot(wxt[:, first * 384:(first + len(chips)) * 384], rhs, preferred_element_type=F32)
        vbuf_s[i2, :, :] = prod if first == 0 else vbuf_s[i2, :, :] + prod

    def exchange(chips, first):
        @pl.loop(0, 4)
        def _(i2):
            exchange_pair(chips, first, i2)

    direct(c)

    x0.wait_recv()
    for p in range(4):
        fcopy(nx, h0, p, _dev(ny, r)).start()
    y1.wait_recv()
    for p in range(4):
        fcopy(ny, h1, p, _dev(nx, r)).start()
    q = n // 4
    for cc in (nx, ny, dg):
        cp = _rcopy(xp.at[pl.ds(pl.multiple_of(cc * q, q), q)], xr.at[c], xs, xrs, _dev(cc, r))
        cp.start()
    xr[c, :, :] = xp[pl.ds(pl.multiple_of(c * q, q), q), :]
    spread(nx, 0, 3)
    spread(ny, 3, 3)
    x1.wait_recv()
    d_x = tcopy(nx, whole, 5, _dev(c, o))
    d_x.start()
    y0.wait_recv()
    d_y = tcopy(ny, whole, 5, _dev(c, o))
    d_y.start()
    spread(nx, 3, 3)
    spread(ny, 0, 3)
    direct(nx)
    direct(ny)
    exchange((c, nx, ny), 0)

    def s_rows(i, j):
        return pl.ds(pl.multiple_of((i * 4 + j) * PITCH, 8), VIRT)

    def t_rows(i, j):
        return pl.ds(pl.multiple_of(((i // 4) * 16 + j * 4 + i % 4) * PITCH, 8), VIRT)

    def block(i, j):
        direct_part = jnp.concatenate(
            [ubuf[chip, pl.ds(pl.multiple_of(i * 24, 8), 24), pl.ds(pl.multiple_of(j * LANE, LANE), LANE)]
             for chip in range(4)], axis=0)
        return direct_part - vbuf_s[
            i // 2, pl.ds(pl.multiple_of(j * VIRT, 8), VIRT), pl.ds(pl.multiple_of((i % 2) * LANE, LANE), LANE)]

    def fill_s(ih):
        @pl.loop(0, 4)
        def _(j):
            for e in range(4):
                s4[s_rows(ih * 4 + e, j), :] = block(ih * 4 + e, j)

    def fill_t(ih):
        @pl.loop(0, 4)
        def _(j):
            for e in range(4):
                st4[t_rows(ih * 4 + e, j), :VIRT] = s4[s_rows(ih * 4 + e, j), :].T[:VIRT, :]

    def put(src, ih, m, chip, dst):
        first = (ih * 16 + m * 8) * PITCH + chip * 24
        for g in range(6):
            vals = [src[pl.ds(first + g * 4 + e, 8, stride=PITCH), :][:, :VIRT] for e in range(4)]
            dst[:, g * 384:(g + 1) * 384] = jnp.concatenate(vals, axis=1)

    def s_copy(slot, ih, m, chip):
        buf = smsg.at[slot * 4 + ih * 2 + m]
        return _rcopy(buf, srecv.at[slot_s(c, ih, m)], ss, srs, _dev(chip, r))

    def p_copy(slot, ih, m, chip):
        buf = pmsg.at[slot * 4 + ih * 2 + m]
        return _rcopy(buf, precv.at[slot_p(1 - home, half, ih, m)], ps, prs, _dev(chip, own))

    def relay(kind, src):
        @pl.loop(0, 2)
        def _(m):
            put(src, ro, m, dg, rmsg.at[kind * 2 + m])
            to = rrecv.at[pl.ds(pl.multiple_of((kind * 2 + m) * 8, 8), 8)]
            _rcopy(rmsg.at[kind * 2 + m], to, rls, rlr, _dev(via, own)).start()

    def send(src, msg, copy, slot, ih, chip):
        @pl.loop(0, 2)
        def _(m):
            put(src, ih, m, chip, msg.at[slot * 4 + ih * 2 + m])
            copy(slot, ih, m, chip).start()

    def mirror():
        @pl.loop(0, 4)
        def _(j):
            for e in range(4):
                at = s_rows(half * 4 + e, j)
                s4[at, :VIRT] = s4[at, :VIRT] + block(half * 4 + j, e).T[:VIRT, :]

    @pl.loop(0, 4)
    def _(p):
        landed(tg.at[dg, pl.ds(0, n // 4)], fr.at[p]).wait()
        for ib in range(2):
            spread_rows(dg, 2 * p + ib, 0, 6)
        ubuf[dg, pl.ds(pl.multiple_of(p * 48, 16), 48), :] = direct_rows(dg, 2 * p, 2)
        exchange_pair((dg,), 3, p)

        @pl.when(p == 1)
        def _():
            fill_s(0)

            @pl.when(ro == 0)
            def _():
                relay(0, s4)

            @pl.when(ro == 1)
            def _():
                @pl.when(home == 1)
                def _():
                    mirror()

                send(s4, smsg, s_copy, 1, 0, via)

    d_d = tcopy(dg, whole, 5, _dev(c, o))
    d_d.start()

    fill_s(1)

    @pl.when(ro == 1)
    def _():
        relay(0, s4)

    fill_t(ro)
    relay(1, st4)

    landed(xr.at[pl.ds(0, 3)], xrs).wait()
    xsum = (xr[0] + xr[1]) + (xr[2] + xr[3])
    krows = pl.ds(pl.multiple_of(r * n + c * q, q), q)
    mfull[krows, :] = (oooo[krows, :].astype(F32) + 0.5 * xsum).astype(BF16)
    for cc, rr in ((nx, r), (ny, r), (dg, r), (c, o), (nx, o), (ny, o), (dg, o)):
        part_m = mfull.at[krows, pl.ds(pl.multiple_of(rr * n, n), n)]
        _rcopy(part_m, part_m, ms, mrs, _dev(cc, rr)).start()

    @pl.when(jnp.logical_and(home == 1, di == 1))
    def _():
        mirror()

    send(s4, smsg, s_copy, 2, di, past)
    send(s4, smsg, s_copy, 0, di, dg)

    @pl.when(home == 0)
    def _():
        fill_t(di)
        send(st4, pmsg, p_copy, 2, di, past)
        send(st4, pmsg, p_copy, 0, di, dg)
        send(st4, pmsg, p_copy, 3, ro, c)
        send(st4, pmsg, p_copy, 3, di, c)

    @pl.loop(0, 2)
    def _(m):
        for ih in range(2):
            put(s4, ih, m, c, srecv.at[slot_s(c, ih, m)])

    @pl.when(home == 1)
    def _():
        @pl.loop(0, 2)
        def _(m):
            put(st4, ro, m, c, precv.at[slot_p(0, half, ro, m)])

    def pass_on():
        landed(rrecv, rlr).wait()
        for kind, (src, msg, copy) in ((1, (s4, smsg, s_copy)), (0, (st4, pmsg, p_copy))):
            for m in range(2):
                buf = msg.at[2 * 4 + ro * 2 + m]
                put(src, ro, m, past, buf)
                buf[...] = buf[...] + rrecv[(kind * 2 + m) * 8:(kind * 2 + m + 1) * 8, :]
                copy(2, ro, m, past).start()

    landed(tg.at[pl.ds(0, 3), pl.ds(0, n)], gr.at[5]).wait()

    def ladder_copy(s):
        lanes = pl.ds(pl.multiple_of(s * STEP, STEP), STEP)
        return _rcopy(part.at[s, orows], theirs.at[:, lanes], rs, rrs, _dev(c, o))

    @pl.loop(0, w // STEP)
    def _(s):
        slot = s % 3

        @pl.when(s + 2 < w // STEP)
        def _():
            vcopy(s + 2, (s + 2) % 3).start()

        vcopy(s, slot).wait()
        va, vb = vv.at[slot, pl.ds(0, w)], vv.at[slot, pl.ds(w, w)]
        part[s, :, :] = (jnp.dot(tg[2 * r], va[...], preferred_element_type=F32)
                         + jnp.dot(tg[2 * r + 1], vb[...], preferred_element_type=F32))
        ladder_copy(s).start()

        @pl.when(s == 0)
        def _():
            send(s4, smsg, s_copy, 1, ro, via)

        @pl.when(jnp.logical_and(s == 1, di == 1))
        def _():
            send(s4, smsg, s_copy, 1, 1, via)

        @pl.when(s == 2)
        def _():
            send(st4, pmsg, p_copy, 1, ro, via)

        @pl.when(jnp.logical_and(s == 3, home == 0))
        def _():
            send(st4, pmsg, p_copy, 1, di, via)

        @pl.when(s == 5)
        def _():
            pass_on()

    landed(theirs, rrs).wait()
    landed(theirs, rs).wait()

    landed(tg.at[pl.ds(0, 3)], gs).wait()
    landed(tg.at[0, pl.ds(0, n)], fs).wait()
    landed(xr.at[pl.ds(0, 3)], xs).wait()
    all_m = mfull.at[pl.ds(0, 7 * q), pl.ds(0, n)]
    landed(all_m, mrs).wait()
    landed(all_m, ms).wait()
    m_mine = mfull[:, rows]

    @pl.loop(0, w // STEP)
    def _(s):
        lanes = pl.ds(pl.multiple_of(s * STEP, STEP), STEP)
        hole[:, lanes] = lax.dot_general(m_mine, tg[c, :, lanes], TN, preferred_element_type=F32)

    @pl.loop(0, 8)
    def _(i):
        line = pl.ds(pl.multiple_of(i * 16, 16), 16)
        line_r = pl.ds(pl.multiple_of(r * n + i * 16, 16), 16)
        mine = jnp.concatenate([part[s, line_r, :] for s in range(w // STEP)], axis=1)
        out_ref[line, :] = oovv[line, :].astype(F32) + (mine + theirs[line, :] + hole[line, :])

    landed(rmsg, rls).wait()
    landed(srecv.at[pl.ds(0, 80)], srs).wait()
    for i in range(8):
        for jh in range(2):
            line = slice(i * 16 + jh * 8, i * 16 + jh * 8 + 8)
            rows4 = [((2 * jh + cc) * 4 + i // 2) * 8 + i % 2 * 4 for cc in range(2)]
            out_ref[line, :] = out_ref[line, :] + jnp.concatenate([srecv[k:k + 4, :] for k in rows4], axis=0)

    @pl.when(home == 1)
    def _():
        landed(precv.at[pl.ds(0, 10)], prs).wait()

    @pl.when(home == 0)
    def _():
        landed(precv.at[pl.ds(0, 8)], prs).wait()

    zero4 = jnp.zeros((4, w), F32)
    for a in range(2):
        for j in range(4):
            m, rows4 = j // 2, slice(j % 2 * 4, j % 2 * 4 + 4)
            for kind, row in ((0, r), (1, o)):
                line = pl.ds(pl.multiple_of((a * 4 + j) * 16 + row * 8, 8), 8)
                both = [zero4 if kind == 0 and ih == a else precv[slot_p(kind, a, ih, m), rows4, :] for ih in range(2)]
                out_ref[line, :] = out_ref[line, :] + jnp.concatenate(both, axis=0)

    landed(smsg.at[pl.ds(0, 10)], ss).wait()

    @pl.when(home == 1)
    def _():
        landed(pmsg.at[pl.ds(0, 4)], ps).wait()

    @pl.when(home == 0)
    def _():
        landed(pmsg.at[pl.ds(0, 14)], ps).wait()


ANY = pl.BlockSpec(memory_space=pl.ANY)
DMA = pltpu.SemaphoreType.DMA


def sweep(t, oovv, vvvv, oooo, wd, wx):
    n, w = t.shape
    depth = vvvv.shape[0]
    V = pltpu.VMEM
    return pl.pallas_call(
        sweep_kernel,
        out_shape=jax.ShapeDtypeStruct((n, w), F32),
        in_specs=[ANY] * 6,
        out_specs=pl.BlockSpec(memory_space=pltpu.VMEM),
        scratch_shapes=[
            V((n, w), F32), V((n, w), BF16), V(oooo.shape, BF16), V((2,) + wd.shape, BF16),
            V((4, 2 * n, w), BF16),
            V((n, 2 * n), F32), V((4, n // 4, 2 * n), F32), V((2 * n, 2 * n), BF16), V((n, w), F32),
            V((n * PITCH, LANE), F32), V((OCC * LANE, 4 * LANE), BF16), V((wx.shape[1], wx.shape[0]), BF16),
            V((4, 2 * VIRT, 4 * LANE), F32), V((4, 4 * VIRT, 2 * LANE), F32),
            V((32 * PITCH, LANE), F32), V((32 * PITCH, LANE), F32),
            V((12, 8, w), F32), V((16, 8, w), F32), V((128, w), F32), V((16, 8, w), F32), V((4, 8, w), F32), V((32, w), F32),
            V((3, depth, STEP), BF16), V((n, w), F32), V((w // STEP, 2 * n, STEP), F32), V(wx.shape, F32),
            DMA((7,)), DMA, DMA((6,)), DMA, DMA((4,)), DMA, DMA, DMA, DMA,
            DMA, DMA, DMA, DMA, DMA, DMA, DMA((3,)), DMA, DMA,
        ],
        compiler_params=pltpu.CompilerParams(collective_id=0, has_side_effects=True, vmem_limit_bytes=46 << 20),
        name="sweep",
    )(*(pltpu.with_memory_space_constraint(a, pltpu.HBM) for a in (t, oovv, vvvv, oooo, wd, wx)))


def solution(mesh):
    def local_sweep(t_blk, d_blk, oovv_blk, vvvv_blk, oooo_full, wd_blk, wx_blk):
        return sweep(t_blk, oovv_blk, vvvv_blk, oooo_full, wd_blk, wx_blk) / d_blk

    amp = P("row", "col")
    wide = P(None, "col")
    return jax.shard_map(local_sweep, mesh=mesh, in_specs=(amp, amp, amp, amp, P(), wide, wide), out_specs=amp, check_vma=False)
```

```python
import jax
import jax.numpy as jnp
from jax import lax
from jax.experimental import pallas as pl
from jax.experimental.pallas import tpu as pltpu
from jax.sharding import PartitionSpec as P

MESH = pl.DeviceIdType.MESH
F32 = jnp.float32
BF16 = jnp.bfloat16
NT = (((1,), (1,)), ((), ()))
TN = (((0,), (0,)), ((), ()))

OCC = 16
VIRT = 96
LANE = 128
PITCH = 104
STEP = 256


def _dev(c, r):
    return {"col": c, "row": r}


def _rcopy(src, dst, ssem, rsem, dev):
    return pltpu.make_async_remote_copy(src, dst, ssem, rsem, device_id=dev, device_id_type=MESH)


def sweep_kernel(t_hbm, oovv_hbm, v_hbm, oooo_hbm, wd_hbm, wx_hbm, out_ref,
                 t32, oovv, oooo, ww, tg, xp, xr, mfull, hole, t4, wd4, wxt, ubuf, vbuf_s, s4, st4,
                 smsg, pmsg, srecv, precv, rmsg, rrecv, vv, theirs, part, wxf,
                 lsem, gs, gr, fs, fr, xs, xrs, ms, mrs, ss, srs, ps, prs, rls, rlr, vsem, rs, rrs):
    r, c = lax.axis_index("row"), lax.axis_index("col")
    x, y = c % 2, c // 2
    o = 1 - r
    nx, ny, dg = y * 2 + (1 - x), (1 - y) * 2 + x, (1 - y) * 2 + (1 - x)
    n, w = t32.shape
    h = w // 2
    h0, h1 = pl.ds(0, h), pl.ds(h, h)
    rows = pl.ds(pl.multiple_of(r * n, n), n)
    orows = pl.ds(pl.multiple_of(o * n, n), n)

    chunk = n // 4
    tloads = [pltpu.make_async_copy(t_hbm.at[pl.ds(k * chunk, chunk)], t32.at[pl.ds(k * chunk, chunk)], lsem.at[k])
              for k in range(4)]
    for cp in tloads:
        cp.start()
    oload = pltpu.make_async_copy(oovv_hbm, oovv, lsem.at[4])
    hload = pltpu.make_async_copy(oooo_hbm, oooo, lsem.at[5])
    wloads = [pltpu.make_async_copy(a, ww.at[k], lsem.at[6]) for k, a in enumerate((wd_hbm, wx_hbm))]

    own = c // 2
    half = c % 2
    home = (own + r + 1) % 2
    via = home * nx + (1 - home) * ny
    past = home * ny + (1 - home) * nx
    ro = (home + half) % 2
    di = 1 - ro

    def slot_s(chip, ih, m):
        return pl.ds(pl.multiple_of(((chip * 2 + ih) * 2 + m) * 8, 8), 8)

    def slot_p(kind, a, ih, m):
        return ((kind * 2 + a) * 2 + ih) * 2 + m

    zero8 = jnp.zeros((8, w), F32)
    for m in range(2):
        srecv[slot_s(dg, ro, m), :] = zero8
        precv[slot_p(0, 1 - half, half, m)] = zero8
        precv[slot_p(1, 1 - half, 1 - half, m)] = zero8

    sem = pltpu.get_barrier_semaphore()
    for cc, rr in ((nx, r), (ny, r), (dg, r), (c, o), (nx, o), (ny, o), (dg, o)):
        pl.semaphore_signal(sem, inc=1, device_id=_dev(cc, rr), device_id_type=MESH)

    def vcopy(s, slot):
        lanes = pl.ds(pl.multiple_of(s * STEP, STEP), STEP)
        return pltpu.make_async_copy(v_hbm.at[:, lanes], vv.at[slot], vsem.at[slot])

    def landed(like, sem):
        return pltpu.make_async_copy(like, like, sem)

    for k in range(4):
        tloads[k].wait()
        part_t = pl.ds(pl.multiple_of(r * n + k * chunk, chunk), chunk)
        tg[c, part_t, :] = t32[k * chunk:(k + 1) * chunk, :].astype(BF16)
        if k == 0:
            pl.semaphore_wait(sem, 7)
        for lanes, g, chip in ((h0, 1, nx), (h1, 2, ny)):
            ref = tg.at[c, part_t, lanes]
            _rcopy(ref, ref, gs, gr.at[g], _dev(chip, r)).start()

    for cp in (*wloads, oload, hload):
        cp.start()

    def tcopy(chip, lanes, k, dev):
        ref = tg.at[chip, rows, lanes]
        return _rcopy(ref, ref, gs, gr.at[k], dev)

    def fcopy(chip, lanes, p, dev):
        ref = tg.at[chip, pl.ds(pl.multiple_of(r * n + p * 32, 32), 32), lanes]
        return _rcopy(ref, ref, fs, fr.at[p], dev)

    whole = pl.ds(0, w)
    x0 = tcopy(c, h0, 1, _dev(nx, r))
    y1 = tcopy(c, h1, 2, _dev(ny, r))
    d_own = tcopy(c, whole, 0, _dev(c, o))
    x1 = tcopy(c, h1, 3, _dev(nx, r))
    y0 = tcopy(c, h0, 4, _dev(ny, r))
    d_own.start()
    x1.start()
    y0.start()
    vcopy(0, 0).start()
    vcopy(1, 1).start()

    def spread_rows(chip, ib, first, groups):
        for g in range(first, first + groups):
            tile = tg[chip, pl.ds(pl.multiple_of(r * n + ib * 16, 16), 16), g * 384:(g + 1) * 384].astype(F32)
            for e in range(4):
                slab = tile[:, e * VIRT:(e + 1) * VIRT]
                slab = jnp.concatenate([slab, jnp.zeros((16, LANE - VIRT), F32)], axis=1)
                for half in range(2):
                    start = (ib * 16 + half * 8) * PITCH + chip * 24 + g * 4 + e
                    t4[pl.ds(start, 8, stride=PITCH), :] = slab[half * 8:half * 8 + 8]

    def spread(chip, first, groups):
        @pl.loop(0, n // 16)
        def _(ib):
            spread_rows(chip, ib, first, groups)

    spread(c, 0, 6)

    landed(ww, lsem.at[6]).wait()
    zrow = jnp.zeros((LANE - VIRT, 4 * LANE), BF16)

    @pl.loop(0, OCC)
    def _(k):
        blk = ww[0, pl.ds(pl.multiple_of(k * VIRT, 16), VIRT), :].astype(F32)
        parts = []
        for j in range(4):
            parts += [blk[:, j * VIRT:(j + 1) * VIRT], jnp.zeros((VIRT, LANE - VIRT), F32)]
        wd4[pl.ds(pl.multiple_of(k * LANE, LANE), VIRT), :] = jnp.concatenate(parts, axis=1).astype(BF16)
        wd4[pl.ds(pl.multiple_of(k * LANE + VIRT, 32), LANE - VIRT), :] = zrow
        wxf[pl.ds(pl.multiple_of(k * VIRT, 16), VIRT), :] = ww[1, pl.ds(pl.multiple_of(k * VIRT, 16), VIRT), :].astype(F32)

    for s, chip in enumerate((c, nx, ny, dg)):
        for b in range(3):
            blk = jnp.concatenate(
                [wxf[pl.ds(pl.multiple_of(k * VIRT + chip * 24, 8), 24), b * LANE:(b + 1) * LANE] for k in range(OCC)],
                axis=0)
            wxt[b * LANE:(b + 1) * LANE, s * 384:(s + 1) * 384] = blk.astype(BF16).T

    oload.wait()
    hload.wait()
    d_own.wait_recv()
    xp[...] = lax.dot_general(oovv[...], tg[c], NT, preferred_element_type=F32)

    def direct_rows(chip, i0, count):
        lhs = jnp.concatenate(
            [jnp.concatenate(
                [t4[pl.ds(pl.multiple_of(((i0 + i) * OCC + k) * PITCH + chip * 24, 8), 24), :] for i in range(count)],
                axis=0)
             for k in range(OCC)], axis=1).astype(BF16)
        return jnp.dot(lhs, wd4[...], preferred_element_type=F32)

    def direct(chip):
        ubuf[chip, :, :] = direct_rows(chip, 0, 8)

    def exchange_pair(chips, first, i2):
        halves = []
        for e in range(2):
            halves.append(jnp.concatenate(
                [t4[pl.ds(pl.multiple_of(((2 * i2 + e) * OCC + k) * PITCH + chip * 24, 8), 24), :]
                 for chip in chips for k in range(OCC)], axis=0))
        rhs = jnp.concatenate(halves, axis=1).astype(BF16)
        prod = jnp.dot(wxt[:, first * 384:(first + len(chips)) * 384], rhs, preferred_element_type=F32)
        vbuf_s[i2, :, :] = prod if first == 0 else vbuf_s[i2, :, :] + prod

    def exchange(chips, first):
        @pl.loop(0, 4)
        def _(i2):
            exchange_pair(chips, first, i2)

    direct(c)

    x0.wait_recv()
    for p in range(4):
        fcopy(nx, h0, p, _dev(ny, r)).start()
    y1.wait_recv()
    for p in range(4):
        fcopy(ny, h1, p, _dev(nx, r)).start()
    q = n // 4
    for cc in (nx, ny, dg):
        cp = _rcopy(xp.at[pl.ds(pl.multiple_of(cc * q, q), q)], xr.at[c], xs, xrs, _dev(cc, r))
        cp.start()
    xr[c, :, :] = xp[pl.ds(pl.multiple_of(c * q, q), q), :]
    spread(nx, 0, 3)
    spread(ny, 3, 3)
    x1.wait_recv()
    d_x = tcopy(nx, whole, 5, _dev(c, o))
    d_x.start()
    y0.wait_recv()
    d_y = tcopy(ny, whole, 5, _dev(c, o))
    d_y.start()
    spread(nx, 3, 3)
    spread(ny, 0, 3)
    direct(nx)
    direct(ny)
    exchange((c, nx, ny), 0)

    def s_rows(i, j):
        return pl.ds(pl.multiple_of((i * 4 + j) * PITCH, 8), VIRT)

    def t_rows(i, j):
        return pl.ds(pl.multiple_of(((i // 4) * 16 + j * 4 + i % 4) * PITCH, 8), VIRT)

    def block(i, j):
        direct_part = jnp.concatenate(
            [ubuf[chip, pl.ds(pl.multiple_of(i * 24, 8), 24), pl.ds(pl.multiple_of(j * LANE, LANE), LANE)]
             for chip in range(4)], axis=0)
        return direct_part - vbuf_s[
            i // 2, pl.ds(pl.multiple_of(j * VIRT, 8), VIRT), pl.ds(pl.multiple_of((i % 2) * LANE, LANE), LANE)]

    def fill_s(ih):
        @pl.loop(0, 4)
        def _(j):
            for e in range(4):
                s4[s_rows(ih * 4 + e, j), :] = block(ih * 4 + e, j)

    def fill_t(ih):
        @pl.loop(0, 4)
        def _(j):
            for e in range(4):
                st4[t_rows(ih * 4 + e, j), :VIRT] = s4[s_rows(ih * 4 + e, j), :].T[:VIRT, :]

    def put(src, ih, m, chip, dst):
        first = (ih * 16 + m * 8) * PITCH + chip * 24
        for g in range(6):
            vals = [src[pl.ds(first + g * 4 + e, 8, stride=PITCH), :][:, :VIRT] for e in range(4)]
            dst[:, g * 384:(g + 1) * 384] = jnp.concatenate(vals, axis=1)

    def s_copy(slot, ih, m, chip):
        buf = smsg.at[slot * 4 + ih * 2 + m]
        return _rcopy(buf, srecv.at[slot_s(c, ih, m)], ss, srs, _dev(chip, r))

    def p_copy(slot, ih, m, chip):
        buf = pmsg.at[slot * 4 + ih * 2 + m]
        return _rcopy(buf, precv.at[slot_p(1 - home, half, ih, m)], ps, prs, _dev(chip, own))

    def relay(kind, src):
        @pl.loop(0, 2)
        def _(m):
            put(src, ro, m, dg, rmsg.at[kind * 2 + m])
            to = rrecv.at[pl.ds(pl.multiple_of((kind * 2 + m) * 8, 8), 8)]
            _rcopy(rmsg.at[kind * 2 + m], to, rls, rlr, _dev(via, own)).start()

    def send(src, msg, copy, slot, ih, chip):
        @pl.loop(0, 2)
        def _(m):
            put(src, ih, m, chip, msg.at[slot * 4 + ih * 2 + m])
            copy(slot, ih, m, chip).start()

    def mirror():
        @pl.loop(0, 4)
        def _(j):
            for e in range(4):
                at = s_rows(half * 4 + e, j)
                s4[at, :VIRT] = s4[at, :VIRT] + block(half * 4 + j, e).T[:VIRT, :]

    @pl.loop(0, 4)
    def _(p):
        landed(tg.at[dg, pl.ds(0, n // 4)], fr.at[p]).wait()
        for ib in range(2):
            spread_rows(dg, 2 * p + ib, 0, 6)
        ubuf[dg, pl.ds(pl.multiple_of(p * 48, 16), 48), :] = direct_rows(dg, 2 * p, 2)
        exchange_pair((dg,), 3, p)

        @pl.when(p == 1)
        def _():
            fill_s(0)

            @pl.when(ro == 0)
            def _():
                relay(0, s4)

            @pl.when(ro == 1)
            def _():
                @pl.when(home == 1)
                def _():
                    mirror()

                send(s4, smsg, s_copy, 1, 0, via)

    d_d = tcopy(dg, whole, 5, _dev(c, o))
    d_d.start()

    fill_s(1)

    @pl.when(ro == 1)
    def _():
        relay(0, s4)

    fill_t(ro)
    relay(1, st4)

    landed(xr.at[pl.ds(0, 3)], xrs).wait()
    xsum = (xr[0] + xr[1]) + (xr[2] + xr[3])
    krows = pl.ds(pl.multiple_of(r * n + c * q, q), q)
    mfull[krows, :] = (oooo[krows, :].astype(F32) + 0.5 * xsum).astype(BF16)
    for cc, rr in ((nx, r), (ny, r), (dg, r), (c, o), (nx, o), (ny, o), (dg, o)):
        part_m = mfull.at[krows, pl.ds(pl.multiple_of(rr * n, n), n)]
        _rcopy(part_m, part_m, ms, mrs, _dev(cc, rr)).start()

    @pl.when(jnp.logical_and(home == 1, di == 1))
    def _():
        mirror()

    early = via == 0
    late = jnp.logical_not(early)

    @pl.when(home == 0)
    def _():
        fill_t(di)

    @pl.when(early)
    def _():
        send(s4, smsg, s_copy, 1, ro, via)
        send(st4, pmsg, p_copy, 1, ro, via)

        @pl.when(di == 1)
        def _():
            send(s4, smsg, s_copy, 1, 1, via)

        @pl.when(home == 0)
        def _():
            send(st4, pmsg, p_copy, 1, di, via)

    @pl.when(late)
    def _():
        send(s4, smsg, s_copy, 0, di, dg)
        send(s4, smsg, s_copy, 2, di, past)

        @pl.when(home == 0)
        def _():
            send(st4, pmsg, p_copy, 0, di, dg)
            send(st4, pmsg, p_copy, 2, di, past)

    @pl.when(home == 0)
    def _():
        send(st4, pmsg, p_copy, 3, ro, c)
        send(st4, pmsg, p_copy, 3, di, c)

    @pl.loop(0, 2)
    def _(m):
        for ih in range(2):
            put(s4, ih, m, c, srecv.at[slot_s(c, ih, m)])

    @pl.when(home == 1)
    def _():
        @pl.loop(0, 2)
        def _(m):
            put(st4, ro, m, c, precv.at[slot_p(0, half, ro, m)])

    def pass_on():
        landed(rrecv, rlr).wait()
        for kind, (src, msg, copy) in ((1, (s4, smsg, s_copy)), (0, (st4, pmsg, p_copy))):
            for m in range(2):
                buf = msg.at[2 * 4 + ro * 2 + m]
                put(src, ro, m, past, buf)
                buf[...] = buf[...] + rrecv[(kind * 2 + m) * 8:(kind * 2 + m + 1) * 8, :]
                copy(2, ro, m, past).start()

    landed(tg.at[pl.ds(0, 3), pl.ds(0, n)], gr.at[5]).wait()

    def ladder_copy(s):
        lanes = pl.ds(pl.multiple_of(s * STEP, STEP), STEP)
        return _rcopy(part.at[s, orows], theirs.at[:, lanes], rs, rrs, _dev(c, o))

    @pl.loop(0, w // STEP)
    def _(s):
        slot = s % 3

        @pl.when(s + 2 < w // STEP)
        def _():
            vcopy(s + 2, (s + 2) % 3).start()

        vcopy(s, slot).wait()
        va, vb = vv.at[slot, pl.ds(0, w)], vv.at[slot, pl.ds(w, w)]
        part[s, :, :] = (jnp.dot(tg[2 * r], va[...], preferred_element_type=F32)
                         + jnp.dot(tg[2 * r + 1], vb[...], preferred_element_type=F32))
        ladder_copy(s).start()

        @pl.when(jnp.logical_and(s == 0, late))
        def _():
            send(s4, smsg, s_copy, 1, ro, via)

        @pl.when(jnp.logical_and(s == 1, jnp.logical_and(late, di == 1)))
        def _():
            send(s4, smsg, s_copy, 1, 1, via)

        @pl.when(jnp.logical_and(s == 2, late))
        def _():
            send(st4, pmsg, p_copy, 1, ro, via)

        @pl.when(jnp.logical_and(s == 3, jnp.logical_and(late, home == 0)))
        def _():
            send(st4, pmsg, p_copy, 1, di, via)

        @pl.when(jnp.logical_and(s == 0, early))
        def _():
            send(s4, smsg, s_copy, 2, di, past)
            send(s4, smsg, s_copy, 0, di, dg)

        @pl.when(jnp.logical_and(s == 1, jnp.logical_and(early, home == 0)))
        def _():
            send(st4, pmsg, p_copy, 2, di, past)
            send(st4, pmsg, p_copy, 0, di, dg)

        @pl.when(s == 5)
        def _():
            pass_on()

    landed(theirs, rrs).wait()
    landed(theirs, rs).wait()

    landed(tg.at[pl.ds(0, 3)], gs).wait()
    landed(tg.at[0, pl.ds(0, n)], fs).wait()
    landed(xr.at[pl.ds(0, 3)], xs).wait()
    all_m = mfull.at[pl.ds(0, 7 * q), pl.ds(0, n)]
    landed(all_m, mrs).wait()
    landed(all_m, ms).wait()
    m_mine = mfull[:, rows]

    @pl.loop(0, w // STEP)
    def _(s):
        lanes = pl.ds(pl.multiple_of(s * STEP, STEP), STEP)
        hole[:, lanes] = lax.dot_general(m_mine, tg[c, :, lanes], TN, preferred_element_type=F32)

    @pl.loop(0, 8)
    def _(i):
        line = pl.ds(pl.multiple_of(i * 16, 16), 16)
        line_r = pl.ds(pl.multiple_of(r * n + i * 16, 16), 16)
        mine = jnp.concatenate([part[s, line_r, :] for s in range(w // STEP)], axis=1)
        out_ref[line, :] = oovv[line, :].astype(F32) + (mine + theirs[line, :] + hole[line, :])

    landed(rmsg, rls).wait()
    landed(srecv.at[pl.ds(0, 80)], srs).wait()
    for i in range(8):
        for jh in range(2):
            line = slice(i * 16 + jh * 8, i * 16 + jh * 8 + 8)
            rows4 = [((2 * jh + cc) * 4 + i // 2) * 8 + i % 2 * 4 for cc in range(2)]
            out_ref[line, :] = out_ref[line, :] + jnp.concatenate([srecv[k:k + 4, :] for k in rows4], axis=0)

    @pl.when(home == 1)
    def _():
        landed(precv.at[pl.ds(0, 10)], prs).wait()

    @pl.when(home == 0)
    def _():
        landed(precv.at[pl.ds(0, 8)], prs).wait()

    zero4 = jnp.zeros((4, w), F32)
    for a in range(2):
        for j in range(4):
            m, rows4 = j // 2, slice(j % 2 * 4, j % 2 * 4 + 4)
            for kind, row in ((0, r), (1, o)):
                line = pl.ds(pl.multiple_of((a * 4 + j) * 16 + row * 8, 8), 8)
                both = [zero4 if kind == 0 and ih == a else precv[slot_p(kind, a, ih, m), rows4, :] for ih in range(2)]
                out_ref[line, :] = out_ref[line, :] + jnp.concatenate(both, axis=0)

    landed(smsg.at[pl.ds(0, 10)], ss).wait()

    @pl.when(home == 1)
    def _():
        landed(pmsg.at[pl.ds(0, 4)], ps).wait()

    @pl.when(home == 0)
    def _():
        landed(pmsg.at[pl.ds(0, 14)], ps).wait()


ANY = pl.BlockSpec(memory_space=pl.ANY)
DMA = pltpu.SemaphoreType.DMA


def sweep(t, oovv, vvvv, oooo, wd, wx):
    n, w = t.shape
    depth = vvvv.shape[0]
    V = pltpu.VMEM
    return pl.pallas_call(
        sweep_kernel,
        out_shape=jax.ShapeDtypeStruct((n, w), F32),
        in_specs=[ANY] * 6,
        out_specs=pl.BlockSpec(memory_space=pltpu.VMEM),
        scratch_shapes=[
            V((n, w), F32), V((n, w), BF16), V(oooo.shape, BF16), V((2,) + wd.shape, BF16),
            V((4, 2 * n, w), BF16),
            V((n, 2 * n), F32), V((4, n // 4, 2 * n), F32), V((2 * n, 2 * n), BF16), V((n, w), F32),
            V((n * PITCH, LANE), F32), V((OCC * LANE, 4 * LANE), BF16), V((wx.shape[1], wx.shape[0]), BF16),
            V((4, 2 * VIRT, 4 * LANE), F32), V((4, 4 * VIRT, 2 * LANE), F32),
            V((32 * PITCH, LANE), F32), V((32 * PITCH, LANE), F32),
            V((12, 8, w), F32), V((16, 8, w), F32), V((128, w), F32), V((16, 8, w), F32), V((4, 8, w), F32), V((32, w), F32),
            V((3, depth, STEP), BF16), V((n, w), F32), V((w // STEP, 2 * n, STEP), F32), V(wx.shape, F32),
            DMA((7,)), DMA, DMA((6,)), DMA, DMA((4,)), DMA, DMA, DMA, DMA,
            DMA, DMA, DMA, DMA, DMA, DMA, DMA((3,)), DMA, DMA,
        ],
        compiler_params=pltpu.CompilerParams(collective_id=0, has_side_effects=True, vmem_limit_bytes=46 << 20),
        name="sweep",
    )(*(pltpu.with_memory_space_constraint(a, pltpu.HBM) for a in (t, oovv, vvvv, oooo, wd, wx)))


def solution(mesh):
    def local_sweep(t_blk, d_blk, oovv_blk, vvvv_blk, oooo_full, wd_blk, wx_blk):
        return sweep(t_blk, oovv_blk, vvvv_blk, oooo_full, wd_blk, wx_blk) / d_blk

    amp = P("row", "col")
    wide = P(None, "col")
    return jax.shard_map(local_sweep, mesh=mesh, in_specs=(amp, amp, amp, amp, P(), wide, wide), out_specs=amp, check_vma=False)
```

```python
import jax
import jax.numpy as jnp
from jax import lax
from jax.experimental import pallas as pl
from jax.experimental.pallas import tpu as pltpu
from jax.sharding import PartitionSpec as P

MESH = pl.DeviceIdType.MESH
F32 = jnp.float32
BF16 = jnp.bfloat16
NT = (((1,), (1,)), ((), ()))
TN = (((0,), (0,)), ((), ()))

OCC = 16
VIRT = 96
LANE = 128
PITCH = 104
STEP = 256


def _dev(c, r):
    return {"col": c, "row": r}


def _rcopy(src, dst, ssem, rsem, dev):
    return pltpu.make_async_remote_copy(src, dst, ssem, rsem, device_id=dev, device_id_type=MESH)


def sweep_kernel(t_hbm, oovv_hbm, v_hbm, oooo_hbm, wd_hbm, wx_hbm, out_ref,
                 t32, oovv, oooo, ww, tg, xp, xr, mfull, hole, t4, wd4, wxt, ubuf, vbuf_s, s4, st4,
                 smsg, pmsg, srecv, precv, rmsg, rrecv, vv, theirs, part, wxf,
                 lsem, gs, gr, fs, fr, xs, xrs, ms, mrs, ss, srs, ps, prs, rls, rlr, vsem, rs, rrs):
    r, c = lax.axis_index("row"), lax.axis_index("col")
    x, y = c % 2, c // 2
    o = 1 - r
    nx, ny, dg = y * 2 + (1 - x), (1 - y) * 2 + x, (1 - y) * 2 + (1 - x)
    n, w = t32.shape
    h = w // 2
    h0, h1 = pl.ds(0, h), pl.ds(h, h)
    rows = pl.ds(pl.multiple_of(r * n, n), n)
    orows = pl.ds(pl.multiple_of(o * n, n), n)

    chunk = n // 4
    tloads = [pltpu.make_async_copy(t_hbm.at[pl.ds(k * chunk, chunk)], t32.at[pl.ds(k * chunk, chunk)], lsem.at[k])
              for k in range(4)]
    for cp in tloads:
        cp.start()
    oload = pltpu.make_async_copy(oovv_hbm, oovv, lsem.at[4])
    hload = pltpu.make_async_copy(oooo_hbm, oooo, lsem.at[5])
    wloads = [pltpu.make_async_copy(a, ww.at[k], lsem.at[6]) for k, a in enumerate((wd_hbm, wx_hbm))]

    own = c // 2
    half = c % 2
    home = (own + r + 1) % 2
    via = home * nx + (1 - home) * ny
    past = home * ny + (1 - home) * nx
    ro = (home + half) % 2
    di = 1 - ro

    def slot_s(chip, ih):
        return (chip * 2 + ih) * 2

    def slot_p(kind, a, ih):
        return ((kind * 2 + a) * 2 + ih) * 2

    zero8 = jnp.zeros((8, w), F32)
    for m in range(2):
        srecv[slot_s(dg, ro) + m] = zero8
        precv[slot_p(0, 1 - half, half) + m] = zero8
        precv[slot_p(1, 1 - half, 1 - half) + m] = zero8

    sem = pltpu.get_barrier_semaphore()
    for cc, rr in ((nx, r), (ny, r), (dg, r), (c, o), (nx, o), (ny, o), (dg, o)):
        pl.semaphore_signal(sem, inc=1, device_id=_dev(cc, rr), device_id_type=MESH)

    def vcopy(s, slot):
        lanes = pl.ds(pl.multiple_of(s * STEP, STEP), STEP)
        return pltpu.make_async_copy(v_hbm.at[:, lanes], vv.at[slot], vsem.at[slot])

    def landed(like, sem):
        return pltpu.make_async_copy(like, like, sem)

    for k in range(4):
        tloads[k].wait()
        part_t = pl.ds(pl.multiple_of(r * n + k * chunk, chunk), chunk)
        tg[c, part_t, :] = t32[k * chunk:(k + 1) * chunk, :].astype(BF16)
        if k == 0:
            pl.semaphore_wait(sem, 7)
        for lanes, g, chip in ((h0, 1, nx), (h1, 2, ny)):
            ref = tg.at[c, part_t, lanes]
            _rcopy(ref, ref, gs, gr.at[g], _dev(chip, r)).start()

    for cp in (*wloads, oload, hload):
        cp.start()

    def tcopy(chip, lanes, k, dev):
        ref = tg.at[chip, rows, lanes]
        return _rcopy(ref, ref, gs, gr.at[k], dev)

    def fcopy(chip, lanes, p, dev):
        ref = tg.at[chip, pl.ds(pl.multiple_of(r * n + p * 32, 32), 32), lanes]
        return _rcopy(ref, ref, fs, fr.at[p], dev)

    whole = pl.ds(0, w)
    x0 = tcopy(c, h0, 1, _dev(nx, r))
    y1 = tcopy(c, h1, 2, _dev(ny, r))
    d_own = tcopy(c, whole, 0, _dev(c, o))
    x1 = tcopy(c, h1, 3, _dev(nx, r))
    y0 = tcopy(c, h0, 4, _dev(ny, r))
    d_own.start()
    x1.start()
    y0.start()
    vcopy(0, 0).start()
    vcopy(1, 1).start()

    def spread_rows(chip, ib, first, groups):
        for g in range(first, first + groups):
            tile = tg[chip, pl.ds(pl.multiple_of(r * n + ib * 16, 16), 16), g * 384:(g + 1) * 384].astype(F32)
            for e in range(4):
                slab = tile[:, e * VIRT:(e + 1) * VIRT]
                slab = jnp.concatenate([slab, jnp.zeros((16, LANE - VIRT), F32)], axis=1)
                for half in range(2):
                    start = (ib * 16 + half * 8) * PITCH + chip * 24 + g * 4 + e
                    t4[pl.ds(start, 8, stride=PITCH), :] = slab[half * 8:half * 8 + 8]

    def spread(chip, first, groups):
        @pl.loop(0, n // 16)
        def _(ib):
            spread_rows(chip, ib, first, groups)

    spread(c, 0, 6)

    landed(ww, lsem.at[6]).wait()
    zrow = jnp.zeros((LANE - VIRT, 4 * LANE), BF16)

    @pl.loop(0, OCC)
    def _(k):
        blk = ww[0, pl.ds(pl.multiple_of(k * VIRT, 16), VIRT), :].astype(F32)
        parts = []
        for j in range(4):
            parts += [blk[:, j * VIRT:(j + 1) * VIRT], jnp.zeros((VIRT, LANE - VIRT), F32)]
        wd4[pl.ds(pl.multiple_of(k * LANE, LANE), VIRT), :] = jnp.concatenate(parts, axis=1).astype(BF16)
        wd4[pl.ds(pl.multiple_of(k * LANE + VIRT, 32), LANE - VIRT), :] = zrow
        wxf[pl.ds(pl.multiple_of(k * VIRT, 16), VIRT), :] = ww[1, pl.ds(pl.multiple_of(k * VIRT, 16), VIRT), :].astype(F32)

    for s, chip in enumerate((c, nx, ny, dg)):
        for b in range(3):
            blk = jnp.concatenate(
                [wxf[pl.ds(pl.multiple_of(k * VIRT + chip * 24, 8), 24), b * LANE:(b + 1) * LANE] for k in range(OCC)],
                axis=0)
            wxt[b * LANE:(b + 1) * LANE, s * 384:(s + 1) * 384] = blk.astype(BF16).T

    oload.wait()
    hload.wait()
    d_own.wait_recv()
    xp[...] = lax.dot_general(oovv[...], tg[c], NT, preferred_element_type=F32)

    def direct_rows(chip, i0, count):
        lhs = jnp.concatenate(
            [jnp.concatenate(
                [t4[pl.ds(pl.multiple_of(((i0 + i) * OCC + k) * PITCH + chip * 24, 8), 24), :] for i in range(count)],
                axis=0)
             for k in range(OCC)], axis=1).astype(BF16)
        return jnp.dot(lhs, wd4[...], preferred_element_type=F32)

    def direct(chip):
        ubuf[chip, :, :] = direct_rows(chip, 0, 8)

    def exchange_pair(chips, first, i2):
        halves = []
        for e in range(2):
            halves.append(jnp.concatenate(
                [t4[pl.ds(pl.multiple_of(((2 * i2 + e) * OCC + k) * PITCH + chip * 24, 8), 24), :]
                 for chip in chips for k in range(OCC)], axis=0))
        rhs = jnp.concatenate(halves, axis=1).astype(BF16)
        prod = jnp.dot(wxt[:, first * 384:(first + len(chips)) * 384], rhs, preferred_element_type=F32)
        vbuf_s[i2, :, :] = prod if first == 0 else vbuf_s[i2, :, :] + prod

    def exchange(chips, first):
        @pl.loop(0, 4)
        def _(i2):
            exchange_pair(chips, first, i2)

    direct(c)

    x0.wait_recv()
    for p in range(4):
        fcopy(nx, h0, p, _dev(ny, r)).start()
    y1.wait_recv()
    for p in range(4):
        fcopy(ny, h1, p, _dev(nx, r)).start()
    q = n // 4
    for cc in (nx, ny, dg):
        cp = _rcopy(xp.at[pl.ds(pl.multiple_of(cc * q, q), q)], xr.at[c], xs, xrs, _dev(cc, r))
        cp.start()
    xr[c, :, :] = xp[pl.ds(pl.multiple_of(c * q, q), q), :]
    spread(nx, 0, 3)
    spread(ny, 3, 3)
    x1.wait_recv()
    d_x = tcopy(nx, whole, 5, _dev(c, o))
    d_x.start()
    y0.wait_recv()
    d_y = tcopy(ny, whole, 5, _dev(c, o))
    d_y.start()
    spread(nx, 3, 3)
    spread(ny, 0, 3)
    direct(nx)
    direct(ny)
    exchange((c, nx, ny), 0)

    def s_rows(i, j):
        return pl.ds(pl.multiple_of((i * 4 + j) * PITCH, 8), VIRT)

    def t_rows(i, j):
        return pl.ds(pl.multiple_of(((i // 4) * 16 + j * 4 + i % 4) * PITCH, 8), VIRT)

    def block(i, j):
        direct_part = jnp.concatenate(
            [ubuf[chip, pl.ds(pl.multiple_of(i * 24, 8), 24), pl.ds(pl.multiple_of(j * LANE, LANE), LANE)]
             for chip in range(4)], axis=0)
        return direct_part - vbuf_s[
            i // 2, pl.ds(pl.multiple_of(j * VIRT, 8), VIRT), pl.ds(pl.multiple_of((i % 2) * LANE, LANE), LANE)]

    def fill_s(ih):
        @pl.loop(0, 4)
        def _(j):
            for e in range(4):
                s4[s_rows(ih * 4 + e, j), :] = block(ih * 4 + e, j)

    def fill_t(ih):
        @pl.loop(0, 4)
        def _(j):
            for e in range(4):
                st4[t_rows(ih * 4 + e, j), :VIRT] = s4[s_rows(ih * 4 + e, j), :].T[:VIRT, :]

    def put(src, ih, m, chip, dst):
        first = (ih * 16 + m * 8) * PITCH + chip * 24
        for g in range(6):
            vals = [src[pl.ds(first + g * 4 + e, 8, stride=PITCH), :][:, :VIRT] for e in range(4)]
            dst[:, g * 384:(g + 1) * 384] = jnp.concatenate(vals, axis=1)

    def s_copy(slot, ih, chip):
        buf = smsg.at[pl.ds(slot * 4 + ih * 2, 2)]
        return _rcopy(buf, srecv.at[pl.ds(slot_s(c, ih), 2)], ss, srs, _dev(chip, r))

    def p_copy(slot, ih, chip):
        buf = pmsg.at[pl.ds(slot * 4 + ih * 2, 2)]
        return _rcopy(buf, precv.at[pl.ds(slot_p(1 - home, half, ih), 2)], ps, prs, _dev(chip, own))

    def relay(kind, src):
        @pl.loop(0, 2)
        def _(m):
            put(src, ro, m, dg, rmsg.at[kind * 2 + m])

        pair = pl.ds(kind * 2, 2)
        _rcopy(rmsg.at[pair], rrecv.at[pair], rls, rlr, _dev(via, own)).start()

    def send(src, msg, copy, slot, ih, chip):
        @pl.loop(0, 2)
        def _(m):
            put(src, ih, m, chip, msg.at[slot * 4 + ih * 2 + m])

        copy(slot, ih, chip).start()

    def mirror():
        @pl.loop(0, 4)
        def _(j):
            for e in range(4):
                at = s_rows(half * 4 + e, j)
                s4[at, :VIRT] = s4[at, :VIRT] + block(half * 4 + j, e).T[:VIRT, :]

    @pl.loop(0, 4)
    def _(p):
        landed(tg.at[dg, pl.ds(0, n // 4)], fr.at[p]).wait()
        for ib in range(2):
            spread_rows(dg, 2 * p + ib, 0, 6)
        ubuf[dg, pl.ds(pl.multiple_of(p * 48, 16), 48), :] = direct_rows(dg, 2 * p, 2)
        exchange_pair((dg,), 3, p)

        @pl.when(p == 1)
        def _():
            fill_s(0)

            @pl.when(ro == 0)
            def _():
                relay(0, s4)

            @pl.when(ro == 1)
            def _():
                @pl.when(home == 1)
                def _():
                    mirror()

                send(s4, smsg, s_copy, 1, 0, via)

    d_d = tcopy(dg, whole, 5, _dev(c, o))
    d_d.start()

    fill_s(1)

    @pl.when(ro == 1)
    def _():
        relay(0, s4)

    fill_t(ro)
    relay(1, st4)

    landed(xr.at[pl.ds(0, 3)], xrs).wait()
    xsum = (xr[0] + xr[1]) + (xr[2] + xr[3])
    krows = pl.ds(pl.multiple_of(r * n + c * q, q), q)
    mfull[krows, :] = (oooo[krows, :].astype(F32) + 0.5 * xsum).astype(BF16)
    for cc, rr in ((nx, r), (ny, r), (dg, r), (c, o), (nx, o), (ny, o), (dg, o)):
        part_m = mfull.at[krows, pl.ds(pl.multiple_of(rr * n, n), n)]
        _rcopy(part_m, part_m, ms, mrs, _dev(cc, rr)).start()

    @pl.when(jnp.logical_and(home == 1, di == 1))
    def _():
        mirror()

    send(s4, smsg, s_copy, 2, di, past)
    send(s4, smsg, s_copy, 0, di, dg)

    @pl.when(home == 0)
    def _():
        fill_t(di)
        send(st4, pmsg, p_copy, 2, di, past)
        send(st4, pmsg, p_copy, 0, di, dg)
        send(st4, pmsg, p_copy, 3, ro, c)
        send(st4, pmsg, p_copy, 3, di, c)

    @pl.loop(0, 2)
    def _(m):
        for ih in range(2):
            put(s4, ih, m, c, srecv.at[slot_s(c, ih) + m])

    @pl.when(home == 1)
    def _():
        @pl.loop(0, 2)
        def _(m):
            put(st4, ro, m, c, precv.at[slot_p(0, half, ro) + m])

    def pass_on():
        landed(rrecv, rlr).wait()
        for kind, (src, msg, copy) in ((1, (s4, smsg, s_copy)), (0, (st4, pmsg, p_copy))):
            for m in range(2):
                buf = msg.at[2 * 4 + ro * 2 + m]
                put(src, ro, m, past, buf)
                buf[...] = buf[...] + rrecv[kind * 2 + m]
            copy(2, ro, past).start()

    landed(tg.at[pl.ds(0, 3), pl.ds(0, n)], gr.at[5]).wait()

    def ladder_copy(s):
        lanes = pl.ds(pl.multiple_of(s * STEP, STEP), STEP)
        return _rcopy(part.at[s, orows], theirs.at[:, lanes], rs, rrs, _dev(c, o))

    @pl.loop(0, w // STEP)
    def _(s):
        slot = s % 3

        @pl.when(s + 2 < w // STEP)
        def _():
            vcopy(s + 2, (s + 2) % 3).start()

        vcopy(s, slot).wait()
        va, vb = vv.at[slot, pl.ds(0, w)], vv.at[slot, pl.ds(w, w)]
        part[s, :, :] = (jnp.dot(tg[2 * r], va[...], preferred_element_type=F32)
                         + jnp.dot(tg[2 * r + 1], vb[...], preferred_element_type=F32))
        ladder_copy(s).start()

        @pl.when(s == 0)
        def _():
            send(s4, smsg, s_copy, 1, ro, via)

        @pl.when(jnp.logical_and(s == 1, di == 1))
        def _():
            send(s4, smsg, s_copy, 1, 1, via)

        @pl.when(s == 2)
        def _():
            send(st4, pmsg, p_copy, 1, ro, via)

        @pl.when(jnp.logical_and(s == 3, home == 0))
        def _():
            send(st4, pmsg, p_copy, 1, di, via)

        @pl.when(s == 5)
        def _():
            pass_on()

    landed(theirs, rrs).wait()
    landed(theirs, rs).wait()

    landed(tg.at[pl.ds(0, 3)], gs).wait()
    landed(tg.at[0, pl.ds(0, n)], fs).wait()
    landed(xr.at[pl.ds(0, 3)], xs).wait()
    all_m = mfull.at[pl.ds(0, 7 * q), pl.ds(0, n)]
    landed(all_m, mrs).wait()
    landed(all_m, ms).wait()
    m_mine = mfull[:, rows]

    @pl.loop(0, w // STEP)
    def _(s):
        lanes = pl.ds(pl.multiple_of(s * STEP, STEP), STEP)
        hole[:, lanes] = lax.dot_general(m_mine, tg[c, :, lanes], TN, preferred_element_type=F32)

    @pl.loop(0, 8)
    def _(i):
        line = pl.ds(pl.multiple_of(i * 16, 16), 16)
        line_r = pl.ds(pl.multiple_of(r * n + i * 16, 16), 16)
        mine = jnp.concatenate([part[s, line_r, :] for s in range(w // STEP)], axis=1)
        out_ref[line, :] = oovv[line, :].astype(F32) + (mine + theirs[line, :] + hole[line, :])

    landed(rmsg, rls).wait()
    landed(srecv.at[pl.ds(0, 10)], srs).wait()
    for i in range(8):
        for jh in range(2):
            line = slice(i * 16 + jh * 8, i * 16 + jh * 8 + 8)
            rows4 = slice(i % 2 * 4, i % 2 * 4 + 4)
            both = [srecv[(2 * jh + cc) * 4 + i // 2, rows4, :] for cc in range(2)]
            out_ref[line, :] = out_ref[line, :] + jnp.concatenate(both, axis=0)

    @pl.when(home == 1)
    def _():
        landed(precv.at[pl.ds(0, 10)], prs).wait()

    @pl.when(home == 0)
    def _():
        landed(precv.at[pl.ds(0, 8)], prs).wait()

    zero4 = jnp.zeros((4, w), F32)
    for a in range(2):
        for j in range(4):
            m, rows4 = j // 2, slice(j % 2 * 4, j % 2 * 4 + 4)
            for kind, row in ((0, r), (1, o)):
                line = pl.ds(pl.multiple_of((a * 4 + j) * 16 + row * 8, 8), 8)
                both = [zero4 if kind == 0 and ih == a else precv[slot_p(kind, a, ih) + m, rows4, :] for ih in range(2)]
                out_ref[line, :] = out_ref[line, :] + jnp.concatenate(both, axis=0)

    landed(smsg.at[pl.ds(0, 10)], ss).wait()

    @pl.when(home == 1)
    def _():
        landed(pmsg.at[pl.ds(0, 4)], ps).wait()

    @pl.when(home == 0)
    def _():
        landed(pmsg.at[pl.ds(0, 14)], ps).wait()


ANY = pl.BlockSpec(memory_space=pl.ANY)
DMA = pltpu.SemaphoreType.DMA


def sweep(t, oovv, vvvv, oooo, wd, wx):
    n, w = t.shape
    depth = vvvv.shape[0]
    V = pltpu.VMEM
    return pl.pallas_call(
        sweep_kernel,
        out_shape=jax.ShapeDtypeStruct((n, w), F32),
        in_specs=[ANY] * 6,
        out_specs=pl.BlockSpec(memory_space=pltpu.VMEM),
        scratch_shapes=[
            V((n, w), F32), V((n, w), BF16), V(oooo.shape, BF16), V((2,) + wd.shape, BF16),
            V((4, 2 * n, w), BF16),
            V((n, 2 * n), F32), V((4, n // 4, 2 * n), F32), V((2 * n, 2 * n), BF16), V((n, w), F32),
            V((n * PITCH, LANE), F32), V((OCC * LANE, 4 * LANE), BF16), V((wx.shape[1], wx.shape[0]), BF16),
            V((4, 2 * VIRT, 4 * LANE), F32), V((4, 4 * VIRT, 2 * LANE), F32),
            V((32 * PITCH, LANE), F32), V((32 * PITCH, LANE), F32),
            V((12, 8, w), F32), V((16, 8, w), F32), V((16, 8, w), F32), V((16, 8, w), F32), V((4, 8, w), F32), V((4, 8, w), F32),
            V((3, depth, STEP), BF16), V((n, w), F32), V((w // STEP, 2 * n, STEP), F32), V(wx.shape, F32),
            DMA((7,)), DMA, DMA((6,)), DMA, DMA((4,)), DMA, DMA, DMA, DMA,
            DMA, DMA, DMA, DMA, DMA, DMA, DMA((3,)), DMA, DMA,
        ],
        compiler_params=pltpu.CompilerParams(collective_id=0, has_side_effects=True, vmem_limit_bytes=46 << 20),
        name="sweep",
    )(*(pltpu.with_memory_space_constraint(a, pltpu.HBM) for a in (t, oovv, vvvv, oooo, wd, wx)))


def solution(mesh):
    def local_sweep(t_blk, d_blk, oovv_blk, vvvv_blk, oooo_full, wd_blk, wx_blk):
        return sweep(t_blk, oovv_blk, vvvv_blk, oooo_full, wd_blk, wx_blk) / d_blk

    amp = P("row", "col")
    wide = P(None, "col")
    return jax.shard_map(local_sweep, mesh=mesh, in_specs=(amp, amp, amp, amp, P(), wide, wide), out_specs=amp, check_vma=False)
```

```python
import jax
import jax.numpy as jnp
from jax import lax
from jax.experimental import pallas as pl
from jax.experimental.pallas import tpu as pltpu
from jax.sharding import PartitionSpec as P

MESH = pl.DeviceIdType.MESH
F32 = jnp.float32
BF16 = jnp.bfloat16
NT = (((1,), (1,)), ((), ()))
TN = (((0,), (0,)), ((), ()))

OCC = 16
VIRT = 96
LANE = 128
PITCH = 104
STEP = 256


def _dev(c, r):
    return {"col": c, "row": r}


def _rcopy(src, dst, ssem, rsem, dev):
    return pltpu.make_async_remote_copy(src, dst, ssem, rsem, device_id=dev, device_id_type=MESH)


def sweep_kernel(t_hbm, oovv_hbm, v_hbm, oooo_hbm, wd_hbm, wx_hbm, out_ref,
                 t32, oovv, oooo, ww, tg, xp, xr, mfull, hole, t4, wd4, wxt, ubuf, vbuf_s, s4, st4,
                 smsg, pmsg, srecv, precv, rmsg, rrecv, vv, theirs, part, wxf,
                 lsem, gs, gr, fs, fr, xs, xrs, ms, mrs, ss, srs, ps, prs, rls, rlr, vsem, rs, rrs):
    r, c = lax.axis_index("row"), lax.axis_index("col")
    x, y = c % 2, c // 2
    o = 1 - r
    nx, ny, dg = y * 2 + (1 - x), (1 - y) * 2 + x, (1 - y) * 2 + (1 - x)
    n, w = t32.shape
    h = w // 2
    h0, h1 = pl.ds(0, h), pl.ds(h, h)
    rows = pl.ds(pl.multiple_of(r * n, n), n)
    orows = pl.ds(pl.multiple_of(o * n, n), n)

    sem = pltpu.get_barrier_semaphore()
    for cc, rr in ((nx, r), (ny, r), (dg, r), (c, o), (nx, o), (ny, o), (dg, o)):
        pl.semaphore_signal(sem, inc=1, device_id=_dev(cc, rr), device_id_type=MESH)

    chunk = n // 4
    tloads = [pltpu.make_async_copy(t_hbm.at[pl.ds(k * chunk, chunk)], t32.at[pl.ds(k * chunk, chunk)], lsem.at[k])
              for k in range(4)]
    for cp in tloads:
        cp.start()
    oload = pltpu.make_async_copy(oovv_hbm, oovv, lsem.at[4])
    hload = pltpu.make_async_copy(oooo_hbm, oooo, lsem.at[5])
    wloads = [pltpu.make_async_copy(a, ww.at[k], lsem.at[6]) for k, a in enumerate((wd_hbm, wx_hbm))]
    for cp in (*wloads, oload, hload):
        cp.start()

    own = c // 2
    half = c % 2
    home = (own + r + 1) % 2
    via = home * nx + (1 - home) * ny
    past = home * ny + (1 - home) * nx
    ro = (home + half) % 2
    di = 1 - ro

    def slot_s(chip, ih, m):
        return pl.ds(pl.multiple_of(((chip * 2 + ih) * 2 + m) * 8, 8), 8)

    def slot_p(kind, a, ih, m):
        return ((kind * 2 + a) * 2 + ih) * 2 + m

    def vcopy(s, slot):
        lanes = pl.ds(pl.multiple_of(s * STEP, STEP), STEP)
        return pltpu.make_async_copy(v_hbm.at[:, lanes], vv.at[slot], vsem.at[slot])

    def landed(like, sem):
        return pltpu.make_async_copy(like, like, sem)

    for k in range(4):
        tloads[k].wait()
        tg[c, pl.ds(pl.multiple_of(r * n + k * chunk, chunk), chunk), :] = t32[k * chunk:(k + 1) * chunk, :].astype(BF16)

    pl.semaphore_wait(sem, 7)

    def tcopy(chip, lanes, k, dev):
        ref = tg.at[chip, rows, lanes]
        return _rcopy(ref, ref, gs, gr.at[k], dev)

    def fcopy(chip, lanes, p, dev):
        ref = tg.at[chip, pl.ds(pl.multiple_of(r * n + p * 32, 32), 32), lanes]
        return _rcopy(ref, ref, fs, fr.at[p], dev)

    whole = pl.ds(0, w)
    x0 = tcopy(c, h0, 1, _dev(nx, r))
    y1 = tcopy(c, h1, 2, _dev(ny, r))
    d_own = tcopy(c, whole, 0, _dev(c, o))
    x1 = tcopy(c, h1, 3, _dev(nx, r))
    y0 = tcopy(c, h0, 4, _dev(ny, r))
    x0.start()
    y1.start()
    d_own.start()
    x1.start()
    y0.start()
    vcopy(0, 0).start()
    vcopy(1, 1).start()

    def spread_rows(chip, ib, first, groups):
        for g in range(first, first + groups):
            tile = tg[chip, pl.ds(pl.multiple_of(r * n + ib * 16, 16), 16), g * 384:(g + 1) * 384].astype(F32)
            for e in range(4):
                slab = tile[:, e * VIRT:(e + 1) * VIRT]
                slab = jnp.concatenate([slab, jnp.zeros((16, LANE - VIRT), F32)], axis=1)
                for half in range(2):
                    start = (ib * 16 + half * 8) * PITCH + chip * 24 + g * 4 + e
                    t4[pl.ds(start, 8, stride=PITCH), :] = slab[half * 8:half * 8 + 8]

    def spread(chip, first, groups):
        @pl.loop(0, n // 16)
        def _(ib):
            spread_rows(chip, ib, first, groups)

    zero8 = jnp.zeros((8, w), F32)
    for m in range(2):
        srecv[slot_s(dg, ro, m), :] = zero8

    @pl.when(home == 0)
    def _():
        for m in range(2):
            precv[slot_p(0, 1 - half, half, m)] = zero8
            precv[slot_p(1, 1 - half, 1 - half, m)] = zero8

    spread(c, 0, 6)

    landed(ww, lsem.at[6]).wait()
    zrow = jnp.zeros((LANE - VIRT, 4 * LANE), BF16)

    @pl.loop(0, OCC)
    def _(k):
        blk = ww[0, pl.ds(pl.multiple_of(k * VIRT, 16), VIRT), :].astype(F32)
        parts = []
        for j in range(4):
            parts += [blk[:, j * VIRT:(j + 1) * VIRT], jnp.zeros((VIRT, LANE - VIRT), F32)]
        wd4[pl.ds(pl.multiple_of(k * LANE, LANE), VIRT), :] = jnp.concatenate(parts, axis=1).astype(BF16)
        wd4[pl.ds(pl.multiple_of(k * LANE + VIRT, 32), LANE - VIRT), :] = zrow
        wxf[pl.ds(pl.multiple_of(k * VIRT, 16), VIRT), :] = ww[1, pl.ds(pl.multiple_of(k * VIRT, 16), VIRT), :].astype(F32)

    for s, chip in enumerate((c, nx, ny, dg)):
        for b in range(3):
            blk = jnp.concatenate(
                [wxf[pl.ds(pl.multiple_of(k * VIRT + chip * 24, 8), 24), b * LANE:(b + 1) * LANE] for k in range(OCC)],
                axis=0)
            wxt[b * LANE:(b + 1) * LANE, s * 384:(s + 1) * 384] = blk.astype(BF16).T

    oload.wait()
    hload.wait()
    d_own.wait_recv()
    xp[...] = lax.dot_general(oovv[...], tg[c], NT, preferred_element_type=F32)

    def direct_rows(chip, i0, count):
        lhs = jnp.concatenate(
            [jnp.concatenate(
                [t4[pl.ds(pl.multiple_of(((i0 + i) * OCC + k) * PITCH + chip * 24, 8), 24), :] for i in range(count)],
                axis=0)
             for k in range(OCC)], axis=1).astype(BF16)
        return jnp.dot(lhs, wd4[...], preferred_element_type=F32)

    def direct(chip):
        ubuf[chip, :, :] = direct_rows(chip, 0, 8)

    def exchange_pair(chips, first, i2):
        halves = []
        for e in range(2):
            halves.append(jnp.concatenate(
                [t4[pl.ds(pl.multiple_of(((2 * i2 + e) * OCC + k) * PITCH + chip * 24, 8), 24), :]
                 for chip in chips for k in range(OCC)], axis=0))
        rhs = jnp.concatenate(halves, axis=1).astype(BF16)
        prod = jnp.dot(wxt[:, first * 384:(first + len(chips)) * 384], rhs, preferred_element_type=F32)
        vbuf_s[i2, :, :] = prod if first == 0 else vbuf_s[i2, :, :] + prod

    def exchange(chips, first):
        @pl.loop(0, 4)
        def _(i2):
            exchange_pair(chips, first, i2)

    direct(c)

    x0.wait_recv()
    for p in range(4):
        fcopy(nx, h0, p, _dev(ny, r)).start()
    y1.wait_recv()
    for p in range(4):
        fcopy(ny, h1, p, _dev(nx, r)).start()
    q = n // 4
    for cc in (nx, ny, dg):
        cp = _rcopy(xp.at[pl.ds(pl.multiple_of(cc * q, q), q)], xr.at[c], xs, xrs, _dev(cc, r))
        cp.start()
    xr[c, :, :] = xp[pl.ds(pl.multiple_of(c * q, q), q), :]
    spread(nx, 0, 3)
    spread(ny, 3, 3)
    x1.wait_recv()
    d_x = tcopy(nx, whole, 5, _dev(c, o))
    d_x.start()
    y0.wait_recv()
    d_y = tcopy(ny, whole, 5, _dev(c, o))
    d_y.start()
    spread(nx, 3, 3)
    spread(ny, 0, 3)
    direct(nx)
    direct(ny)
    exchange((c, nx, ny), 0)

    def s_rows(i, j):
        return pl.ds(pl.multiple_of((i * 4 + j) * PITCH, 8), VIRT)

    def t_rows(i, j):
        return pl.ds(pl.multiple_of(((i // 4) * 16 + j * 4 + i % 4) * PITCH, 8), VIRT)

    def block(i, j):
        direct_part = jnp.concatenate(
            [ubuf[chip, pl.ds(pl.multiple_of(i * 24, 8), 24), pl.ds(pl.multiple_of(j * LANE, LANE), LANE)]
             for chip in range(4)], axis=0)
        return direct_part - vbuf_s[
            i // 2, pl.ds(pl.multiple_of(j * VIRT, 8), VIRT), pl.ds(pl.multiple_of((i % 2) * LANE, LANE), LANE)]

    def fill_s(ih):
        @pl.loop(0, 4)
        def _(j):
            for e in range(4):
                s4[s_rows(ih * 4 + e, j), :] = block(ih * 4 + e, j)

    def fill_t(ih):
        @pl.loop(0, 4)
        def _(j):
            for e in range(4):
                st4[t_rows(ih * 4 + e, j), :VIRT] = s4[s_rows(ih * 4 + e, j), :].T[:VIRT, :]

    def put(src, ih, m, chip, dst):
        first = (ih * 16 + m * 8) * PITCH + chip * 24
        for g in range(6):
            vals = [src[pl.ds(first + g * 4 + e, 8, stride=PITCH), :][:, :VIRT] for e in range(4)]
            dst[:, g * 384:(g + 1) * 384] = jnp.concatenate(vals, axis=1)

    def s_copy(slot, ih, m, chip):
        buf = smsg.at[slot * 4 + ih * 2 + m]
        return _rcopy(buf, srecv.at[slot_s(c, ih, m)], ss, srs, _dev(chip, r))

    def p_copy(slot, ih, m, chip):
        buf = pmsg.at[slot * 4 + ih * 2 + m]
        return _rcopy(buf, precv.at[slot_p(1 - home, half, ih, m)], ps, prs, _dev(chip, own))

    def relay(kind, src):
        @pl.loop(0, 2)
        def _(m):
            put(src, ro, m, dg, rmsg.at[kind * 2 + m])
            to = rrecv.at[pl.ds(pl.multiple_of((kind * 2 + m) * 8, 8), 8)]
            _rcopy(rmsg.at[kind * 2 + m], to, rls, rlr, _dev(via, own)).start()

    def send(src, msg, copy, slot, ih, chip):
        @pl.loop(0, 2)
        def _(m):
            put(src, ih, m, chip, msg.at[slot * 4 + ih * 2 + m])
            copy(slot, ih, m, chip).start()

    def mirror():
        @pl.loop(0, 4)
        def _(j):
            for e in range(4):
                at = s_rows(half * 4 + e, j)
                s4[at, :VIRT] = s4[at, :VIRT] + block(half * 4 + j, e).T[:VIRT, :]

    @pl.loop(0, 4)
    def _(p):
        landed(tg.at[dg, pl.ds(0, n // 4)], fr.at[p]).wait()
        for ib in range(2):
            spread_rows(dg, 2 * p + ib, 0, 6)
        ubuf[dg, pl.ds(pl.multiple_of(p * 48, 16), 48), :] = direct_rows(dg, 2 * p, 2)
        exchange_pair((dg,), 3, p)

        @pl.when(p == 1)
        def _():
            fill_s(0)

            @pl.when(jnp.logical_and(home == 1, ro == 1))
            def _():
                mirror()

        @pl.when(jnp.logical_and(p == 2, ro == 0))
        def _():
            relay(0, s4)

        @pl.when(jnp.logical_and(p == 2, ro == 1))
        def _():
            send(s4, smsg, s_copy, 1, 0, via)

    d_d = tcopy(dg, whole, 5, _dev(c, o))
    d_d.start()

    fill_s(1)

    @pl.when(ro == 1)
    def _():
        relay(0, s4)

    fill_t(ro)
    relay(1, st4)

    landed(xr.at[pl.ds(0, 3)], xrs).wait()
    xsum = (xr[0] + xr[1]) + (xr[2] + xr[3])
    krows = pl.ds(pl.multiple_of(r * n + c * q, q), q)
    mfull[krows, :] = (oooo[krows, :].astype(F32) + 0.5 * xsum).astype(BF16)
    for cc, rr in ((nx, r), (ny, r), (dg, r), (c, o), (nx, o), (ny, o), (dg, o)):
        part_m = mfull.at[krows, pl.ds(pl.multiple_of(rr * n, n), n)]
        _rcopy(part_m, part_m, ms, mrs, _dev(cc, rr)).start()

    @pl.when(jnp.logical_and(home == 1, di == 1))
    def _():
        mirror()

    send(s4, smsg, s_copy, 2, di, past)
    send(s4, smsg, s_copy, 0, di, dg)

    @pl.when(home == 0)
    def _():
        fill_t(di)
        send(st4, pmsg, p_copy, 2, di, past)
        send(st4, pmsg, p_copy, 0, di, dg)
        send(st4, pmsg, p_copy, 3, ro, c)
        send(st4, pmsg, p_copy, 3, di, c)

    @pl.loop(0, 2)
    def _(m):
        for ih in range(2):
            put(s4, ih, m, c, srecv.at[slot_s(c, ih, m)])

    @pl.when(home == 1)
    def _():
        @pl.loop(0, 2)
        def _(m):
            put(st4, ro, m, c, precv.at[slot_p(0, half, ro, m)])

    def pass_on():
        landed(rrecv, rlr).wait()
        for kind, (src, msg, copy) in ((1, (s4, smsg, s_copy)), (0, (st4, pmsg, p_copy))):
            for m in range(2):
                buf = msg.at[2 * 4 + ro * 2 + m]
                put(src, ro, m, past, buf)
                buf[...] = buf[...] + rrecv[(kind * 2 + m) * 8:(kind * 2 + m + 1) * 8, :]
                copy(2, ro, m, past).start()

    landed(tg.at[pl.ds(0, 3), pl.ds(0, n)], gr.at[5]).wait()

    def ladder_copy(s):
        lanes = pl.ds(pl.multiple_of(s * STEP, STEP), STEP)
        return _rcopy(part.at[s, orows], theirs.at[:, lanes], rs, rrs, _dev(c, o))

    @pl.loop(0, w // STEP)
    def _(s):
        slot = s % 3

        @pl.when(s + 2 < w // STEP)
        def _():
            vcopy(s + 2, (s + 2) % 3).start()

        vcopy(s, slot).wait()
        va, vb = vv.at[slot, pl.ds(0, w)], vv.at[slot, pl.ds(w, w)]
        part[s, :, :] = (jnp.dot(tg[2 * r], va[...], preferred_element_type=F32)
                         + jnp.dot(tg[2 * r + 1], vb[...], preferred_element_type=F32))
        ladder_copy(s).start()

        @pl.when(s == 0)
        def _():
            send(s4, smsg, s_copy, 1, ro, via)

        @pl.when(jnp.logical_and(s == 1, di == 1))
        def _():
            send(s4, smsg, s_copy, 1, 1, via)

        @pl.when(s == 2)
        def _():
            send(st4, pmsg, p_copy, 1, ro, via)

        @pl.when(jnp.logical_and(s == 3, home == 0))
        def _():
            send(st4, pmsg, p_copy, 1, di, via)

        @pl.when(s == 5)
        def _():
            pass_on()

    landed(theirs, rrs).wait()
    landed(theirs, rs).wait()

    landed(tg.at[pl.ds(0, 3)], gs).wait()
    landed(tg.at[0, pl.ds(0, n)], fs).wait()
    landed(xr.at[pl.ds(0, 3)], xs).wait()
    all_m = mfull.at[pl.ds(0, 7 * q), pl.ds(0, n)]
    landed(all_m, mrs).wait()
    landed(all_m, ms).wait()
    m_mine = mfull[:, rows]

    @pl.loop(0, w // STEP)
    def _(s):
        lanes = pl.ds(pl.multiple_of(s * STEP, STEP), STEP)
        hole[:, lanes] = lax.dot_general(m_mine, tg[c, :, lanes], TN, preferred_element_type=F32)

    @pl.loop(0, 8)
    def _(i):
        line = pl.ds(pl.multiple_of(i * 16, 16), 16)
        line_r = pl.ds(pl.multiple_of(r * n + i * 16, 16), 16)
        mine = jnp.concatenate([part[s, line_r, :] for s in range(w // STEP)], axis=1)
        out_ref[line, :] = oovv[line, :].astype(F32) + (mine + theirs[line, :] + hole[line, :])

    landed(rmsg, rls).wait()
    landed(srecv.at[pl.ds(0, 80)], srs).wait()
    for i in range(8):
        for jh in range(2):
            line = slice(i * 16 + jh * 8, i * 16 + jh * 8 + 8)
            rows4 = [((2 * jh + cc) * 4 + i // 2) * 8 + i % 2 * 4 for cc in range(2)]
            out_ref[line, :] = out_ref[line, :] + jnp.concatenate([srecv[k:k + 4, :] for k in rows4], axis=0)

    @pl.when(home == 1)
    def _():
        landed(precv.at[pl.ds(0, 10)], prs).wait()

    @pl.when(home == 0)
    def _():
        landed(precv.at[pl.ds(0, 8)], prs).wait()

    zero4 = jnp.zeros((4, w), F32)
    for a in range(2):
        for j in range(4):
            m, rows4 = j // 2, slice(j % 2 * 4, j % 2 * 4 + 4)
            for kind, row in ((0, r), (1, o)):
                line = pl.ds(pl.multiple_of((a * 4 + j) * 16 + row * 8, 8), 8)
                both = [zero4 if kind == 0 and ih == a else precv[slot_p(kind, a, ih, m), rows4, :] for ih in range(2)]
                out_ref[line, :] = out_ref[line, :] + jnp.concatenate(both, axis=0)

    landed(smsg.at[pl.ds(0, 10)], ss).wait()

    @pl.when(home == 1)
    def _():
        landed(pmsg.at[pl.ds(0, 4)], ps).wait()

    @pl.when(home == 0)
    def _():
        landed(pmsg.at[pl.ds(0, 14)], ps).wait()


ANY = pl.BlockSpec(memory_space=pl.ANY)
DMA = pltpu.SemaphoreType.DMA


def sweep(t, oovv, vvvv, oooo, wd, wx):
    n, w = t.shape
    depth = vvvv.shape[0]
    V = pltpu.VMEM
    return pl.pallas_call(
        sweep_kernel,
        out_shape=jax.ShapeDtypeStruct((n, w), F32),
        in_specs=[ANY] * 6,
        out_specs=pl.BlockSpec(memory_space=pltpu.VMEM),
        scratch_shapes=[
            V((n, w), F32), V((n, w), BF16), V(oooo.shape, BF16), V((2,) + wd.shape, BF16),
            V((4, 2 * n, w), BF16),
            V((n, 2 * n), F32), V((4, n // 4, 2 * n), F32), V((2 * n, 2 * n), BF16), V((n, w), F32),
            V((n * PITCH, LANE), F32), V((OCC * LANE, 4 * LANE), BF16), V((wx.shape[1], wx.shape[0]), BF16),
            V((4, 2 * VIRT, 4 * LANE), F32), V((4, 4 * VIRT, 2 * LANE), F32),
            V((32 * PITCH, LANE), F32), V((32 * PITCH, LANE), F32),
            V((12, 8, w), F32), V((16, 8, w), F32), V((128, w), F32), V((16, 8, w), F32), V((4, 8, w), F32), V((32, w), F32),
            V((3, depth, STEP), BF16), V((n, w), F32), V((w // STEP, 2 * n, STEP), F32), V(wx.shape, F32),
            DMA((7,)), DMA, DMA((6,)), DMA, DMA((4,)), DMA, DMA, DMA, DMA,
            DMA, DMA, DMA, DMA, DMA, DMA, DMA((3,)), DMA, DMA,
        ],
        compiler_params=pltpu.CompilerParams(collective_id=0, has_side_effects=True, vmem_limit_bytes=46 << 20),
        name="sweep",
    )(*(pltpu.with_memory_space_constraint(a, pltpu.HBM) for a in (t, oovv, vvvv, oooo, wd, wx)))


def solution(mesh):
    def local_sweep(t_blk, d_blk, oovv_blk, vvvv_blk, oooo_full, wd_blk, wx_blk):
        return sweep(t_blk, oovv_blk, vvvv_blk, oooo_full, wd_blk, wx_blk) / d_blk

    amp = P("row", "col")
    wide = P(None, "col")
    return jax.shard_map(local_sweep, mesh=mesh, in_specs=(amp, amp, amp, amp, P(), wide, wide), out_specs=amp, check_vma=False)
```

```python
import jax
import jax.numpy as jnp
from jax import lax
from jax.experimental import pallas as pl
from jax.experimental.pallas import tpu as pltpu
from jax.sharding import PartitionSpec as P

MESH = pl.DeviceIdType.MESH
F32 = jnp.float32
BF16 = jnp.bfloat16
NT = (((1,), (1,)), ((), ()))
TN = (((0,), (0,)), ((), ()))

OCC = 16
VIRT = 96
LANE = 128
PITCH = 104
STEP = 256


def _dev(c, r):
    return {"col": c, "row": r}


def _rcopy(src, dst, ssem, rsem, dev):
    return pltpu.make_async_remote_copy(src, dst, ssem, rsem, device_id=dev, device_id_type=MESH)


def sweep_kernel(t_hbm, oovv_hbm, v_hbm, oooo_hbm, wd_hbm, wx_hbm, out_ref,
                 t32, oovv, oooo, ww, tg, xp, xr, mfull, hole, t4, wd4, wxt, ubuf, vbuf_s, s4, st4,
                 smsg, pmsg, srecv, precv, rmsg, rrecv, vv, theirs, part, wxf,
                 lsem, gs, gr, fs, fr, xs, xrs, ms, mrs, ss, srs, ps, prs, rls, rlr, vsem, rs, rrs):
    r, c = lax.axis_index("row"), lax.axis_index("col")
    x, y = c % 2, c // 2
    o = 1 - r
    nx, ny, dg = y * 2 + (1 - x), (1 - y) * 2 + x, (1 - y) * 2 + (1 - x)
    n, w = t32.shape
    h = w // 2
    h0, h1 = pl.ds(0, h), pl.ds(h, h)
    rows = pl.ds(pl.multiple_of(r * n, n), n)
    orows = pl.ds(pl.multiple_of(o * n, n), n)

    sem = pltpu.get_barrier_semaphore()
    for cc, rr in ((nx, r), (ny, r), (dg, r), (c, o), (nx, o), (ny, o), (dg, o)):
        pl.semaphore_signal(sem, inc=1, device_id=_dev(cc, rr), device_id_type=MESH)

    chunk = n // 4
    tloads = [pltpu.make_async_copy(t_hbm.at[pl.ds(k * chunk, chunk)], t32.at[pl.ds(k * chunk, chunk)], lsem.at[k])
              for k in range(4)]
    for cp in tloads:
        cp.start()
    oload = pltpu.make_async_copy(oovv_hbm, oovv, lsem.at[4])
    hload = pltpu.make_async_copy(oooo_hbm, oooo, lsem.at[5])
    wloads = [pltpu.make_async_copy(a, ww.at[k], lsem.at[6]) for k, a in enumerate((wd_hbm, wx_hbm))]
    for cp in (*wloads, oload, hload):
        cp.start()

    own = c // 2
    half = c % 2
    home = (own + r + 1) % 2
    via = home * nx + (1 - home) * ny
    past = home * ny + (1 - home) * nx
    ro = (home + half) % 2
    di = 1 - ro

    def slot_s(chip, ih, m):
        return pl.ds(pl.multiple_of(((chip * 2 + ih) * 2 + m) * 8, 8), 8)

    def slot_p(kind, a, ih, m):
        return ((kind * 2 + a) * 2 + ih) * 2 + m

    def vcopy(s, slot):
        lanes = pl.ds(pl.multiple_of(s * STEP, STEP), STEP)
        return pltpu.make_async_copy(v_hbm.at[:, lanes], vv.at[slot], vsem.at[slot])

    def landed(like, sem):
        return pltpu.make_async_copy(like, like, sem)

    for k in range(4):
        tloads[k].wait()
        tg[c, pl.ds(pl.multiple_of(r * n + k * chunk, chunk), chunk), :] = t32[k * chunk:(k + 1) * chunk, :].astype(BF16)

    pl.semaphore_wait(sem, 7)

    def tcopy(chip, lanes, k, dev):
        ref = tg.at[chip, rows, lanes]
        return _rcopy(ref, ref, gs, gr.at[k], dev)

    def fcopy(chip, lanes, p, dev):
        ref = tg.at[chip, pl.ds(pl.multiple_of(r * n + p * 32, 32), 32), lanes]
        return _rcopy(ref, ref, fs, fr.at[p], dev)

    whole = pl.ds(0, w)
    x0 = tcopy(c, h0, 1, _dev(nx, r))
    y1 = tcopy(c, h1, 2, _dev(ny, r))
    d_own = tcopy(c, whole, 0, _dev(c, o))
    x1 = tcopy(c, h1, 3, _dev(nx, r))
    y0 = tcopy(c, h0, 4, _dev(ny, r))
    x0.start()
    y1.start()
    d_own.start()
    x1.start()
    y0.start()
    vcopy(0, 0).start()
    vcopy(1, 1).start()

    def spread_rows(chip, ib, first, groups):
        for g in range(first, first + groups):
            tile = tg[chip, pl.ds(pl.multiple_of(r * n + ib * 16, 16), 16), g * 384:(g + 1) * 384].astype(F32)
            for e in range(4):
                slab = tile[:, e * VIRT:(e + 1) * VIRT]
                slab = jnp.concatenate([slab, jnp.zeros((16, LANE - VIRT), F32)], axis=1)
                for half in range(2):
                    start = (ib * 16 + half * 8) * PITCH + chip * 24 + g * 4 + e
                    t4[pl.ds(start, 8, stride=PITCH), :] = slab[half * 8:half * 8 + 8]

    def spread(chip, first, groups):
        @pl.loop(0, n // 16)
        def _(ib):
            spread_rows(chip, ib, first, groups)

    zero8 = jnp.zeros((8, w), F32)
    for m in range(2):
        srecv[slot_s(dg, ro, m), :] = zero8

    @pl.when(home == 0)
    def _():
        for m in range(2):
            precv[slot_p(0, 1 - half, half, m)] = zero8
            precv[slot_p(1, 1 - half, 1 - half, m)] = zero8

    spread(c, 0, 6)

    landed(ww, lsem.at[6]).wait()
    zrow = jnp.zeros((LANE - VIRT, 4 * LANE), BF16)

    @pl.loop(0, OCC)
    def _(k):
        blk = ww[0, pl.ds(pl.multiple_of(k * VIRT, 16), VIRT), :].astype(F32)
        parts = []
        for j in range(4):
            parts += [blk[:, j * VIRT:(j + 1) * VIRT], jnp.zeros((VIRT, LANE - VIRT), F32)]
        wd4[pl.ds(pl.multiple_of(k * LANE, LANE), VIRT), :] = jnp.concatenate(parts, axis=1).astype(BF16)
        wd4[pl.ds(pl.multiple_of(k * LANE + VIRT, 32), LANE - VIRT), :] = zrow
        wxf[pl.ds(pl.multiple_of(k * VIRT, 16), VIRT), :] = ww[1, pl.ds(pl.multiple_of(k * VIRT, 16), VIRT), :].astype(F32)

    for s, chip in enumerate((c, nx, ny, dg)):
        for b in range(3):
            blk = jnp.concatenate(
                [wxf[pl.ds(pl.multiple_of(k * VIRT + chip * 24, 8), 24), b * LANE:(b + 1) * LANE] for k in range(OCC)],
                axis=0)
            wxt[b * LANE:(b + 1) * LANE, s * 384:(s + 1) * 384] = blk.astype(BF16).T

    oload.wait()
    hload.wait()
    d_own.wait_recv()
    xp[...] = lax.dot_general(oovv[...], tg[c], NT, preferred_element_type=F32)

    def direct_rows(chip, i0, count):
        lhs = jnp.concatenate(
            [jnp.concatenate(
                [t4[pl.ds(pl.multiple_of(((i0 + i) * OCC + k) * PITCH + chip * 24, 8), 24), :] for i in range(count)],
                axis=0)
             for k in range(OCC)], axis=1).astype(BF16)
        return jnp.dot(lhs, wd4[...], preferred_element_type=F32)

    def direct(chip):
        ubuf[chip, :, :] = direct_rows(chip, 0, 8)

    def exchange_pair(chips, first, i2):
        halves = []
        for e in range(2):
            halves.append(jnp.concatenate(
                [t4[pl.ds(pl.multiple_of(((2 * i2 + e) * OCC + k) * PITCH + chip * 24, 8), 24), :]
                 for chip in chips for k in range(OCC)], axis=0))
        rhs = jnp.concatenate(halves, axis=1).astype(BF16)
        prod = jnp.dot(wxt[:, first * 384:(first + len(chips)) * 384], rhs, preferred_element_type=F32)
        vbuf_s[i2, :, :] = prod if first == 0 else vbuf_s[i2, :, :] + prod

    def exchange(chips, first):
        @pl.loop(0, 4)
        def _(i2):
            exchange_pair(chips, first, i2)

    direct(c)

    x0.wait_recv()
    for p in range(4):
        fcopy(nx, h0, p, _dev(ny, r)).start()
    y1.wait_recv()
    for p in range(4):
        fcopy(ny, h1, p, _dev(nx, r)).start()
    q = n // 4
    for cc in (nx, ny, dg):
        cp = _rcopy(xp.at[pl.ds(pl.multiple_of(cc * q, q), q)], xr.at[c], xs, xrs, _dev(cc, r))
        cp.start()
    xr[c, :, :] = xp[pl.ds(pl.multiple_of(c * q, q), q), :]
    spread(nx, 0, 3)
    spread(ny, 3, 3)
    x1.wait_recv()
    d_x = tcopy(nx, whole, 5, _dev(c, o))
    d_x.start()
    y0.wait_recv()
    d_y = tcopy(ny, whole, 5, _dev(c, o))
    d_y.start()
    spread(nx, 3, 3)
    spread(ny, 0, 3)
    direct(nx)
    direct(ny)
    exchange((c, nx, ny), 0)

    def s_rows(i, j):
        return pl.ds(pl.multiple_of((i * 4 + j) * PITCH, 8), VIRT)

    def t_rows(i, j):
        return pl.ds(pl.multiple_of(((i // 4) * 16 + j * 4 + i % 4) * PITCH, 8), VIRT)

    def block(i, j):
        direct_part = jnp.concatenate(
            [ubuf[chip, pl.ds(pl.multiple_of(i * 24, 8), 24), pl.ds(pl.multiple_of(j * LANE, LANE), LANE)]
             for chip in range(4)], axis=0)
        return direct_part - vbuf_s[
            i // 2, pl.ds(pl.multiple_of(j * VIRT, 8), VIRT), pl.ds(pl.multiple_of((i % 2) * LANE, LANE), LANE)]

    def fill_s(ih):
        @pl.loop(0, 4)
        def _(j):
            for e in range(4):
                s4[s_rows(ih * 4 + e, j), :] = block(ih * 4 + e, j)

    def fill_t(ih):
        @pl.loop(0, 4)
        def _(j):
            for e in range(4):
                st4[t_rows(ih * 4 + e, j), :VIRT] = s4[s_rows(ih * 4 + e, j), :].T[:VIRT, :]

    def put(src, ih, m, chip, dst):
        first = (ih * 16 + m * 8) * PITCH + chip * 24
        for g in range(6):
            vals = [src[pl.ds(first + g * 4 + e, 8, stride=PITCH), :][:, :VIRT] for e in range(4)]
            dst[:, g * 384:(g + 1) * 384] = jnp.concatenate(vals, axis=1)

    def s_copy(slot, ih, m, chip):
        buf = smsg.at[slot * 4 + ih * 2 + m]
        return _rcopy(buf, srecv.at[slot_s(c, ih, m)], ss, srs, _dev(chip, r))

    def p_copy(slot, ih, m, chip):
        buf = pmsg.at[slot * 4 + ih * 2 + m]
        return _rcopy(buf, precv.at[slot_p(1 - home, half, ih, m)], ps, prs, _dev(chip, own))

    def relay(kind, src):
        @pl.loop(0, 2)
        def _(m):
            put(src, ro, m, dg, rmsg.at[kind * 2 + m])
            to = rrecv.at[pl.ds(pl.multiple_of((kind * 2 + m) * 8, 8), 8)]
            _rcopy(rmsg.at[kind * 2 + m], to, rls, rlr, _dev(via, own)).start()

    def send(src, msg, copy, slot, ih, chip):
        @pl.loop(0, 2)
        def _(m):
            put(src, ih, m, chip, msg.at[slot * 4 + ih * 2 + m])
            copy(slot, ih, m, chip).start()

    def mirror():
        @pl.loop(0, 4)
        def _(j):
            for e in range(4):
                at = s_rows(half * 4 + e, j)
                s4[at, :VIRT] = s4[at, :VIRT] + block(half * 4 + j, e).T[:VIRT, :]

    @pl.loop(0, 4)
    def _(p):
        landed(tg.at[dg, pl.ds(0, n // 4)], fr.at[p]).wait()
        for ib in range(2):
            spread_rows(dg, 2 * p + ib, 0, 6)
        ubuf[dg, pl.ds(pl.multiple_of(p * 48, 16), 48), :] = direct_rows(dg, 2 * p, 2)
        exchange_pair((dg,), 3, p)

        @pl.when(p == 1)
        def _():
            fill_s(0)

            @pl.when(ro == 0)
            def _():
                relay(0, s4)

            @pl.when(jnp.logical_and(ro == 1, home == 0))
            def _():
                send(s4, smsg, s_copy, 1, 0, via)

        @pl.when(jnp.logical_and(p == 2, jnp.logical_and(ro == 1, home == 1)))
        def _():
            mirror()
            send(s4, smsg, s_copy, 1, 0, via)

    d_d = tcopy(dg, whole, 5, _dev(c, o))
    d_d.start()

    fill_s(1)

    @pl.when(ro == 1)
    def _():
        relay(0, s4)

    fill_t(ro)
    relay(1, st4)

    landed(xr.at[pl.ds(0, 3)], xrs).wait()
    xsum = (xr[0] + xr[1]) + (xr[2] + xr[3])
    krows = pl.ds(pl.multiple_of(r * n + c * q, q), q)
    mfull[krows, :] = (oooo[krows, :].astype(F32) + 0.5 * xsum).astype(BF16)
    for cc, rr in ((nx, r), (ny, r), (dg, r), (c, o), (nx, o), (ny, o), (dg, o)):
        part_m = mfull.at[krows, pl.ds(pl.multiple_of(rr * n, n), n)]
        _rcopy(part_m, part_m, ms, mrs, _dev(cc, rr)).start()

    @pl.when(jnp.logical_and(home == 1, di == 1))
    def _():
        mirror()

    send(s4, smsg, s_copy, 2, di, past)
    send(s4, smsg, s_copy, 0, di, dg)

    @pl.when(home == 0)
    def _():
        fill_t(di)
        send(st4, pmsg, p_copy, 2, di, past)
        send(st4, pmsg, p_copy, 0, di, dg)
        send(st4, pmsg, p_copy, 3, ro, c)
        send(st4, pmsg, p_copy, 3, di, c)

    @pl.loop(0, 2)
    def _(m):
        for ih in range(2):
            put(s4, ih, m, c, srecv.at[slot_s(c, ih, m)])

    @pl.when(home == 1)
    def _():
        @pl.loop(0, 2)
        def _(m):
            put(st4, ro, m, c, precv.at[slot_p(0, half, ro, m)])

    def pass_on():
        landed(rrecv, rlr).wait()
        for kind, (src, msg, copy) in ((1, (s4, smsg, s_copy)), (0, (st4, pmsg, p_copy))):
            for m in range(2):
                buf = msg.at[2 * 4 + ro * 2 + m]
                put(src, ro, m, past, buf)
                buf[...] = buf[...] + rrecv[(kind * 2 + m) * 8:(kind * 2 + m + 1) * 8, :]
                copy(2, ro, m, past).start()

    landed(tg.at[pl.ds(0, 3), pl.ds(0, n)], gr.at[5]).wait()

    def ladder_copy(s):
        lanes = pl.ds(pl.multiple_of(s * STEP, STEP), STEP)
        return _rcopy(part.at[s, orows], theirs.at[:, lanes], rs, rrs, _dev(c, o))

    @pl.loop(0, w // STEP)
    def _(s):
        slot = s % 3

        @pl.when(s + 2 < w // STEP)
        def _():
            vcopy(s + 2, (s + 2) % 3).start()

        vcopy(s, slot).wait()
        va, vb = vv.at[slot, pl.ds(0, w)], vv.at[slot, pl.ds(w, w)]
        part[s, :, :] = (jnp.dot(tg[2 * r], va[...], preferred_element_type=F32)
                         + jnp.dot(tg[2 * r + 1], vb[...], preferred_element_type=F32))
        ladder_copy(s).start()

        @pl.when(s == 0)
        def _():
            send(s4, smsg, s_copy, 1, ro, via)

        @pl.when(jnp.logical_and(s == 1, di == 1))
        def _():
            send(s4, smsg, s_copy, 1, 1, via)

        @pl.when(s == 2)
        def _():
            send(st4, pmsg, p_copy, 1, ro, via)

        @pl.when(jnp.logical_and(s == 3, home == 0))
        def _():
            send(st4, pmsg, p_copy, 1, di, via)

        @pl.when(s == 5)
        def _():
            pass_on()

    landed(theirs, rrs).wait()
    landed(theirs, rs).wait()

    landed(tg.at[pl.ds(0, 3)], gs).wait()
    landed(tg.at[0, pl.ds(0, n)], fs).wait()
    landed(xr.at[pl.ds(0, 3)], xs).wait()
    all_m = mfull.at[pl.ds(0, 7 * q), pl.ds(0, n)]
    landed(all_m, mrs).wait()
    landed(all_m, ms).wait()
    m_mine = mfull[:, rows]

    @pl.loop(0, w // STEP)
    def _(s):
        lanes = pl.ds(pl.multiple_of(s * STEP, STEP), STEP)
        hole[:, lanes] = lax.dot_general(m_mine, tg[c, :, lanes], TN, preferred_element_type=F32)

    @pl.loop(0, 8)
    def _(i):
        line = pl.ds(pl.multiple_of(i * 16, 16), 16)
        line_r = pl.ds(pl.multiple_of(r * n + i * 16, 16), 16)
        mine = jnp.concatenate([part[s, line_r, :] for s in range(w // STEP)], axis=1)
        out_ref[line, :] = oovv[line, :].astype(F32) + (mine + theirs[line, :] + hole[line, :])

    landed(rmsg, rls).wait()
    landed(srecv.at[pl.ds(0, 80)], srs).wait()
    for i in range(8):
        for jh in range(2):
            line = slice(i * 16 + jh * 8, i * 16 + jh * 8 + 8)
            rows4 = [((2 * jh + cc) * 4 + i // 2) * 8 + i % 2 * 4 for cc in range(2)]
            out_ref[line, :] = out_ref[line, :] + jnp.concatenate([srecv[k:k + 4, :] for k in rows4], axis=0)

    @pl.when(home == 1)
    def _():
        landed(precv.at[pl.ds(0, 10)], prs).wait()

    @pl.when(home == 0)
    def _():
        landed(precv.at[pl.ds(0, 8)], prs).wait()

    zero4 = jnp.zeros((4, w), F32)
    for a in range(2):
        for j in range(4):
            m, rows4 = j // 2, slice(j % 2 * 4, j % 2 * 4 + 4)
            for kind, row in ((0, r), (1, o)):
                line = pl.ds(pl.multiple_of((a * 4 + j) * 16 + row * 8, 8), 8)
                both = [zero4 if kind == 0 and ih == a else precv[slot_p(kind, a, ih, m), rows4, :] for ih in range(2)]
                out_ref[line, :] = out_ref[line, :] + jnp.concatenate(both, axis=0)

    landed(smsg.at[pl.ds(0, 10)], ss).wait()

    @pl.when(home == 1)
    def _():
        landed(pmsg.at[pl.ds(0, 4)], ps).wait()

    @pl.when(home == 0)
    def _():
        landed(pmsg.at[pl.ds(0, 14)], ps).wait()


ANY = pl.BlockSpec(memory_space=pl.ANY)
DMA = pltpu.SemaphoreType.DMA


def sweep(t, oovv, vvvv, oooo, wd, wx):
    n, w = t.shape
    depth = vvvv.shape[0]
    V = pltpu.VMEM
    return pl.pallas_call(
        sweep_kernel,
        out_shape=jax.ShapeDtypeStruct((n, w), F32),
        in_specs=[ANY] * 6,
        out_specs=pl.BlockSpec(memory_space=pltpu.VMEM),
        scratch_shapes=[
            V((n, w), F32), V((n, w), BF16), V(oooo.shape, BF16), V((2,) + wd.shape, BF16),
            V((4, 2 * n, w), BF16),
            V((n, 2 * n), F32), V((4, n // 4, 2 * n), F32), V((2 * n, 2 * n), BF16), V((n, w), F32),
            V((n * PITCH, LANE), F32), V((OCC * LANE, 4 * LANE), BF16), V((wx.shape[1], wx.shape[0]), BF16),
            V((4, 2 * VIRT, 4 * LANE), F32), V((4, 4 * VIRT, 2 * LANE), F32),
            V((32 * PITCH, LANE), F32), V((32 * PITCH, LANE), F32),
            V((12, 8, w), F32), V((16, 8, w), F32), V((128, w), F32), V((16, 8, w), F32), V((4, 8, w), F32), V((32, w), F32),
            V((3, depth, STEP), BF16), V((n, w), F32), V((w // STEP, 2 * n, STEP), F32), V(wx.shape, F32),
            DMA((7,)), DMA, DMA((6,)), DMA, DMA((4,)), DMA, DMA, DMA, DMA,
            DMA, DMA, DMA, DMA, DMA, DMA, DMA((3,)), DMA, DMA,
        ],
        compiler_params=pltpu.CompilerParams(collective_id=0, has_side_effects=True, vmem_limit_bytes=46 << 20),
        name="sweep",
    )(*(pltpu.with_memory_space_constraint(a, pltpu.HBM) for a in (t, oovv, vvvv, oooo, wd, wx)))


def solution(mesh):
    def local_sweep(t_blk, d_blk, oovv_blk, vvvv_blk, oooo_full, wd_blk, wx_blk):
        return sweep(t_blk, oovv_blk, vvvv_blk, oooo_full, wd_blk, wx_blk) / d_blk

    amp = P("row", "col")
    wide = P(None, "col")
    return jax.shard_map(local_sweep, mesh=mesh, in_specs=(amp, amp, amp, amp, P(), wide, wide), out_specs=amp, check_vma=False)
```

```python
import jax
import jax.numpy as jnp
from jax import lax
from jax.experimental import pallas as pl
from jax.experimental.pallas import tpu as pltpu
from jax.sharding import PartitionSpec as P

MESH = pl.DeviceIdType.MESH
F32 = jnp.float32
BF16 = jnp.bfloat16
NT = (((1,), (1,)), ((), ()))
TN = (((0,), (0,)), ((), ()))

OCC = 16
VIRT = 96
LANE = 128
PITCH = 104
STEP = 256


def _dev(c, r):
    return {"col": c, "row": r}


def _rcopy(src, dst, ssem, rsem, dev):
    return pltpu.make_async_remote_copy(src, dst, ssem, rsem, device_id=dev, device_id_type=MESH)


def sweep_kernel(t_hbm, oovv_hbm, v_hbm, oooo_hbm, wd_hbm, wx_hbm, out_ref,
                 t32, oovv, oooo, ww, tg, xp, xr, mfull, hole, t4, wd4, wxt, ubuf, vbuf_s, s4, st4,
                 smsg, pmsg, srecv, precv, rmsg, rrecv, vv, theirs, part, wxf,
                 lsem, gs, gr, fs, fr, xs, xrs, ms, mrs, ss, srs, ps, prs, rls, rlr, vsem, rs, rrs):
    r, c = lax.axis_index("row"), lax.axis_index("col")
    x, y = c % 2, c // 2
    o = 1 - r
    nx, ny, dg = y * 2 + (1 - x), (1 - y) * 2 + x, (1 - y) * 2 + (1 - x)
    n, w = t32.shape
    h = w // 2
    h0, h1 = pl.ds(0, h), pl.ds(h, h)
    rows = pl.ds(pl.multiple_of(r * n, n), n)
    orows = pl.ds(pl.multiple_of(o * n, n), n)

    sem = pltpu.get_barrier_semaphore()
    for cc, rr in ((nx, r), (ny, r), (dg, r), (c, o), (nx, o), (ny, o), (dg, o)):
        pl.semaphore_signal(sem, inc=1, device_id=_dev(cc, rr), device_id_type=MESH)

    chunk = n // 4
    tloads = [pltpu.make_async_copy(t_hbm.at[pl.ds(k * chunk, chunk)], t32.at[pl.ds(k * chunk, chunk)], lsem.at[k])
              for k in range(4)]
    for cp in tloads:
        cp.start()
    oload = pltpu.make_async_copy(oovv_hbm, oovv, lsem.at[4])
    hload = pltpu.make_async_copy(oooo_hbm, oooo, lsem.at[5])
    wloads = [pltpu.make_async_copy(a, ww.at[k], lsem.at[6]) for k, a in enumerate((wd_hbm, wx_hbm))]
    for cp in (*wloads, oload, hload):
        cp.start()

    own = c // 2
    half = c % 2
    home = (own + r + 1) % 2
    via = home * nx + (1 - home) * ny
    past = home * ny + (1 - home) * nx
    ro = (home + half) % 2
    di = 1 - ro

    def slot_s(chip, ih, m):
        return pl.ds(pl.multiple_of(((chip * 2 + ih) * 2 + m) * 8, 8), 8)

    def slot_p(kind, a, ih, m):
        return ((kind * 2 + a) * 2 + ih) * 2 + m

    def vcopy(s, slot):
        lanes = pl.ds(pl.multiple_of(s * STEP, STEP), STEP)
        return pltpu.make_async_copy(v_hbm.at[:, lanes], vv.at[slot], vsem.at[slot])

    def landed(like, sem):
        return pltpu.make_async_copy(like, like, sem)

    for k in range(4):
        tloads[k].wait()
        tg[c, pl.ds(pl.multiple_of(r * n + k * chunk, chunk), chunk), :] = t32[k * chunk:(k + 1) * chunk, :].astype(BF16)

    pl.semaphore_wait(sem, 7)

    def tcopy(chip, lanes, k, dev):
        ref = tg.at[chip, rows, lanes]
        return _rcopy(ref, ref, gs, gr.at[k], dev)

    def fcopy(chip, lanes, p, dev):
        ref = tg.at[chip, pl.ds(pl.multiple_of(r * n + p * 32, 32), 32), lanes]
        return _rcopy(ref, ref, fs, fr.at[p], dev)

    whole = pl.ds(0, w)
    x0 = tcopy(c, h0, 1, _dev(nx, r))
    y1 = tcopy(c, h1, 2, _dev(ny, r))
    d_own = tcopy(c, whole, 0, _dev(c, o))
    x1 = tcopy(c, h1, 3, _dev(nx, r))
    y0 = tcopy(c, h0, 4, _dev(ny, r))
    x0.start()
    y1.start()
    d_own.start()
    x1.start()
    y0.start()
    vcopy(0, 0).start()
    vcopy(1, 1).start()

    def spread_rows(chip, ib, first, groups):
        for g in range(first, first + groups):
            tile = tg[chip, pl.ds(pl.multiple_of(r * n + ib * 16, 16), 16), g * 384:(g + 1) * 384].astype(F32)
            for e in range(4):
                slab = tile[:, e * VIRT:(e + 1) * VIRT]
                slab = jnp.concatenate([slab, jnp.zeros((16, LANE - VIRT), F32)], axis=1)
                for half in range(2):
                    start = (ib * 16 + half * 8) * PITCH + chip * 24 + g * 4 + e
                    t4[pl.ds(start, 8, stride=PITCH), :] = slab[half * 8:half * 8 + 8]

    def spread(chip, first, groups):
        @pl.loop(0, n // 16)
        def _(ib):
            spread_rows(chip, ib, first, groups)

    zero8 = jnp.zeros((8, w), F32)
    for m in range(2):
        srecv[slot_s(dg, ro, m), :] = zero8

    @pl.when(home == 0)
    def _():
        for m in range(2):
            precv[slot_p(0, 1 - half, half, m)] = zero8
            precv[slot_p(1, 1 - half, 1 - half, m)] = zero8

    spread(c, 0, 6)

    landed(ww, lsem.at[6]).wait()
    zrow = jnp.zeros((LANE - VIRT, 4 * LANE), BF16)

    @pl.loop(0, OCC)
    def _(k):
        blk = ww[0, pl.ds(pl.multiple_of(k * VIRT, 16), VIRT), :].astype(F32)
        parts = []
        for j in range(4):
            parts += [blk[:, j * VIRT:(j + 1) * VIRT], jnp.zeros((VIRT, LANE - VIRT), F32)]
        wd4[pl.ds(pl.multiple_of(k * LANE, LANE), VIRT), :] = jnp.concatenate(parts, axis=1).astype(BF16)
        wd4[pl.ds(pl.multiple_of(k * LANE + VIRT, 32), LANE - VIRT), :] = zrow
        wxf[pl.ds(pl.multiple_of(k * VIRT, 16), VIRT), :] = ww[1, pl.ds(pl.multiple_of(k * VIRT, 16), VIRT), :].astype(F32)

    for s, chip in enumerate((c, nx, ny, dg)):
        for b in range(3):
            blk = jnp.concatenate(
                [wxf[pl.ds(pl.multiple_of(k * VIRT + chip * 24, 8), 24), b * LANE:(b + 1) * LANE] for k in range(OCC)],
                axis=0)
            wxt[b * LANE:(b + 1) * LANE, s * 384:(s + 1) * 384] = blk.astype(BF16).T

    oload.wait()
    hload.wait()
    d_own.wait_recv()
    xp[...] = lax.dot_general(oovv[...], tg[c], NT, preferred_element_type=F32)

    def direct_rows(chip, i0, count):
        lhs = jnp.concatenate(
            [jnp.concatenate(
                [t4[pl.ds(pl.multiple_of(((i0 + i) * OCC + k) * PITCH + chip * 24, 8), 24), :] for i in range(count)],
                axis=0)
             for k in range(OCC)], axis=1).astype(BF16)
        return jnp.dot(lhs, wd4[...], preferred_element_type=F32)

    def direct(chip):
        ubuf[chip, :, :] = direct_rows(chip, 0, 8)

    def exchange_pair(chips, first, i2):
        halves = []
        for e in range(2):
            halves.append(jnp.concatenate(
                [t4[pl.ds(pl.multiple_of(((2 * i2 + e) * OCC + k) * PITCH + chip * 24, 8), 24), :]
                 for chip in chips for k in range(OCC)], axis=0))
        rhs = jnp.concatenate(halves, axis=1).astype(BF16)
        prod = jnp.dot(wxt[:, first * 384:(first + len(chips)) * 384], rhs, preferred_element_type=F32)
        vbuf_s[i2, :, :] = prod if first == 0 else vbuf_s[i2, :, :] + prod

    def exchange(chips, first):
        @pl.loop(0, 4)
        def _(i2):
            exchange_pair(chips, first, i2)

    direct(c)

    x0.wait_recv()
    for p in range(4):
        fcopy(nx, h0, p, _dev(ny, r)).start()
    y1.wait_recv()
    for p in range(4):
        fcopy(ny, h1, p, _dev(nx, r)).start()
    q = n // 4
    for cc in (nx, ny, dg):
        cp = _rcopy(xp.at[pl.ds(pl.multiple_of(cc * q, q), q)], xr.at[c], xs, xrs, _dev(cc, r))
        cp.start()
    xr[c, :, :] = xp[pl.ds(pl.multiple_of(c * q, q), q), :]
    spread(nx, 0, 3)
    spread(ny, 3, 3)
    x1.wait_recv()
    d_x = tcopy(nx, whole, 5, _dev(c, o))
    d_x.start()
    y0.wait_recv()
    d_y = tcopy(ny, whole, 5, _dev(c, o))
    d_y.start()
    spread(nx, 3, 3)
    spread(ny, 0, 3)
    direct(nx)
    direct(ny)
    exchange((c, nx, ny), 0)

    def s_rows(i, j):
        return pl.ds(pl.multiple_of((i * 4 + j) * PITCH, 8), VIRT)

    def t_rows(i, j):
        return pl.ds(pl.multiple_of(((i // 4) * 16 + j * 4 + i % 4) * PITCH, 8), VIRT)

    def block(i, j):
        direct_part = jnp.concatenate(
            [ubuf[chip, pl.ds(pl.multiple_of(i * 24, 8), 24), pl.ds(pl.multiple_of(j * LANE, LANE), LANE)]
             for chip in range(4)], axis=0)
        return direct_part - vbuf_s[
            i // 2, pl.ds(pl.multiple_of(j * VIRT, 8), VIRT), pl.ds(pl.multiple_of((i % 2) * LANE, LANE), LANE)]

    def fill_s(ih):
        @pl.loop(0, 4)
        def _(j):
            for e in range(4):
                s4[s_rows(ih * 4 + e, j), :] = block(ih * 4 + e, j)

    def fill_t(ih):
        @pl.loop(0, 4)
        def _(j):
            for e in range(4):
                st4[t_rows(ih * 4 + e, j), :VIRT] = s4[s_rows(ih * 4 + e, j), :].T[:VIRT, :]

    def put(src, ih, m, chip, dst):
        first = (ih * 16 + m * 8) * PITCH + chip * 24
        for g in range(6):
            vals = [src[pl.ds(first + g * 4 + e, 8, stride=PITCH), :][:, :VIRT] for e in range(4)]
            dst[:, g * 384:(g + 1) * 384] = jnp.concatenate(vals, axis=1)

    def s_copy(slot, ih, m, chip):
        buf = smsg.at[slot * 4 + ih * 2 + m]
        return _rcopy(buf, srecv.at[slot_s(c, ih, m)], ss, srs, _dev(chip, r))

    def p_copy(slot, ih, m, chip):
        buf = pmsg.at[slot * 4 + ih * 2 + m]
        return _rcopy(buf, precv.at[slot_p(1 - home, half, ih, m)], ps, prs, _dev(chip, own))

    def relay(kind, src):
        @pl.loop(0, 2)
        def _(m):
            put(src, ro, m, dg, rmsg.at[kind * 2 + m])
            to = rrecv.at[pl.ds(pl.multiple_of((kind * 2 + m) * 8, 8), 8)]
            _rcopy(rmsg.at[kind * 2 + m], to, rls, rlr, _dev(via, own)).start()

    def send(src, msg, copy, slot, ih, chip):
        @pl.loop(0, 2)
        def _(m):
            put(src, ih, m, chip, msg.at[slot * 4 + ih * 2 + m])
            copy(slot, ih, m, chip).start()

    def mirror():
        @pl.loop(0, 4)
        def _(j):
            for e in range(4):
                at = s_rows(half * 4 + e, j)
                s4[at, :VIRT] = s4[at, :VIRT] + block(half * 4 + j, e).T[:VIRT, :]

    @pl.loop(0, 4)
    def _(p):
        landed(tg.at[dg, pl.ds(0, n // 4)], fr.at[p]).wait()
        for ib in range(2):
            spread_rows(dg, 2 * p + ib, 0, 6)
        ubuf[dg, pl.ds(pl.multiple_of(p * 48, 16), 48), :] = direct_rows(dg, 2 * p, 2)
        exchange_pair((dg,), 3, p)

        @pl.when(p == 1)
        def _():
            fill_s(0)

            @pl.when(ro == 0)
            def _():
                relay(0, s4)

            @pl.when(jnp.logical_and(ro == 1, home == 0))
            def _():
                send(s4, smsg, s_copy, 1, 0, via)

        @pl.when(jnp.logical_and(p == 2, jnp.logical_and(ro == 1, home == 1)))
        def _():
            mirror()
            send(s4, smsg, s_copy, 1, 0, via)

    d_d = tcopy(dg, whole, 5, _dev(c, o))
    d_d.start()

    fill_s(1)

    @pl.when(ro == 1)
    def _():
        relay(0, s4)

    fill_t(ro)
    relay(1, st4)

    landed(xr.at[pl.ds(0, 3)], xrs).wait()
    xsum = (xr[0] + xr[1]) + (xr[2] + xr[3])
    krows = pl.ds(pl.multiple_of(r * n + c * q, q), q)
    mfull[krows, :] = (oooo[krows, :].astype(F32) + 0.5 * xsum).astype(BF16)
    for cc, rr in ((nx, r), (ny, r), (dg, r), (c, o), (nx, o), (ny, o), (dg, o)):
        part_m = mfull.at[krows, pl.ds(pl.multiple_of(rr * n, n), n)]
        _rcopy(part_m, part_m, ms, mrs, _dev(cc, rr)).start()

    @pl.when(jnp.logical_and(home == 1, di == 1))
    def _():
        mirror()

    send(s4, smsg, s_copy, 2, di, past)

    def across():
        send(s4, smsg, s_copy, 0, di, dg)

        @pl.when(home == 0)
        def _():
            send(st4, pmsg, p_copy, 0, di, dg)

    @pl.when(home == 0)
    def _():
        fill_t(di)
        send(st4, pmsg, p_copy, 2, di, past)

    @pl.when(dg == 0)
    def _():
        across()

    @pl.when(home == 0)
    def _():
        send(st4, pmsg, p_copy, 3, ro, c)
        send(st4, pmsg, p_copy, 3, di, c)

    @pl.loop(0, 2)
    def _(m):
        for ih in range(2):
            put(s4, ih, m, c, srecv.at[slot_s(c, ih, m)])

    @pl.when(home == 1)
    def _():
        @pl.loop(0, 2)
        def _(m):
            put(st4, ro, m, c, precv.at[slot_p(0, half, ro, m)])

    def pass_on():
        landed(rrecv, rlr).wait()
        for kind, (src, msg, copy) in ((1, (s4, smsg, s_copy)), (0, (st4, pmsg, p_copy))):
            for m in range(2):
                buf = msg.at[2 * 4 + ro * 2 + m]
                put(src, ro, m, past, buf)
                buf[...] = buf[...] + rrecv[(kind * 2 + m) * 8:(kind * 2 + m + 1) * 8, :]
                copy(2, ro, m, past).start()

    landed(tg.at[pl.ds(0, 3), pl.ds(0, n)], gr.at[5]).wait()

    def ladder_copy(s):
        lanes = pl.ds(pl.multiple_of(s * STEP, STEP), STEP)
        return _rcopy(part.at[s, orows], theirs.at[:, lanes], rs, rrs, _dev(c, o))

    @pl.loop(0, w // STEP)
    def _(s):
        slot = s % 3

        @pl.when(s + 2 < w // STEP)
        def _():
            vcopy(s + 2, (s + 2) % 3).start()

        vcopy(s, slot).wait()
        va, vb = vv.at[slot, pl.ds(0, w)], vv.at[slot, pl.ds(w, w)]
        part[s, :, :] = (jnp.dot(tg[2 * r], va[...], preferred_element_type=F32)
                         + jnp.dot(tg[2 * r + 1], vb[...], preferred_element_type=F32))
        ladder_copy(s).start()

        @pl.when(s == 0)
        def _():
            send(s4, smsg, s_copy, 1, ro, via)

        @pl.when(jnp.logical_and(s == 1, di == 1))
        def _():
            send(s4, smsg, s_copy, 1, 1, via)

        @pl.when(s == 2)
        def _():
            send(st4, pmsg, p_copy, 1, ro, via)

        @pl.when(jnp.logical_and(s == 3, home == 0))
        def _():
            send(st4, pmsg, p_copy, 1, di, via)

        @pl.when(s == 5)
        def _():
            pass_on()

        @pl.when(jnp.logical_and(s == 6, dg > 0))
        def _():
            across()

    landed(theirs, rrs).wait()
    landed(theirs, rs).wait()

    landed(tg.at[pl.ds(0, 3)], gs).wait()
    landed(tg.at[0, pl.ds(0, n)], fs).wait()
    landed(xr.at[pl.ds(0, 3)], xs).wait()
    all_m = mfull.at[pl.ds(0, 7 * q), pl.ds(0, n)]
    landed(all_m, mrs).wait()
    landed(all_m, ms).wait()
    m_mine = mfull[:, rows]

    @pl.loop(0, w // STEP)
    def _(s):
        lanes = pl.ds(pl.multiple_of(s * STEP, STEP), STEP)
        hole[:, lanes] = lax.dot_general(m_mine, tg[c, :, lanes], TN, preferred_element_type=F32)

    @pl.loop(0, 8)
    def _(i):
        line = pl.ds(pl.multiple_of(i * 16, 16), 16)
        line_r = pl.ds(pl.multiple_of(r * n + i * 16, 16), 16)
        mine = jnp.concatenate([part[s, line_r, :] for s in range(w // STEP)], axis=1)
        out_ref[line, :] = oovv[line, :].astype(F32) + (mine + theirs[line, :] + hole[line, :])

    landed(rmsg, rls).wait()
    landed(srecv.at[pl.ds(0, 80)], srs).wait()
    for i in range(8):
        for jh in range(2):
            line = slice(i * 16 + jh * 8, i * 16 + jh * 8 + 8)
            rows4 = [((2 * jh + cc) * 4 + i // 2) * 8 + i % 2 * 4 for cc in range(2)]
            out_ref[line, :] = out_ref[line, :] + jnp.concatenate([srecv[k:k + 4, :] for k in rows4], axis=0)

    @pl.when(home == 1)
    def _():
        landed(precv.at[pl.ds(0, 10)], prs).wait()

    @pl.when(home == 0)
    def _():
        landed(precv.at[pl.ds(0, 8)], prs).wait()

    zero4 = jnp.zeros((4, w), F32)
    for a in range(2):
        for j in range(4):
            m, rows4 = j // 2, slice(j % 2 * 4, j % 2 * 4 + 4)
            for kind, row in ((0, r), (1, o)):
                line = pl.ds(pl.multiple_of((a * 4 + j) * 16 + row * 8, 8), 8)
                both = [zero4 if kind == 0 and ih == a else precv[slot_p(kind, a, ih, m), rows4, :] for ih in range(2)]
                out_ref[line, :] = out_ref[line, :] + jnp.concatenate(both, axis=0)

    landed(smsg.at[pl.ds(0, 10)], ss).wait()

    @pl.when(home == 1)
    def _():
        landed(pmsg.at[pl.ds(0, 4)], ps).wait()

    @pl.when(home == 0)
    def _():
        landed(pmsg.at[pl.ds(0, 14)], ps).wait()


ANY = pl.BlockSpec(memory_space=pl.ANY)
DMA = pltpu.SemaphoreType.DMA


def sweep(t, oovv, vvvv, oooo, wd, wx):
    n, w = t.shape
    depth = vvvv.shape[0]
    V = pltpu.VMEM
    return pl.pallas_call(
        sweep_kernel,
        out_shape=jax.ShapeDtypeStruct((n, w), F32),
        in_specs=[ANY] * 6,
        out_specs=pl.BlockSpec(memory_space=pltpu.VMEM),
        scratch_shapes=[
            V((n, w), F32), V((n, w), BF16), V(oooo.shape, BF16), V((2,) + wd.shape, BF16),
            V((4, 2 * n, w), BF16),
            V((n, 2 * n), F32), V((4, n // 4, 2 * n), F32), V((2 * n, 2 * n), BF16), V((n, w), F32),
            V((n * PITCH, LANE), F32), V((OCC * LANE, 4 * LANE), BF16), V((wx.shape[1], wx.shape[0]), BF16),
            V((4, 2 * VIRT, 4 * LANE), F32), V((4, 4 * VIRT, 2 * LANE), F32),
            V((32 * PITCH, LANE), F32), V((32 * PITCH, LANE), F32),
            V((12, 8, w), F32), V((16, 8, w), F32), V((128, w), F32), V((16, 8, w), F32), V((4, 8, w), F32), V((32, w), F32),
            V((3, depth, STEP), BF16), V((n, w), F32), V((w // STEP, 2 * n, STEP), F32), V(wx.shape, F32),
            DMA((7,)), DMA, DMA((6,)), DMA, DMA((4,)), DMA, DMA, DMA, DMA,
            DMA, DMA, DMA, DMA, DMA, DMA, DMA((3,)), DMA, DMA,
        ],
        compiler_params=pltpu.CompilerParams(collective_id=0, has_side_effects=True, vmem_limit_bytes=46 << 20),
        name="sweep",
    )(*(pltpu.with_memory_space_constraint(a, pltpu.HBM) for a in (t, oovv, vvvv, oooo, wd, wx)))


def solution(mesh):
    def local_sweep(t_blk, d_blk, oovv_blk, vvvv_blk, oooo_full, wd_blk, wx_blk):
        return sweep(t_blk, oovv_blk, vvvv_blk, oooo_full, wd_blk, wx_blk) / d_blk

    amp = P("row", "col")
    wide = P(None, "col")
    return jax.shard_map(local_sweep, mesh=mesh, in_specs=(amp, amp, amp, amp, P(), wide, wide), out_specs=amp, check_vma=False)
```

```python
import jax
import jax.numpy as jnp
from jax import lax
from jax.experimental import pallas as pl
from jax.experimental.pallas import tpu as pltpu
from jax.sharding import PartitionSpec as P

MESH = pl.DeviceIdType.MESH
F32 = jnp.float32
BF16 = jnp.bfloat16
NT = (((1,), (1,)), ((), ()))
TN = (((0,), (0,)), ((), ()))

OCC = 16
VIRT = 96
LANE = 128
PITCH = 104
STEP = 256


def _dev(c, r):
    return {"col": c, "row": r}


def _rcopy(src, dst, ssem, rsem, dev):
    return pltpu.make_async_remote_copy(src, dst, ssem, rsem, device_id=dev, device_id_type=MESH)


def sweep_kernel(t_hbm, oovv_hbm, v_hbm, oooo_hbm, wd_hbm, wx_hbm, out_ref,
                 t32, oovv, oooo, ww, tg, xp, xr, mfull, hole, t4, wd4, wxt, ubuf, vbuf_s, s4, st4,
                 smsg, pmsg, srecv, precv, rmsg, rrecv, vv, theirs, part, wxf,
                 lsem, gs, gr, fs, fr, xs, xrs, ms, mrs, ss, srs, ps, prs, rls, rlr, vsem, rs, rrs):
    r, c = lax.axis_index("row"), lax.axis_index("col")
    x, y = c % 2, c // 2
    o = 1 - r
    nx, ny, dg = y * 2 + (1 - x), (1 - y) * 2 + x, (1 - y) * 2 + (1 - x)
    n, w = t32.shape
    h = w // 2
    h0, h1 = pl.ds(0, h), pl.ds(h, h)
    rows = pl.ds(pl.multiple_of(r * n, n), n)
    orows = pl.ds(pl.multiple_of(o * n, n), n)

    sem = pltpu.get_barrier_semaphore()
    for cc, rr in ((nx, r), (ny, r), (dg, r), (c, o), (nx, o), (ny, o), (dg, o)):
        pl.semaphore_signal(sem, inc=1, device_id=_dev(cc, rr), device_id_type=MESH)

    chunk = n // 4
    tloads = [pltpu.make_async_copy(t_hbm.at[pl.ds(k * chunk, chunk)], t32.at[pl.ds(k * chunk, chunk)], lsem.at[k])
              for k in range(4)]
    for cp in tloads:
        cp.start()
    oload = pltpu.make_async_copy(oovv_hbm, oovv, lsem.at[4])
    hload = pltpu.make_async_copy(oooo_hbm, oooo, lsem.at[5])
    wloads = [pltpu.make_async_copy(a, ww.at[k], lsem.at[6]) for k, a in enumerate((wd_hbm, wx_hbm))]
    for cp in (*wloads, oload, hload):
        cp.start()

    own = c // 2
    half = c % 2
    home = (own + r + 1) % 2
    via = home * nx + (1 - home) * ny
    past = home * ny + (1 - home) * nx
    ro = (home + half) % 2
    di = 1 - ro

    def slot_s(chip, ih, m):
        return pl.ds(pl.multiple_of(((chip * 2 + ih) * 2 + m) * 8, 8), 8)

    def slot_p(kind, a, ih, m):
        return ((kind * 2 + a) * 2 + ih) * 2 + m

    def vcopy(s, slot):
        lanes = pl.ds(pl.multiple_of(s * STEP, STEP), STEP)
        return pltpu.make_async_copy(v_hbm.at[:, lanes], vv.at[slot], vsem.at[slot])

    def landed(like, sem):
        return pltpu.make_async_copy(like, like, sem)

    for k in range(4):
        tloads[k].wait()
        tg[c, pl.ds(pl.multiple_of(r * n + k * chunk, chunk), chunk), :] = t32[k * chunk:(k + 1) * chunk, :].astype(BF16)

    pl.semaphore_wait(sem, 7)

    def tcopy(chip, lanes, k, dev):
        ref = tg.at[chip, rows, lanes]
        return _rcopy(ref, ref, gs, gr.at[k], dev)

    def fcopy(chip, lanes, p, dev):
        ref = tg.at[chip, pl.ds(pl.multiple_of(r * n + p * 32, 32), 32), lanes]
        return _rcopy(ref, ref, fs, fr.at[p], dev)

    whole = pl.ds(0, w)
    x0 = tcopy(c, h0, 1, _dev(nx, r))
    y1 = tcopy(c, h1, 2, _dev(ny, r))
    d_own = tcopy(c, whole, 0, _dev(c, o))
    x1 = tcopy(c, h1, 3, _dev(nx, r))
    y0 = tcopy(c, h0, 4, _dev(ny, r))
    x0.start()
    y1.start()
    d_own.start()
    x1.start()
    y0.start()
    vcopy(0, 0).start()
    vcopy(1, 1).start()

    def spread_rows(chip, ib, first, groups):
        for g in range(first, first + groups):
            tile = tg[chip, pl.ds(pl.multiple_of(r * n + ib * 16, 16), 16), g * 384:(g + 1) * 384].astype(F32)
            for e in range(4):
                slab = tile[:, e * VIRT:(e + 1) * VIRT]
                slab = jnp.concatenate([slab, jnp.zeros((16, LANE - VIRT), F32)], axis=1)
                for half in range(2):
                    start = (ib * 16 + half * 8) * PITCH + chip * 24 + g * 4 + e
                    t4[pl.ds(start, 8, stride=PITCH), :] = slab[half * 8:half * 8 + 8]

    def spread(chip, first, groups):
        @pl.loop(0, n // 16)
        def _(ib):
            spread_rows(chip, ib, first, groups)

    zero8 = jnp.zeros((8, w), F32)
    for m in range(2):
        srecv[slot_s(dg, ro, m), :] = zero8

    @pl.when(home == 0)
    def _():
        for m in range(2):
            precv[slot_p(0, 1 - half, half, m)] = zero8
            precv[slot_p(1, 1 - half, 1 - half, m)] = zero8

    spread(c, 0, 6)

    landed(ww, lsem.at[6]).wait()
    zrow = jnp.zeros((LANE - VIRT, 4 * LANE), BF16)

    @pl.loop(0, OCC)
    def _(k):
        blk = ww[0, pl.ds(pl.multiple_of(k * VIRT, 16), VIRT), :].astype(F32)
        parts = []
        for j in range(4):
            parts += [blk[:, j * VIRT:(j + 1) * VIRT], jnp.zeros((VIRT, LANE - VIRT), F32)]
        wd4[pl.ds(pl.multiple_of(k * LANE, LANE), VIRT), :] = jnp.concatenate(parts, axis=1).astype(BF16)
        wd4[pl.ds(pl.multiple_of(k * LANE + VIRT, 32), LANE - VIRT), :] = zrow
        wxf[pl.ds(pl.multiple_of(k * VIRT, 16), VIRT), :] = ww[1, pl.ds(pl.multiple_of(k * VIRT, 16), VIRT), :].astype(F32)

    for s, chip in enumerate((c, nx, ny, dg)):
        for b in range(3):
            blk = jnp.concatenate(
                [wxf[pl.ds(pl.multiple_of(k * VIRT + chip * 24, 8), 24), b * LANE:(b + 1) * LANE] for k in range(OCC)],
                axis=0)
            wxt[b * LANE:(b + 1) * LANE, s * 384:(s + 1) * 384] = blk.astype(BF16).T

    oload.wait()
    hload.wait()
    d_own.wait_recv()
    xp[...] = lax.dot_general(oovv[...], tg[c], NT, preferred_element_type=F32)

    def direct_rows(chip, i0, count):
        lhs = jnp.concatenate(
            [jnp.concatenate(
                [t4[pl.ds(pl.multiple_of(((i0 + i) * OCC + k) * PITCH + chip * 24, 8), 24), :] for i in range(count)],
                axis=0)
             for k in range(OCC)], axis=1).astype(BF16)
        return jnp.dot(lhs, wd4[...], preferred_element_type=F32)

    def direct(chip):
        ubuf[chip, :, :] = direct_rows(chip, 0, 8)

    def exchange_pair(chips, first, i2):
        halves = []
        for e in range(2):
            halves.append(jnp.concatenate(
                [t4[pl.ds(pl.multiple_of(((2 * i2 + e) * OCC + k) * PITCH + chip * 24, 8), 24), :]
                 for chip in chips for k in range(OCC)], axis=0))
        rhs = jnp.concatenate(halves, axis=1).astype(BF16)
        prod = jnp.dot(wxt[:, first * 384:(first + len(chips)) * 384], rhs, preferred_element_type=F32)
        vbuf_s[i2, :, :] = prod if first == 0 else vbuf_s[i2, :, :] + prod

    def exchange(chips, first):
        @pl.loop(0, 4)
        def _(i2):
            exchange_pair(chips, first, i2)

    direct(c)

    x0.wait_recv()
    for p in range(4):
        fcopy(nx, h0, p, _dev(ny, r)).start()
    y1.wait_recv()
    for p in range(4):
        fcopy(ny, h1, p, _dev(nx, r)).start()
    q = n // 4
    for cc in (nx, ny, dg):
        cp = _rcopy(xp.at[pl.ds(pl.multiple_of(cc * q, q), q)], xr.at[c], xs, xrs, _dev(cc, r))
        cp.start()
    xr[c, :, :] = xp[pl.ds(pl.multiple_of(c * q, q), q), :]
    spread(nx, 0, 3)
    spread(ny, 3, 3)
    x1.wait_recv()
    d_x = tcopy(nx, whole, 5, _dev(c, o))
    d_x.start()
    y0.wait_recv()
    d_y = tcopy(ny, whole, 5, _dev(c, o))
    d_y.start()
    spread(nx, 3, 3)
    spread(ny, 0, 3)
    direct(nx)
    direct(ny)
    exchange((c, nx, ny), 0)

    def s_rows(i, j):
        return pl.ds(pl.multiple_of((i * 4 + j) * PITCH, 8), VIRT)

    def t_rows(i, j):
        return pl.ds(pl.multiple_of(((i // 4) * 16 + j * 4 + i % 4) * PITCH, 8), VIRT)

    def block(i, j):
        direct_part = jnp.concatenate(
            [ubuf[chip, pl.ds(pl.multiple_of(i * 24, 8), 24), pl.ds(pl.multiple_of(j * LANE, LANE), LANE)]
             for chip in range(4)], axis=0)
        return direct_part - vbuf_s[
            i // 2, pl.ds(pl.multiple_of(j * VIRT, 8), VIRT), pl.ds(pl.multiple_of((i % 2) * LANE, LANE), LANE)]

    def fill_s(ih):
        @pl.loop(0, 4)
        def _(j):
            for e in range(4):
                s4[s_rows(ih * 4 + e, j), :] = block(ih * 4 + e, j)

    def fill_t(ih):
        @pl.loop(0, 4)
        def _(j):
            for e in range(4):
                st4[t_rows(ih * 4 + e, j), :VIRT] = s4[s_rows(ih * 4 + e, j), :].T[:VIRT, :]

    def put(src, ih, m, chip, dst):
        first = (ih * 16 + m * 8) * PITCH + chip * 24
        for g in range(6):
            vals = [src[pl.ds(first + g * 4 + e, 8, stride=PITCH), :][:, :VIRT] for e in range(4)]
            dst[:, g * 384:(g + 1) * 384] = jnp.concatenate(vals, axis=1)

    def s_copy(slot, ih, m, chip):
        buf = smsg.at[slot * 4 + ih * 2 + m]
        return _rcopy(buf, srecv.at[slot_s(c, ih, m)], ss, srs, _dev(chip, r))

    def p_copy(slot, ih, m, chip):
        buf = pmsg.at[slot * 4 + ih * 2 + m]
        return _rcopy(buf, precv.at[slot_p(1 - home, half, ih, m)], ps, prs, _dev(chip, own))

    def relay(kind, src):
        @pl.loop(0, 2)
        def _(m):
            put(src, ro, m, dg, rmsg.at[kind * 2 + m])
            to = rrecv.at[pl.ds(pl.multiple_of((kind * 2 + m) * 8, 8), 8)]
            _rcopy(rmsg.at[kind * 2 + m], to, rls, rlr, _dev(via, own)).start()

    def send(src, msg, copy, slot, ih, chip):
        @pl.loop(0, 2)
        def _(m):
            put(src, ih, m, chip, msg.at[slot * 4 + ih * 2 + m])
            copy(slot, ih, m, chip).start()

    def mirror():
        @pl.loop(0, 4)
        def _(j):
            for e in range(4):
                at = s_rows(half * 4 + e, j)
                s4[at, :VIRT] = s4[at, :VIRT] + block(half * 4 + j, e).T[:VIRT, :]

    @pl.loop(0, 4)
    def _(p):
        landed(tg.at[dg, pl.ds(0, n // 4)], fr.at[p]).wait()
        for ib in range(2):
            spread_rows(dg, 2 * p + ib, 0, 6)
        ubuf[dg, pl.ds(pl.multiple_of(p * 48, 16), 48), :] = direct_rows(dg, 2 * p, 2)
        exchange_pair((dg,), 3, p)

        @pl.when(p == 1)
        def _():
            fill_s(0)

            @pl.when(ro == 0)
            def _():
                relay(0, s4)

            @pl.when(jnp.logical_and(ro == 1, home == 0))
            def _():
                send(s4, smsg, s_copy, 1, 0, via)

        @pl.when(jnp.logical_and(p == 2, ro == 0))
        def _():
            send(s4, smsg, s_copy, 1, 0, via)

        @pl.when(jnp.logical_and(p == 2, jnp.logical_and(ro == 1, home == 1)))
        def _():
            mirror()
            send(s4, smsg, s_copy, 1, 0, via)

    d_d = tcopy(dg, whole, 5, _dev(c, o))
    d_d.start()

    fill_s(1)

    @pl.when(ro == 1)
    def _():
        relay(0, s4)

    fill_t(ro)
    relay(1, st4)

    landed(xr.at[pl.ds(0, 3)], xrs).wait()
    xsum = (xr[0] + xr[1]) + (xr[2] + xr[3])
    krows = pl.ds(pl.multiple_of(r * n + c * q, q), q)
    mfull[krows, :] = (oooo[krows, :].astype(F32) + 0.5 * xsum).astype(BF16)
    for cc, rr in ((nx, r), (ny, r), (dg, r), (c, o), (nx, o), (ny, o), (dg, o)):
        part_m = mfull.at[krows, pl.ds(pl.multiple_of(rr * n, n), n)]
        _rcopy(part_m, part_m, ms, mrs, _dev(cc, rr)).start()

    @pl.when(jnp.logical_and(home == 1, di == 1))
    def _():
        mirror()

    send(s4, smsg, s_copy, 2, di, past)

    def across():
        send(s4, smsg, s_copy, 0, di, dg)

        @pl.when(home == 0)
        def _():
            send(st4, pmsg, p_copy, 0, di, dg)

    @pl.when(home == 0)
    def _():
        fill_t(di)
        send(st4, pmsg, p_copy, 2, di, past)

    @pl.when(dg == 0)
    def _():
        across()

    @pl.when(home == 0)
    def _():
        send(st4, pmsg, p_copy, 3, ro, c)
        send(st4, pmsg, p_copy, 3, di, c)

    @pl.loop(0, 2)
    def _(m):
        for ih in range(2):
            put(s4, ih, m, c, srecv.at[slot_s(c, ih, m)])

    @pl.when(home == 1)
    def _():
        @pl.loop(0, 2)
        def _(m):
            put(st4, ro, m, c, precv.at[slot_p(0, half, ro, m)])

    def pass_on():
        landed(rrecv, rlr).wait()
        for kind, (src, msg, copy) in ((1, (s4, smsg, s_copy)), (0, (st4, pmsg, p_copy))):
            for m in range(2):
                buf = msg.at[2 * 4 + ro * 2 + m]
                put(src, ro, m, past, buf)
                buf[...] = buf[...] + rrecv[(kind * 2 + m) * 8:(kind * 2 + m + 1) * 8, :]
                copy(2, ro, m, past).start()

    landed(tg.at[pl.ds(0, 3), pl.ds(0, n)], gr.at[5]).wait()

    def ladder_copy(s):
        lanes = pl.ds(pl.multiple_of(s * STEP, STEP), STEP)
        return _rcopy(part.at[s, orows], theirs.at[:, lanes], rs, rrs, _dev(c, o))

    @pl.loop(0, w // STEP)
    def _(s):
        slot = s % 3

        @pl.when(s + 2 < w // STEP)
        def _():
            vcopy(s + 2, (s + 2) % 3).start()

        vcopy(s, slot).wait()
        va, vb = vv.at[slot, pl.ds(0, w)], vv.at[slot, pl.ds(w, w)]
        part[s, :, :] = (jnp.dot(tg[2 * r], va[...], preferred_element_type=F32)
                         + jnp.dot(tg[2 * r + 1], vb[...], preferred_element_type=F32))
        ladder_copy(s).start()

        @pl.when(jnp.logical_and(s == 0, ro == 1))
        def _():
            send(s4, smsg, s_copy, 1, 1, via)

        @pl.when(jnp.logical_and(s == 1, di == 1))
        def _():
            send(s4, smsg, s_copy, 1, 1, via)

        @pl.when(s == 2)
        def _():
            send(st4, pmsg, p_copy, 1, ro, via)

        @pl.when(jnp.logical_and(s == 3, home == 0))
        def _():
            send(st4, pmsg, p_copy, 1, di, via)

        @pl.when(s == 5)
        def _():
            pass_on()

        @pl.when(jnp.logical_and(s == 6, dg > 0))
        def _():
            across()

    landed(theirs, rrs).wait()
    landed(theirs, rs).wait()

    landed(tg.at[pl.ds(0, 3)], gs).wait()
    landed(tg.at[0, pl.ds(0, n)], fs).wait()
    landed(xr.at[pl.ds(0, 3)], xs).wait()
    all_m = mfull.at[pl.ds(0, 7 * q), pl.ds(0, n)]
    landed(all_m, mrs).wait()
    landed(all_m, ms).wait()
    m_mine = mfull[:, rows]

    @pl.loop(0, w // STEP)
    def _(s):
        lanes = pl.ds(pl.multiple_of(s * STEP, STEP), STEP)
        hole[:, lanes] = lax.dot_general(m_mine, tg[c, :, lanes], TN, preferred_element_type=F32)

    @pl.loop(0, 8)
    def _(i):
        line = pl.ds(pl.multiple_of(i * 16, 16), 16)
        line_r = pl.ds(pl.multiple_of(r * n + i * 16, 16), 16)
        mine = jnp.concatenate([part[s, line_r, :] for s in range(w // STEP)], axis=1)
        out_ref[line, :] = oovv[line, :].astype(F32) + (mine + theirs[line, :] + hole[line, :])

    landed(rmsg, rls).wait()
    landed(srecv.at[pl.ds(0, 80)], srs).wait()
    for i in range(8):
        for jh in range(2):
            line = slice(i * 16 + jh * 8, i * 16 + jh * 8 + 8)
            rows4 = [((2 * jh + cc) * 4 + i // 2) * 8 + i % 2 * 4 for cc in range(2)]
            out_ref[line, :] = out_ref[line, :] + jnp.concatenate([srecv[k:k + 4, :] for k in rows4], axis=0)

    @pl.when(home == 1)
    def _():
        landed(precv.at[pl.ds(0, 10)], prs).wait()

    @pl.when(home == 0)
    def _():
        landed(precv.at[pl.ds(0, 8)], prs).wait()

    zero4 = jnp.zeros((4, w), F32)
    for a in range(2):
        for j in range(4):
            m, rows4 = j // 2, slice(j % 2 * 4, j % 2 * 4 + 4)
            for kind, row in ((0, r), (1, o)):
                line = pl.ds(pl.multiple_of((a * 4 + j) * 16 + row * 8, 8), 8)
                both = [zero4 if kind == 0 and ih == a else precv[slot_p(kind, a, ih, m), rows4, :] for ih in range(2)]
                out_ref[line, :] = out_ref[line, :] + jnp.concatenate(both, axis=0)

    landed(smsg.at[pl.ds(0, 10)], ss).wait()

    @pl.when(home == 1)
    def _():
        landed(pmsg.at[pl.ds(0, 4)], ps).wait()

    @pl.when(home == 0)
    def _():
        landed(pmsg.at[pl.ds(0, 14)], ps).wait()


ANY = pl.BlockSpec(memory_space=pl.ANY)
DMA = pltpu.SemaphoreType.DMA


def sweep(t, oovv, vvvv, oooo, wd, wx):
    n, w = t.shape
    depth = vvvv.shape[0]
    V = pltpu.VMEM
    return pl.pallas_call(
        sweep_kernel,
        out_shape=jax.ShapeDtypeStruct((n, w), F32),
        in_specs=[ANY] * 6,
        out_specs=pl.BlockSpec(memory_space=pltpu.VMEM),
        scratch_shapes=[
            V((n, w), F32), V((n, w), BF16), V(oooo.shape, BF16), V((2,) + wd.shape, BF16),
            V((4, 2 * n, w), BF16),
            V((n, 2 * n), F32), V((4, n // 4, 2 * n), F32), V((2 * n, 2 * n), BF16), V((n, w), F32),
            V((n * PITCH, LANE), F32), V((OCC * LANE, 4 * LANE), BF16), V((wx.shape[1], wx.shape[0]), BF16),
            V((4, 2 * VIRT, 4 * LANE), F32), V((4, 4 * VIRT, 2 * LANE), F32),
            V((32 * PITCH, LANE), F32), V((32 * PITCH, LANE), F32),
            V((12, 8, w), F32), V((16, 8, w), F32), V((128, w), F32), V((16, 8, w), F32), V((4, 8, w), F32), V((32, w), F32),
            V((3, depth, STEP), BF16), V((n, w), F32), V((w // STEP, 2 * n, STEP), F32), V(wx.shape, F32),
            DMA((7,)), DMA, DMA((6,)), DMA, DMA((4,)), DMA, DMA, DMA, DMA,
            DMA, DMA, DMA, DMA, DMA, DMA, DMA((3,)), DMA, DMA,
        ],
        compiler_params=pltpu.CompilerParams(collective_id=0, has_side_effects=True, vmem_limit_bytes=46 << 20),
        name="sweep",
    )(*(pltpu.with_memory_space_constraint(a, pltpu.HBM) for a in (t, oovv, vvvv, oooo, wd, wx)))


def solution(mesh):
    def local_sweep(t_blk, d_blk, oovv_blk, vvvv_blk, oooo_full, wd_blk, wx_blk):
        return sweep(t_blk, oovv_blk, vvvv_blk, oooo_full, wd_blk, wx_blk) / d_blk

    amp = P("row", "col")
    wide = P(None, "col")
    return jax.shard_map(local_sweep, mesh=mesh, in_specs=(amp, amp, amp, amp, P(), wide, wide), out_specs=amp, check_vma=False)
```

```python
import jax
import jax.numpy as jnp
from jax import lax
from jax.experimental import pallas as pl
from jax.experimental.pallas import tpu as pltpu
from jax.sharding import PartitionSpec as P

MESH = pl.DeviceIdType.MESH
F32 = jnp.float32
BF16 = jnp.bfloat16
NT = (((1,), (1,)), ((), ()))
TN = (((0,), (0,)), ((), ()))

OCC = 16
VIRT = 96
LANE = 128
PITCH = 104
STEP = 256


def _dev(c, r):
    return {"col": c, "row": r}


def _rcopy(src, dst, ssem, rsem, dev):
    return pltpu.make_async_remote_copy(src, dst, ssem, rsem, device_id=dev, device_id_type=MESH)


def sweep_kernel(t_hbm, oovv_hbm, v_hbm, oooo_hbm, wd_hbm, wx_hbm, out_ref,
                 t32, oovv, oooo, ww, tg, xp, xr, mfull, hole, t4, wd4, wxt, ubuf, vbuf_s, s4, st4,
                 smsg, pmsg, srecv, precv, rmsg, rrecv, vv, theirs, part, wxf,
                 lsem, gs, gr, fs, fr, xs, xrs, ms, mrs, ss, srs, ps, prs, rls, rlr, vsem, rs, rrs):
    r, c = lax.axis_index("row"), lax.axis_index("col")
    x, y = c % 2, c // 2
    o = 1 - r
    nx, ny, dg = y * 2 + (1 - x), (1 - y) * 2 + x, (1 - y) * 2 + (1 - x)
    n, w = t32.shape
    h = w // 2
    h0, h1 = pl.ds(0, h), pl.ds(h, h)
    rows = pl.ds(pl.multiple_of(r * n, n), n)
    orows = pl.ds(pl.multiple_of(o * n, n), n)

    sem = pltpu.get_barrier_semaphore()
    for cc, rr in ((nx, r), (ny, r), (dg, r), (c, o), (nx, o), (ny, o), (dg, o)):
        pl.semaphore_signal(sem, inc=1, device_id=_dev(cc, rr), device_id_type=MESH)

    chunk = n // 4
    tloads = [pltpu.make_async_copy(t_hbm.at[pl.ds(k * chunk, chunk)], t32.at[pl.ds(k * chunk, chunk)], lsem.at[k])
              for k in range(4)]
    for cp in tloads:
        cp.start()
    oload = pltpu.make_async_copy(oovv_hbm, oovv, lsem.at[4])
    hload = pltpu.make_async_copy(oooo_hbm, oooo, lsem.at[5])
    wloads = [pltpu.make_async_copy(a, ww.at[k], lsem.at[6]) for k, a in enumerate((wd_hbm, wx_hbm))]
    for cp in (*wloads, oload, hload):
        cp.start()

    own = c // 2
    half = c % 2
    home = (own + r + 1) % 2
    via = home * nx + (1 - home) * ny
    past = home * ny + (1 - home) * nx
    ro = (home + half) % 2
    di = 1 - ro

    def slot_s(chip, ih, m):
        return pl.ds(pl.multiple_of(((chip * 2 + ih) * 2 + m) * 8, 8), 8)

    def slot_p(kind, a, ih, m):
        return ((kind * 2 + a) * 2 + ih) * 2 + m

    def vcopy(s, slot):
        lanes = pl.ds(pl.multiple_of(s * STEP, STEP), STEP)
        return pltpu.make_async_copy(v_hbm.at[:, lanes], vv.at[slot], vsem.at[slot])

    def landed(like, sem):
        return pltpu.make_async_copy(like, like, sem)

    for k in range(4):
        tloads[k].wait()
        tg[c, pl.ds(pl.multiple_of(r * n + k * chunk, chunk), chunk), :] = t32[k * chunk:(k + 1) * chunk, :].astype(BF16)

    pl.semaphore_wait(sem, 7)

    def tcopy(chip, lanes, k, dev):
        ref = tg.at[chip, rows, lanes]
        return _rcopy(ref, ref, gs, gr.at[k], dev)

    def fcopy(chip, lanes, p, dev):
        ref = tg.at[chip, pl.ds(pl.multiple_of(r * n + p * 32, 32), 32), lanes]
        return _rcopy(ref, ref, fs, fr.at[p], dev)

    whole = pl.ds(0, w)
    x0 = tcopy(c, h0, 1, _dev(nx, r))
    y1 = tcopy(c, h1, 2, _dev(ny, r))
    d_own = tcopy(c, whole, 0, _dev(c, o))
    x1 = tcopy(c, h1, 3, _dev(nx, r))
    y0 = tcopy(c, h0, 4, _dev(ny, r))
    x0.start()
    y1.start()
    d_own.start()
    x1.start()
    y0.start()
    vcopy(0, 0).start()
    vcopy(1, 1).start()

    def spread_rows(chip, ib, first, groups):
        for g in range(first, first + groups):
            tile = tg[chip, pl.ds(pl.multiple_of(r * n + ib * 16, 16), 16), g * 384:(g + 1) * 384].astype(F32)
            for e in range(4):
                slab = tile[:, e * VIRT:(e + 1) * VIRT]
                slab = jnp.concatenate([slab, jnp.zeros((16, LANE - VIRT), F32)], axis=1)
                for half in range(2):
                    start = (ib * 16 + half * 8) * PITCH + chip * 24 + g * 4 + e
                    t4[pl.ds(start, 8, stride=PITCH), :] = slab[half * 8:half * 8 + 8]

    def spread(chip, first, groups):
        @pl.loop(0, n // 16)
        def _(ib):
            spread_rows(chip, ib, first, groups)

    zero8 = jnp.zeros((8, w), F32)
    for m in range(2):
        srecv[slot_s(dg, ro, m), :] = zero8

    @pl.when(home == 0)
    def _():
        for m in range(2):
            precv[slot_p(0, 1 - half, half, m)] = zero8
            precv[slot_p(1, 1 - half, 1 - half, m)] = zero8

    spread(c, 0, 6)

    landed(ww, lsem.at[6]).wait()
    zrow = jnp.zeros((LANE - VIRT, 4 * LANE), BF16)

    @pl.loop(0, OCC)
    def _(k):
        blk = ww[0, pl.ds(pl.multiple_of(k * VIRT, 16), VIRT), :].astype(F32)
        parts = []
        for j in range(4):
            parts += [blk[:, j * VIRT:(j + 1) * VIRT], jnp.zeros((VIRT, LANE - VIRT), F32)]
        wd4[pl.ds(pl.multiple_of(k * LANE, LANE), VIRT), :] = jnp.concatenate(parts, axis=1).astype(BF16)
        wd4[pl.ds(pl.multiple_of(k * LANE + VIRT, 32), LANE - VIRT), :] = zrow
        wxf[pl.ds(pl.multiple_of(k * VIRT, 16), VIRT), :] = ww[1, pl.ds(pl.multiple_of(k * VIRT, 16), VIRT), :].astype(F32)

    for s, chip in enumerate((c, nx, ny, dg)):
        for b in range(3):
            blk = jnp.concatenate(
                [wxf[pl.ds(pl.multiple_of(k * VIRT + chip * 24, 8), 24), b * LANE:(b + 1) * LANE] for k in range(OCC)],
                axis=0)
            wxt[b * LANE:(b + 1) * LANE, s * 384:(s + 1) * 384] = blk.astype(BF16).T

    oload.wait()
    hload.wait()
    d_own.wait_recv()
    xp[...] = lax.dot_general(oovv[...], tg[c], NT, preferred_element_type=F32)

    def direct_rows(chip, i0, count):
        lhs = jnp.concatenate(
            [jnp.concatenate(
                [t4[pl.ds(pl.multiple_of(((i0 + i) * OCC + k) * PITCH + chip * 24, 8), 24), :] for i in range(count)],
                axis=0)
             for k in range(OCC)], axis=1).astype(BF16)
        return jnp.dot(lhs, wd4[...], preferred_element_type=F32)

    def direct(chip):
        ubuf[chip, :, :] = direct_rows(chip, 0, 8)

    def exchange_pair(chips, first, i2):
        halves = []
        for e in range(2):
            halves.append(jnp.concatenate(
                [t4[pl.ds(pl.multiple_of(((2 * i2 + e) * OCC + k) * PITCH + chip * 24, 8), 24), :]
                 for chip in chips for k in range(OCC)], axis=0))
        rhs = jnp.concatenate(halves, axis=1).astype(BF16)
        prod = jnp.dot(wxt[:, first * 384:(first + len(chips)) * 384], rhs, preferred_element_type=F32)
        vbuf_s[i2, :, :] = prod if first == 0 else vbuf_s[i2, :, :] + prod

    def exchange(chips, first):
        @pl.loop(0, 4)
        def _(i2):
            exchange_pair(chips, first, i2)

    direct(c)

    x0.wait_recv()
    for p in range(4):
        fcopy(nx, h0, p, _dev(ny, r)).start()
    y1.wait_recv()
    for p in range(4):
        fcopy(ny, h1, p, _dev(nx, r)).start()
    q = n // 4
    for cc in (nx, ny, dg):
        cp = _rcopy(xp.at[pl.ds(pl.multiple_of(cc * q, q), q)], xr.at[c], xs, xrs, _dev(cc, r))
        cp.start()
    xr[c, :, :] = xp[pl.ds(pl.multiple_of(c * q, q), q), :]
    spread(nx, 0, 3)
    spread(ny, 3, 3)
    x1.wait_recv()
    d_x = tcopy(nx, whole, 5, _dev(c, o))
    d_x.start()
    y0.wait_recv()
    d_y = tcopy(ny, whole, 5, _dev(c, o))
    d_y.start()
    spread(nx, 3, 3)
    spread(ny, 0, 3)
    direct(nx)
    direct(ny)
    exchange((c, nx, ny), 0)

    def s_rows(i, j):
        return pl.ds(pl.multiple_of((i * 4 + j) * PITCH, 8), VIRT)

    def t_rows(i, j):
        return pl.ds(pl.multiple_of(((i // 4) * 16 + j * 4 + i % 4) * PITCH, 8), VIRT)

    def block(i, j):
        direct_part = jnp.concatenate(
            [ubuf[chip, pl.ds(pl.multiple_of(i * 24, 8), 24), pl.ds(pl.multiple_of(j * LANE, LANE), LANE)]
             for chip in range(4)], axis=0)
        return direct_part - vbuf_s[
            i // 2, pl.ds(pl.multiple_of(j * VIRT, 8), VIRT), pl.ds(pl.multiple_of((i % 2) * LANE, LANE), LANE)]

    def fill_s(ih):
        @pl.loop(0, 4)
        def _(j):
            for e in range(4):
                s4[s_rows(ih * 4 + e, j), :] = block(ih * 4 + e, j)

    def fill_t(ih):
        @pl.loop(0, 4)
        def _(j):
            for e in range(4):
                st4[t_rows(ih * 4 + e, j), :VIRT] = s4[s_rows(ih * 4 + e, j), :].T[:VIRT, :]

    def put(src, ih, m, chip, dst):
        first = (ih * 16 + m * 8) * PITCH + chip * 24
        for g in range(6):
            vals = [src[pl.ds(first + g * 4 + e, 8, stride=PITCH), :][:, :VIRT] for e in range(4)]
            dst[:, g * 384:(g + 1) * 384] = jnp.concatenate(vals, axis=1)

    def s_copy(slot, ih, m, chip):
        buf = smsg.at[slot * 4 + ih * 2 + m]
        return _rcopy(buf, srecv.at[slot_s(c, ih, m)], ss, srs, _dev(chip, r))

    def p_copy(slot, ih, m, chip):
        buf = pmsg.at[slot * 4 + ih * 2 + m]
        return _rcopy(buf, precv.at[slot_p(1 - home, half, ih, m)], ps, prs, _dev(chip, own))

    def relay(kind, src):
        @pl.loop(0, 2)
        def _(m):
            put(src, ro, m, dg, rmsg.at[kind * 2 + m])
            to = rrecv.at[pl.ds(pl.multiple_of((kind * 2 + m) * 8, 8), 8)]
            _rcopy(rmsg.at[kind * 2 + m], to, rls, rlr, _dev(via, own)).start()

    def send(src, msg, copy, slot, ih, chip):
        @pl.loop(0, 2)
        def _(m):
            put(src, ih, m, chip, msg.at[slot * 4 + ih * 2 + m])
            copy(slot, ih, m, chip).start()

    def mirror():
        @pl.loop(0, 4)
        def _(j):
            for e in range(4):
                at = s_rows(half * 4 + e, j)
                s4[at, :VIRT] = s4[at, :VIRT] + block(half * 4 + j, e).T[:VIRT, :]

    @pl.loop(0, 4)
    def _(p):
        landed(tg.at[dg, pl.ds(0, n // 4)], fr.at[p]).wait()
        for ib in range(2):
            spread_rows(dg, 2 * p + ib, 0, 6)
        ubuf[dg, pl.ds(pl.multiple_of(p * 48, 16), 48), :] = direct_rows(dg, 2 * p, 2)
        exchange_pair((dg,), 3, p)

        @pl.when(p == 1)
        def _():
            fill_s(0)

            @pl.when(ro == 0)
            def _():
                relay(0, s4)

            @pl.when(jnp.logical_and(ro == 1, home == 0))
            def _():
                send(s4, smsg, s_copy, 1, 0, via)

        @pl.when(jnp.logical_and(p == 2, jnp.logical_and(ro == 1, home == 1)))
        def _():
            mirror()
            send(s4, smsg, s_copy, 1, 0, via)

    d_d = tcopy(dg, whole, 5, _dev(c, o))
    d_d.start()

    fill_s(1)

    @pl.when(ro == 1)
    def _():
        relay(0, s4)

    fill_t(ro)
    relay(1, st4)

    landed(xr.at[pl.ds(0, 3)], xrs).wait()
    xsum = (xr[0] + xr[1]) + (xr[2] + xr[3])
    krows = pl.ds(pl.multiple_of(r * n + c * q, q), q)
    mfull[krows, :] = (oooo[krows, :].astype(F32) + 0.5 * xsum).astype(BF16)
    for cc, rr in ((nx, r), (ny, r), (dg, r), (c, o), (nx, o), (ny, o), (dg, o)):
        part_m = mfull.at[krows, pl.ds(pl.multiple_of(rr * n, n), n)]
        _rcopy(part_m, part_m, ms, mrs, _dev(cc, rr)).start()

    @pl.when(jnp.logical_and(home == 1, di == 1))
    def _():
        mirror()

    send(s4, smsg, s_copy, 2, di, past)

    def across():
        send(s4, smsg, s_copy, 0, di, dg)

        @pl.when(home == 0)
        def _():
            send(st4, pmsg, p_copy, 0, di, dg)

    @pl.when(home == 0)
    def _():
        fill_t(di)
        send(st4, pmsg, p_copy, 2, di, past)

    @pl.when(dg == 0)
    def _():
        across()

    @pl.when(home == 0)
    def _():
        send(st4, pmsg, p_copy, 3, ro, c)
        send(st4, pmsg, p_copy, 3, di, c)

    @pl.loop(0, 2)
    def _(m):
        for ih in range(2):
            put(s4, ih, m, c, srecv.at[slot_s(c, ih, m)])

    @pl.when(home == 1)
    def _():
        @pl.loop(0, 2)
        def _(m):
            put(st4, ro, m, c, precv.at[slot_p(0, half, ro, m)])

    def pass_on():
        landed(rrecv, rlr).wait()
        for kind, (src, msg, copy) in ((1, (s4, smsg, s_copy)), (0, (st4, pmsg, p_copy))):
            for m in range(2):
                buf = msg.at[2 * 4 + ro * 2 + m]
                put(src, ro, m, past, buf)
                buf[...] = buf[...] + rrecv[(kind * 2 + m) * 8:(kind * 2 + m + 1) * 8, :]
                copy(2, ro, m, past).start()

    landed(tg.at[pl.ds(0, 3), pl.ds(0, n)], gr.at[5]).wait()

    def ladder_copy(s):
        lanes = pl.ds(pl.multiple_of(s * STEP, STEP), STEP)
        return _rcopy(part.at[s, orows], theirs.at[:, lanes], rs, rrs, _dev(c, o))

    @pl.loop(0, w // STEP)
    def _(s):
        slot = s % 3

        @pl.when(s + 2 < w // STEP)
        def _():
            vcopy(s + 2, (s + 2) % 3).start()

        vcopy(s, slot).wait()
        va, vb = vv.at[slot, pl.ds(0, w)], vv.at[slot, pl.ds(w, w)]
        part[s, :, :] = (jnp.dot(tg[2 * r], va[...], preferred_element_type=F32)
                         + jnp.dot(tg[2 * r + 1], vb[...], preferred_element_type=F32))
        ladder_copy(s).start()

        @pl.when(s == 0)
        def _():
            send(s4, smsg, s_copy, 1, ro, via)

        @pl.when(jnp.logical_and(s == 1, di == 1))
        def _():
            send(s4, smsg, s_copy, 1, 1, via)

        @pl.when(s == 2)
        def _():
            send(st4, pmsg, p_copy, 1, ro, via)

        @pl.when(jnp.logical_and(s == 3, home == 0))
        def _():
            send(st4, pmsg, p_copy, 1, di, via)

        @pl.when(s == 4)
        def _():
            pass_on()

        @pl.when(jnp.logical_and(s == 7, dg > 0))
        def _():
            across()

    landed(theirs, rrs).wait()
    landed(theirs, rs).wait()

    landed(tg.at[pl.ds(0, 3)], gs).wait()
    landed(tg.at[0, pl.ds(0, n)], fs).wait()
    landed(xr.at[pl.ds(0, 3)], xs).wait()
    all_m = mfull.at[pl.ds(0, 7 * q), pl.ds(0, n)]
    landed(all_m, mrs).wait()
    landed(all_m, ms).wait()
    m_mine = mfull[:, rows]

    @pl.loop(0, w // STEP)
    def _(s):
        lanes = pl.ds(pl.multiple_of(s * STEP, STEP), STEP)
        hole[:, lanes] = lax.dot_general(m_mine, tg[c, :, lanes], TN, preferred_element_type=F32)

    @pl.loop(0, 8)
    def _(i):
        line = pl.ds(pl.multiple_of(i * 16, 16), 16)
        line_r = pl.ds(pl.multiple_of(r * n + i * 16, 16), 16)
        mine = jnp.concatenate([part[s, line_r, :] for s in range(w // STEP)], axis=1)
        out_ref[line, :] = oovv[line, :].astype(F32) + (mine + theirs[line, :] + hole[line, :])

    landed(rmsg, rls).wait()
    landed(srecv.at[pl.ds(0, 80)], srs).wait()
    for i in range(8):
        for jh in range(2):
            line = slice(i * 16 + jh * 8, i * 16 + jh * 8 + 8)
            rows4 = [((2 * jh + cc) * 4 + i // 2) * 8 + i % 2 * 4 for cc in range(2)]
            out_ref[line, :] = out_ref[line, :] + jnp.concatenate([srecv[k:k + 4, :] for k in rows4], axis=0)

    @pl.when(home == 1)
    def _():
        landed(precv.at[pl.ds(0, 10)], prs).wait()

    @pl.when(home == 0)
    def _():
        landed(precv.at[pl.ds(0, 8)], prs).wait()

    zero4 = jnp.zeros((4, w), F32)
    for a in range(2):
        for j in range(4):
            m, rows4 = j // 2, slice(j % 2 * 4, j % 2 * 4 + 4)
            for kind, row in ((0, r), (1, o)):
                line = pl.ds(pl.multiple_of((a * 4 + j) * 16 + row * 8, 8), 8)
                both = [zero4 if kind == 0 and ih == a else precv[slot_p(kind, a, ih, m), rows4, :] for ih in range(2)]
                out_ref[line, :] = out_ref[line, :] + jnp.concatenate(both, axis=0)

    landed(smsg.at[pl.ds(0, 10)], ss).wait()

    @pl.when(home == 1)
    def _():
        landed(pmsg.at[pl.ds(0, 4)], ps).wait()

    @pl.when(home == 0)
    def _():
        landed(pmsg.at[pl.ds(0, 14)], ps).wait()


ANY = pl.BlockSpec(memory_space=pl.ANY)
DMA = pltpu.SemaphoreType.DMA


def sweep(t, oovv, vvvv, oooo, wd, wx):
    n, w = t.shape
    depth = vvvv.shape[0]
    V = pltpu.VMEM
    return pl.pallas_call(
        sweep_kernel,
        out_shape=jax.ShapeDtypeStruct((n, w), F32),
        in_specs=[ANY] * 6,
        out_specs=pl.BlockSpec(memory_space=pltpu.VMEM),
        scratch_shapes=[
            V((n, w), F32), V((n, w), BF16), V(oooo.shape, BF16), V((2,) + wd.shape, BF16),
            V((4, 2 * n, w), BF16),
            V((n, 2 * n), F32), V((4, n // 4, 2 * n), F32), V((2 * n, 2 * n), BF16), V((n, w), F32),
            V((n * PITCH, LANE), F32), V((OCC * LANE, 4 * LANE), BF16), V((wx.shape[1], wx.shape[0]), BF16),
            V((4, 2 * VIRT, 4 * LANE), F32), V((4, 4 * VIRT, 2 * LANE), F32),
            V((32 * PITCH, LANE), F32), V((32 * PITCH, LANE), F32),
            V((12, 8, w), F32), V((16, 8, w), F32), V((128, w), F32), V((16, 8, w), F32), V((4, 8, w), F32), V((32, w), F32),
            V((3, depth, STEP), BF16), V((n, w), F32), V((w // STEP, 2 * n, STEP), F32), V(wx.shape, F32),
            DMA((7,)), DMA, DMA((6,)), DMA, DMA((4,)), DMA, DMA, DMA, DMA,
            DMA, DMA, DMA, DMA, DMA, DMA, DMA((3,)), DMA, DMA,
        ],
        compiler_params=pltpu.CompilerParams(collective_id=0, has_side_effects=True, vmem_limit_bytes=46 << 20),
        name="sweep",
    )(*(pltpu.with_memory_space_constraint(a, pltpu.HBM) for a in (t, oovv, vvvv, oooo, wd, wx)))


def solution(mesh):
    def local_sweep(t_blk, d_blk, oovv_blk, vvvv_blk, oooo_full, wd_blk, wx_blk):
        return sweep(t_blk, oovv_blk, vvvv_blk, oooo_full, wd_blk, wx_blk) / d_blk

    amp = P("row", "col")
    wide = P(None, "col")
    return jax.shard_map(local_sweep, mesh=mesh, in_specs=(amp, amp, amp, amp, P(), wide, wide), out_specs=amp, check_vma=False)
```

```python
import jax
import jax.numpy as jnp
from jax import lax
from jax.experimental import pallas as pl
from jax.experimental.pallas import tpu as pltpu
from jax.sharding import PartitionSpec as P

MESH = pl.DeviceIdType.MESH
F32 = jnp.float32
BF16 = jnp.bfloat16
NT = (((1,), (1,)), ((), ()))
TN = (((0,), (0,)), ((), ()))

OCC = 16
VIRT = 96
LANE = 128
PITCH = 104
STEP = 256


def _dev(c, r):
    return {"col": c, "row": r}


def _rcopy(src, dst, ssem, rsem, dev):
    return pltpu.make_async_remote_copy(src, dst, ssem, rsem, device_id=dev, device_id_type=MESH)


def sweep_kernel(t_hbm, oovv_hbm, v_hbm, oooo_hbm, wd_hbm, wx_hbm, out_ref,
                 t32, oovv, oooo, ww, tg, xp, xr, mfull, hole, t4, wd4, wxt, ubuf, vbuf_s, s4, st4,
                 smsg, pmsg, srecv, precv, rmsg, rrecv, vv, theirs, part, wxf,
                 lsem, gs, gr, fs, fr, xs, xrs, ms, mrs, ss, srs, ps, prs, rls, rlr, vsem, rs, rrs):
    r, c = lax.axis_index("row"), lax.axis_index("col")
    x, y = c % 2, c // 2
    o = 1 - r
    nx, ny, dg = y * 2 + (1 - x), (1 - y) * 2 + x, (1 - y) * 2 + (1 - x)
    n, w = t32.shape
    h = w // 2
    h0, h1 = pl.ds(0, h), pl.ds(h, h)
    rows = pl.ds(pl.multiple_of(r * n, n), n)
    orows = pl.ds(pl.multiple_of(o * n, n), n)

    sem = pltpu.get_barrier_semaphore()
    for cc, rr in ((nx, r), (ny, r), (dg, r), (c, o), (nx, o), (ny, o), (dg, o)):
        pl.semaphore_signal(sem, inc=1, device_id=_dev(cc, rr), device_id_type=MESH)

    chunk = n // 4
    tloads = [pltpu.make_async_copy(t_hbm.at[pl.ds(k * chunk, chunk)], t32.at[pl.ds(k * chunk, chunk)], lsem.at[k])
              for k in range(4)]
    for cp in tloads:
        cp.start()
    oload = pltpu.make_async_copy(oovv_hbm, oovv, lsem.at[4])
    hload = pltpu.make_async_copy(oooo_hbm, oooo, lsem.at[5])
    wloads = [pltpu.make_async_copy(a, ww.at[k], lsem.at[6]) for k, a in enumerate((wd_hbm, wx_hbm))]
    for cp in (*wloads, oload, hload):
        cp.start()

    own = c // 2
    half = c % 2
    home = (own + r + 1) % 2
    via = home * nx + (1 - home) * ny
    past = home * ny + (1 - home) * nx
    ro = (home + half) % 2
    di = 1 - ro

    def slot_s(chip, ih, m):
        return pl.ds(pl.multiple_of(((chip * 2 + ih) * 2 + m) * 8, 8), 8)

    def slot_p(kind, a, ih, m):
        return ((kind * 2 + a) * 2 + ih) * 2 + m

    def vcopy(s, slot):
        lanes = pl.ds(pl.multiple_of(s * STEP, STEP), STEP)
        return pltpu.make_async_copy(v_hbm.at[:, lanes], vv.at[slot], vsem.at[slot])

    def landed(like, sem):
        return pltpu.make_async_copy(like, like, sem)

    for k in range(4):
        tloads[k].wait()
        tg[c, pl.ds(pl.multiple_of(r * n + k * chunk, chunk), chunk), :] = t32[k * chunk:(k + 1) * chunk, :].astype(BF16)

    pl.semaphore_wait(sem, 7)

    def tcopy(chip, lanes, k, dev):
        ref = tg.at[chip, rows, lanes]
        return _rcopy(ref, ref, gs, gr.at[k], dev)

    def fcopy(chip, lanes, p, dev):
        ref = tg.at[chip, pl.ds(pl.multiple_of(r * n + p * 32, 32), 32), lanes]
        return _rcopy(ref, ref, fs, fr.at[p], dev)

    whole = pl.ds(0, w)
    x0 = tcopy(c, h0, 1, _dev(nx, r))
    y1 = tcopy(c, h1, 2, _dev(ny, r))
    d_own = tcopy(c, whole, 0, _dev(c, o))
    x1 = tcopy(c, h1, 3, _dev(nx, r))
    y0 = tcopy(c, h0, 4, _dev(ny, r))
    x0.start()
    y1.start()
    d_own.start()
    x1.start()
    y0.start()
    vcopy(0, 0).start()
    vcopy(1, 1).start()

    def spread_rows(chip, ib, first, groups):
        for g in range(first, first + groups):
            tile = tg[chip, pl.ds(pl.multiple_of(r * n + ib * 16, 16), 16), g * 384:(g + 1) * 384].astype(F32)
            for e in range(4):
                slab = tile[:, e * VIRT:(e + 1) * VIRT]
                slab = jnp.concatenate([slab, jnp.zeros((16, LANE - VIRT), F32)], axis=1)
                for half in range(2):
                    start = (ib * 16 + half * 8) * PITCH + chip * 24 + g * 4 + e
                    t4[pl.ds(start, 8, stride=PITCH), :] = slab[half * 8:half * 8 + 8]

    def spread(chip, first, groups):
        @pl.loop(0, n // 16)
        def _(ib):
            spread_rows(chip, ib, first, groups)

    zero8 = jnp.zeros((8, w), F32)
    for m in range(2):
        srecv[slot_s(dg, ro, m), :] = zero8

    @pl.when(home == 0)
    def _():
        for m in range(2):
            precv[slot_p(0, 1 - half, half, m)] = zero8
            precv[slot_p(1, 1 - half, 1 - half, m)] = zero8

    spread(c, 0, 6)

    landed(ww, lsem.at[6]).wait()
    zrow = jnp.zeros((LANE - VIRT, 4 * LANE), BF16)

    @pl.loop(0, OCC)
    def _(k):
        blk = ww[0, pl.ds(pl.multiple_of(k * VIRT, 16), VIRT), :].astype(F32)
        parts = []
        for j in range(4):
            parts += [blk[:, j * VIRT:(j + 1) * VIRT], jnp.zeros((VIRT, LANE - VIRT), F32)]
        wd4[pl.ds(pl.multiple_of(k * LANE, LANE), VIRT), :] = jnp.concatenate(parts, axis=1).astype(BF16)
        wd4[pl.ds(pl.multiple_of(k * LANE + VIRT, 32), LANE - VIRT), :] = zrow
        wxf[pl.ds(pl.multiple_of(k * VIRT, 16), VIRT), :] = ww[1, pl.ds(pl.multiple_of(k * VIRT, 16), VIRT), :].astype(F32)

    for s, chip in enumerate((c, nx, ny, dg)):
        for b in range(3):
            blk = jnp.concatenate(
                [wxf[pl.ds(pl.multiple_of(k * VIRT + chip * 24, 8), 24), b * LANE:(b + 1) * LANE] for k in range(OCC)],
                axis=0)
            wxt[b * LANE:(b + 1) * LANE, s * 384:(s + 1) * 384] = blk.astype(BF16).T

    oload.wait()
    hload.wait()
    d_own.wait_recv()
    xp[...] = lax.dot_general(oovv[...], tg[c], NT, preferred_element_type=F32)

    def direct_rows(chip, i0, count):
        lhs = jnp.concatenate(
            [jnp.concatenate(
                [t4[pl.ds(pl.multiple_of(((i0 + i) * OCC + k) * PITCH + chip * 24, 8), 24), :] for i in range(count)],
                axis=0)
             for k in range(OCC)], axis=1).astype(BF16)
        return jnp.dot(lhs, wd4[...], preferred_element_type=F32)

    def direct(chip):
        ubuf[chip, :, :] = direct_rows(chip, 0, 8)

    def exchange_pair(chips, first, i2):
        halves = []
        for e in range(2):
            halves.append(jnp.concatenate(
                [t4[pl.ds(pl.multiple_of(((2 * i2 + e) * OCC + k) * PITCH + chip * 24, 8), 24), :]
                 for chip in chips for k in range(OCC)], axis=0))
        rhs = jnp.concatenate(halves, axis=1).astype(BF16)
        prod = jnp.dot(wxt[:, first * 384:(first + len(chips)) * 384], rhs, preferred_element_type=F32)
        vbuf_s[i2, :, :] = prod if first == 0 else vbuf_s[i2, :, :] + prod

    def exchange(chips, first):
        @pl.loop(0, 4)
        def _(i2):
            exchange_pair(chips, first, i2)

    direct(c)

    x0.wait_recv()
    for p in range(4):
        fcopy(nx, h0, p, _dev(ny, r)).start()
    y1.wait_recv()
    for p in range(4):
        fcopy(ny, h1, p, _dev(nx, r)).start()
    q = n // 4
    for cc in (nx, ny, dg):
        cp = _rcopy(xp.at[pl.ds(pl.multiple_of(cc * q, q), q)], xr.at[c], xs, xrs, _dev(cc, r))
        cp.start()
    xr[c, :, :] = xp[pl.ds(pl.multiple_of(c * q, q), q), :]
    spread(nx, 0, 3)
    spread(ny, 3, 3)
    x1.wait_recv()
    d_x = tcopy(nx, whole, 5, _dev(c, o))
    d_x.start()
    y0.wait_recv()
    d_y = tcopy(ny, whole, 5, _dev(c, o))
    d_y.start()
    spread(nx, 3, 3)
    spread(ny, 0, 3)
    direct(nx)
    direct(ny)
    exchange((c, nx, ny), 0)

    def s_rows(i, j):
        return pl.ds(pl.multiple_of((i * 4 + j) * PITCH, 8), VIRT)

    def t_rows(i, j):
        return pl.ds(pl.multiple_of(((i // 4) * 16 + j * 4 + i % 4) * PITCH, 8), VIRT)

    def block(i, j):
        direct_part = jnp.concatenate(
            [ubuf[chip, pl.ds(pl.multiple_of(i * 24, 8), 24), pl.ds(pl.multiple_of(j * LANE, LANE), LANE)]
             for chip in range(4)], axis=0)
        return direct_part - vbuf_s[
            i // 2, pl.ds(pl.multiple_of(j * VIRT, 8), VIRT), pl.ds(pl.multiple_of((i % 2) * LANE, LANE), LANE)]

    def fill_s(ih):
        @pl.loop(0, 4)
        def _(j):
            for e in range(4):
                s4[s_rows(ih * 4 + e, j), :] = block(ih * 4 + e, j)

    def fill_t(ih):
        @pl.loop(0, 4)
        def _(j):
            for e in range(4):
                st4[t_rows(ih * 4 + e, j), :VIRT] = s4[s_rows(ih * 4 + e, j), :].T[:VIRT, :]

    def put(src, ih, m, chip, dst):
        first = (ih * 16 + m * 8) * PITCH + chip * 24
        for g in range(6):
            vals = [src[pl.ds(first + g * 4 + e, 8, stride=PITCH), :][:, :VIRT] for e in range(4)]
            dst[:, g * 384:(g + 1) * 384] = jnp.concatenate(vals, axis=1)

    def s_copy(slot, ih, m, chip):
        buf = smsg.at[slot * 4 + ih * 2 + m]
        return _rcopy(buf, srecv.at[slot_s(c, ih, m)], ss, srs, _dev(chip, r))

    def p_copy(slot, ih, m, chip):
        buf = pmsg.at[slot * 4 + ih * 2 + m]
        return _rcopy(buf, precv.at[slot_p(1 - home, half, ih, m)], ps, prs, _dev(chip, own))

    def relay(kind, src):
        @pl.loop(0, 2)
        def _(m):
            put(src, ro, m, dg, rmsg.at[kind * 2 + m])
            to = rrecv.at[pl.ds(pl.multiple_of((kind * 2 + m) * 8, 8), 8)]
            _rcopy(rmsg.at[kind * 2 + m], to, rls, rlr, _dev(via, own)).start()

    def send(src, msg, copy, slot, ih, chip):
        @pl.loop(0, 2)
        def _(m):
            put(src, ih, m, chip, msg.at[slot * 4 + ih * 2 + m])
            copy(slot, ih, m, chip).start()

    def mirror():
        @pl.loop(0, 4)
        def _(j):
            for e in range(4):
                at = s_rows(half * 4 + e, j)
                s4[at, :VIRT] = s4[at, :VIRT] + block(half * 4 + j, e).T[:VIRT, :]

    @pl.loop(0, 4)
    def _(p):
        landed(tg.at[dg, pl.ds(0, n // 4)], fr.at[p]).wait()
        for ib in range(2):
            spread_rows(dg, 2 * p + ib, 0, 6)
        ubuf[dg, pl.ds(pl.multiple_of(p * 48, 16), 48), :] = direct_rows(dg, 2 * p, 2)
        exchange_pair((dg,), 3, p)

        @pl.when(p == 1)
        def _():
            fill_s(0)

            @pl.when(ro == 0)
            def _():
                relay(0, s4)

            @pl.when(jnp.logical_and(ro == 1, home == 0))
            def _():
                send(s4, smsg, s_copy, 1, 0, via)

        @pl.when(jnp.logical_and(p == 2, jnp.logical_and(ro == 1, home == 1)))
        def _():
            mirror()
            send(s4, smsg, s_copy, 1, 0, via)

    d_d = tcopy(dg, whole, 5, _dev(c, o))
    d_d.start()

    fill_s(1)

    @pl.when(ro == 1)
    def _():
        relay(0, s4)

    fill_t(ro)
    relay(1, st4)

    landed(xr.at[pl.ds(0, 3)], xrs).wait()
    xsum = (xr[0] + xr[1]) + (xr[2] + xr[3])
    krows = pl.ds(pl.multiple_of(r * n + c * q, q), q)
    mfull[krows, :] = (oooo[krows, :].astype(F32) + 0.5 * xsum).astype(BF16)
    for cc, rr in ((nx, r), (ny, r), (dg, r), (c, o), (nx, o), (ny, o), (dg, o)):
        part_m = mfull.at[krows, pl.ds(pl.multiple_of(rr * n, n), n)]
        _rcopy(part_m, part_m, ms, mrs, _dev(cc, rr)).start()

    @pl.when(jnp.logical_and(home == 1, di == 1))
    def _():
        mirror()

    def across():
        send(s4, smsg, s_copy, 0, di, dg)

        @pl.when(home == 0)
        def _():
            send(st4, pmsg, p_copy, 0, di, dg)

    @pl.when(home == 0)
    def _():
        fill_t(di)

    @pl.when(dg == 0)
    def _():
        across()

    send(s4, smsg, s_copy, 2, di, past)

    @pl.when(home == 0)
    def _():
        send(st4, pmsg, p_copy, 2, di, past)

    @pl.when(home == 0)
    def _():
        send(st4, pmsg, p_copy, 3, ro, c)
        send(st4, pmsg, p_copy, 3, di, c)

    @pl.loop(0, 2)
    def _(m):
        for ih in range(2):
            put(s4, ih, m, c, srecv.at[slot_s(c, ih, m)])

    @pl.when(home == 1)
    def _():
        @pl.loop(0, 2)
        def _(m):
            put(st4, ro, m, c, precv.at[slot_p(0, half, ro, m)])

    def pass_on():
        landed(rrecv, rlr).wait()
        for kind, (src, msg, copy) in ((1, (s4, smsg, s_copy)), (0, (st4, pmsg, p_copy))):
            for m in range(2):
                buf = msg.at[2 * 4 + ro * 2 + m]
                put(src, ro, m, past, buf)
                buf[...] = buf[...] + rrecv[(kind * 2 + m) * 8:(kind * 2 + m + 1) * 8, :]
                copy(2, ro, m, past).start()

    landed(tg.at[pl.ds(0, 3), pl.ds(0, n)], gr.at[5]).wait()

    def ladder_copy(s):
        lanes = pl.ds(pl.multiple_of(s * STEP, STEP), STEP)
        return _rcopy(part.at[s, orows], theirs.at[:, lanes], rs, rrs, _dev(c, o))

    @pl.loop(0, w // STEP)
    def _(s):
        slot = s % 3

        @pl.when(s + 2 < w // STEP)
        def _():
            vcopy(s + 2, (s + 2) % 3).start()

        vcopy(s, slot).wait()
        va, vb = vv.at[slot, pl.ds(0, w)], vv.at[slot, pl.ds(w, w)]
        part[s, :, :] = (jnp.dot(tg[2 * r], va[...], preferred_element_type=F32)
                         + jnp.dot(tg[2 * r + 1], vb[...], preferred_element_type=F32))
        ladder_copy(s).start()

        @pl.when(s == 0)
        def _():
            send(s4, smsg, s_copy, 1, ro, via)

        @pl.when(jnp.logical_and(s == 1, di == 1))
        def _():
            send(s4, smsg, s_copy, 1, 1, via)

        @pl.when(s == 2)
        def _():
            send(st4, pmsg, p_copy, 1, ro, via)

        @pl.when(jnp.logical_and(s == 3, home == 0))
        def _():
            send(st4, pmsg, p_copy, 1, di, via)

        @pl.when(s == 5)
        def _():
            pass_on()

        @pl.when(jnp.logical_and(s == 6, dg > 0))
        def _():
            across()

    landed(theirs, rrs).wait()
    landed(theirs, rs).wait()

    landed(tg.at[pl.ds(0, 3)], gs).wait()
    landed(tg.at[0, pl.ds(0, n)], fs).wait()
    landed(xr.at[pl.ds(0, 3)], xs).wait()
    all_m = mfull.at[pl.ds(0, 7 * q), pl.ds(0, n)]
    landed(all_m, mrs).wait()
    landed(all_m, ms).wait()
    m_mine = mfull[:, rows]

    @pl.loop(0, w // STEP)
    def _(s):
        lanes = pl.ds(pl.multiple_of(s * STEP, STEP), STEP)
        hole[:, lanes] = lax.dot_general(m_mine, tg[c, :, lanes], TN, preferred_element_type=F32)

    @pl.loop(0, 8)
    def _(i):
        line = pl.ds(pl.multiple_of(i * 16, 16), 16)
        line_r = pl.ds(pl.multiple_of(r * n + i * 16, 16), 16)
        mine = jnp.concatenate([part[s, line_r, :] for s in range(w // STEP)], axis=1)
        out_ref[line, :] = oovv[line, :].astype(F32) + (mine + theirs[line, :] + hole[line, :])

    landed(rmsg, rls).wait()
    landed(srecv.at[pl.ds(0, 80)], srs).wait()
    for i in range(8):
        for jh in range(2):
            line = slice(i * 16 + jh * 8, i * 16 + jh * 8 + 8)
            rows4 = [((2 * jh + cc) * 4 + i // 2) * 8 + i % 2 * 4 for cc in range(2)]
            out_ref[line, :] = out_ref[line, :] + jnp.concatenate([srecv[k:k + 4, :] for k in rows4], axis=0)

    @pl.when(home == 1)
    def _():
        landed(precv.at[pl.ds(0, 10)], prs).wait()

    @pl.when(home == 0)
    def _():
        landed(precv.at[pl.ds(0, 8)], prs).wait()

    zero4 = jnp.zeros((4, w), F32)
    for a in range(2):
        for j in range(4):
            m, rows4 = j // 2, slice(j % 2 * 4, j % 2 * 4 + 4)
            for kind, row in ((0, r), (1, o)):
                line = pl.ds(pl.multiple_of((a * 4 + j) * 16 + row * 8, 8), 8)
                both = [zero4 if kind == 0 and ih == a else precv[slot_p(kind, a, ih, m), rows4, :] for ih in range(2)]
                out_ref[line, :] = out_ref[line, :] + jnp.concatenate(both, axis=0)

    landed(smsg.at[pl.ds(0, 10)], ss).wait()

    @pl.when(home == 1)
    def _():
        landed(pmsg.at[pl.ds(0, 4)], ps).wait()

    @pl.when(home == 0)
    def _():
        landed(pmsg.at[pl.ds(0, 14)], ps).wait()


ANY = pl.BlockSpec(memory_space=pl.ANY)
DMA = pltpu.SemaphoreType.DMA


def sweep(t, oovv, vvvv, oooo, wd, wx):
    n, w = t.shape
    depth = vvvv.shape[0]
    V = pltpu.VMEM
    return pl.pallas_call(
        sweep_kernel,
        out_shape=jax.ShapeDtypeStruct((n, w), F32),
        in_specs=[ANY] * 6,
        out_specs=pl.BlockSpec(memory_space=pltpu.VMEM),
        scratch_shapes=[
            V((n, w), F32), V((n, w), BF16), V(oooo.shape, BF16), V((2,) + wd.shape, BF16),
            V((4, 2 * n, w), BF16),
            V((n, 2 * n), F32), V((4, n // 4, 2 * n), F32), V((2 * n, 2 * n), BF16), V((n, w), F32),
            V((n * PITCH, LANE), F32), V((OCC * LANE, 4 * LANE), BF16), V((wx.shape[1], wx.shape[0]), BF16),
            V((4, 2 * VIRT, 4 * LANE), F32), V((4, 4 * VIRT, 2 * LANE), F32),
            V((32 * PITCH, LANE), F32), V((32 * PITCH, LANE), F32),
            V((12, 8, w), F32), V((16, 8, w), F32), V((128, w), F32), V((16, 8, w), F32), V((4, 8, w), F32), V((32, w), F32),
            V((3, depth, STEP), BF16), V((n, w), F32), V((w // STEP, 2 * n, STEP), F32), V(wx.shape, F32),
            DMA((7,)), DMA, DMA((6,)), DMA, DMA((4,)), DMA, DMA, DMA, DMA,
            DMA, DMA, DMA, DMA, DMA, DMA, DMA((3,)), DMA, DMA,
        ],
        compiler_params=pltpu.CompilerParams(collective_id=0, has_side_effects=True, vmem_limit_bytes=46 << 20),
        name="sweep",
    )(*(pltpu.with_memory_space_constraint(a, pltpu.HBM) for a in (t, oovv, vvvv, oooo, wd, wx)))


def solution(mesh):
    def local_sweep(t_blk, d_blk, oovv_blk, vvvv_blk, oooo_full, wd_blk, wx_blk):
        return sweep(t_blk, oovv_blk, vvvv_blk, oooo_full, wd_blk, wx_blk) / d_blk

    amp = P("row", "col")
    wide = P(None, "col")
    return jax.shard_map(local_sweep, mesh=mesh, in_specs=(amp, amp, amp, amp, P(), wide, wide), out_specs=amp, check_vma=False)
```
